512 devices in a mesh: row: 16 (over y, core), col: 32 (over z, x).
Axes of the slice: x: 4, y: 8, z: 8, core: 2. Of those that a mesh axis runs over, the one named last changes fastest.
Arguments:
- scatter_vectors: float32 [2, 2, 3, 512, 16384], P(None, None, None, 'row', 'col'), may hold values from -80 to 80
- ground_ratio: float32 [3], replicated, may hold values from 0.1 to 1
- vertical_wavenumber: float32 [512, 16384], P('row', 'col'), may hold values from 0.45 to 1.1
- initial_phase: float32 [512, 16384], P('row', 'col'), may hold values from 0.1 to 3.6
- initial_extinction: float32 [512, 16384], P('row', 'col'), may hold values from 0.1 to 2.9
Outputs:
- heights: float32 [512, 16384], P('row', 'col')
- extinction_depth: float32 [512, 16384], P('row', 'col')
The draws below stay inside these ranges and needn't reach their ends.
All inputs are finite; a program needn't handle non-finite values.
Results may differ from the reference program's by a relative error of at most 0.00022.
Values sent between devices are 32-bit elements; how exact they have to be, the bound alone decides.
No kernel may reach another device: no remote copies, remote signals or barrier semaphores. Data moves between devices by JAX's collectives and lax.ppermute only.
A program may use at most 64 MiB of HBM per device.

```python
import jax
import jax.numpy as jnp
from jax import lax

CHANNELS = 3
RADIUS = 9
LAYERS = 16
GAUSS_STEPS = 2
ITERS = 3
NY = 512
NX = 16384


def forest_scene(key):
    keys = jax.random.split(jax.random.fold_in(key, 4242), 8)
    ground = jnp.exp(jax.random.uniform(keys[0], (CHANNELS,), jnp.float32, jnp.log(0.1), jnp.log(1.0)))
    row_place = jnp.arange(NY, dtype=jnp.float32) / NY
    col_place = jnp.arange(NX, dtype=jnp.float32) / NX
    height_true = (1.2 + 1.2 * row_place)[:, None] * jax.random.uniform(keys[1], (NY, NX), jnp.float32, 0.8, 1.25)
    wavenumber = (0.5 + 0.5 * col_place)[None, :] * jax.random.uniform(keys[2], (NY, NX), jnp.float32, 0.9, 1.1)
    phase_true = height_true * wavenumber
    atten_true = jax.random.uniform(keys[3], (NY, NX), jnp.float32, 0.5, 2.5)
    weight_sum = jnp.zeros((NY, NX), jnp.float32)
    cosine_sum = jnp.zeros((NY, NX), jnp.float32)
    sine_sum = jnp.zeros((NY, NX), jnp.float32)
    for layer_index in range(LAYERS):
        layer_depth = (layer_index + 0.5) / LAYERS
        weight = jnp.exp(atten_true * layer_depth)
        weight_sum = weight_sum + weight
        cosine_sum = cosine_sum + weight * jnp.cos(phase_true * layer_depth)
        sine_sum = sine_sum + weight * jnp.sin(phase_true * layer_depth)
    volume_re = cosine_sum / weight_sum
    volume_im = sine_sum / weight_sum
    model_re = (volume_re[None] + ground[:, None, None]) / (1.0 + ground[:, None, None])
    model_im = volume_im[None] / (1.0 + ground[:, None, None])
    keep = jnp.sqrt(jnp.maximum(1.0 - model_re * model_re - model_im * model_im, 0.0))
    signal = jax.random.truncated_normal(keys[4], -4.0, 4.0, (2, CHANNELS, NY, NX), jnp.float32) * 0.7071
    noise = jax.random.truncated_normal(keys[5], -4.0, 4.0, (2, CHANNELS, NY, NX), jnp.float32) * 0.7071
    real_one = signal[0]
    imag_one = signal[1]
    real_two = model_re * real_one - model_im * imag_one + keep * noise[0]
    imag_two = model_re * imag_one + model_im * real_one + keep * noise[1]
    vectors = jnp.stack([jnp.stack([real_one, imag_one]), jnp.stack([real_two, imag_two])])
    phase_guess = phase_true + jax.random.uniform(keys[6], (NY, NX), jnp.float32, -0.25, 0.25)
    atten_guess = atten_true + jax.random.uniform(keys[7], (NY, NX), jnp.float32, -0.4, 0.4)
    return (vectors, ground, wavenumber, phase_guess, atten_guess)


def draw_scatter_vectors(key, part):
    return forest_scene(key)[0]


def draw_ground_ratio(key, part):
    return forest_scene(key)[1]


def draw_vertical_wavenumber(key, part):
    return forest_scene(key)[2]


def draw_initial_phase(key, part):
    return forest_scene(key)[3]


def draw_initial_extinction(key, part):
    return forest_scene(key)[4]


def setup_inputs(seed: int = 0) -> dict:
    splits = jax.random.split(jax.random.key(seed), 6)
    scatter_vectors = draw_scatter_vectors(jax.random.fold_in(splits[5], 71), 0)
    ground_ratio = draw_ground_ratio(jax.random.fold_in(splits[5], 71), 0)
    vertical_wavenumber = draw_vertical_wavenumber(jax.random.fold_in(splits[5], 71), 0)
    initial_phase = draw_initial_phase(jax.random.fold_in(splits[5], 71), 0)
    initial_extinction = draw_initial_extinction(jax.random.fold_in(splits[5], 71), 0)
    return {"scatter_vectors": scatter_vectors, "ground_ratio": ground_ratio, "vertical_wavenumber": vertical_wavenumber, "initial_phase": initial_phase, "initial_extinction": initial_extinction}


EPSILON = 1e-06
DAMPING = 0.002
SMOOTHING = 1.0

def product_fields(vectors):
    real_one = vectors[0, 0]
    imag_one = vectors[0, 1]
    real_two = vectors[1, 0]
    imag_two = vectors[1, 1]
    return jnp.stack([real_one * real_one + imag_one * imag_one, real_two * real_two + imag_two * imag_two, real_one * real_two + imag_one * imag_two, real_one * imag_two - imag_one * real_two])

def column_window(padded, radius):
    span_cols = padded.shape[-1] - 2 * radius
    running = padded[..., 0:span_cols]
    for offset in range(1, 2 * radius + 1):
        running = running + padded[..., offset:offset + span_cols]
    return running

def row_window(padded, radius):
    span_rows = padded.shape[-2] - 2 * radius
    running = padded[..., 0:span_rows, :]
    for offset in range(1, 2 * radius + 1):
        running = running + padded[..., offset:offset + span_rows, :]
    return running

def coherence_pair(window_sums):
    norm_scale = lax.rsqrt(window_sums[0] * window_sums[1] + EPSILON)
    return (window_sums[2] * norm_scale, window_sums[3] * norm_scale)

def channel_summary(coherence_re, coherence_im, ground_ratio):
    ground_weight = 1.0 / (1.0 + ground_ratio)
    weighted_re = lax.optimization_barrier(jnp.sum(coherence_re * ground_weight[:, None, None], axis=0))
    weighted_im = lax.optimization_barrier(jnp.sum(coherence_im * ground_weight[:, None, None], axis=0))
    weight_total = jnp.sum(ground_weight * ground_weight)
    offset_total = jnp.sum(ground_ratio * ground_weight * ground_weight)
    confidence = lax.optimization_barrier(jnp.mean(coherence_re * coherence_re + coherence_im * coherence_im, axis=0))
    return (weighted_re, weighted_im, weight_total, offset_total, confidence)

def volume_moments(phase_height, attenuation):
    weight_sum = jnp.zeros_like(phase_height)
    depth_sum = jnp.zeros_like(phase_height)
    cosine_sum = jnp.zeros_like(phase_height)
    sine_sum = jnp.zeros_like(phase_height)
    depth_cosine = jnp.zeros_like(phase_height)
    depth_sine = jnp.zeros_like(phase_height)
    for layer_index in range(LAYERS):
        layer_depth = (layer_index + 0.5) / LAYERS
        weight = jnp.exp(attenuation * layer_depth)
        cosine = weight * jnp.cos(phase_height * layer_depth)
        sine_term = weight * jnp.sin(phase_height * layer_depth)
        weight_sum = weight_sum + weight
        depth_sum = depth_sum + weight * layer_depth
        cosine_sum = cosine_sum + cosine
        sine_sum = sine_sum + sine_term
        depth_cosine = depth_cosine + cosine * layer_depth
        depth_sine = depth_sine + sine_term * layer_depth
    norm_scale = 1.0 / weight_sum
    return (depth_sum * norm_scale, cosine_sum * norm_scale, sine_sum * norm_scale, depth_cosine * norm_scale, depth_sine * norm_scale)

def gauss_newton(phase_height, attenuation, weighted_re, weighted_im, weight_total, offset_total):
    for gauss_step in range(GAUSS_STEPS):
        mean_depth, real_part, imag_part, depth_cosine, depth_sine = volume_moments(phase_height, attenuation)
        real_by_atten = depth_cosine - mean_depth * real_part
        real_by_phase = -depth_sine
        imag_by_atten = depth_sine - mean_depth * imag_part
        imag_by_phase = depth_cosine
        misfit_re = weighted_re - weight_total * real_part - offset_total
        misfit_im = weighted_im - weight_total * imag_part
        normal_aa = weight_total * (real_by_atten * real_by_atten + imag_by_atten * imag_by_atten) + DAMPING
        normal_ap = weight_total * (real_by_atten * real_by_phase + imag_by_atten * imag_by_phase)
        normal_pp = weight_total * (real_by_phase * real_by_phase + imag_by_phase * imag_by_phase) + DAMPING
        grad_atten = real_by_atten * misfit_re + imag_by_atten * misfit_im
        grad_phase = real_by_phase * misfit_re + imag_by_phase * misfit_im
        determinant = normal_aa * normal_pp - normal_ap * normal_ap
        new_atten = attenuation + (normal_pp * grad_atten - normal_ap * grad_phase) / determinant
        phase_height = phase_height + (normal_aa * grad_phase - normal_ap * grad_atten) / determinant
        attenuation = new_atten
    return (phase_height, attenuation)

def apply_operator(grid_field, confidence):
    padded = jnp.pad(grid_field, 1)
    beside = padded[2:, 1:-1] + padded[:-2, 1:-1] + padded[1:-1, 2:] + padded[1:-1, :-2]
    return confidence * grid_field + SMOOTHING * (4.0 * grid_field - beside)

def reference(scatter_vectors, ground_ratio, vertical_wavenumber, initial_phase, initial_extinction):
    real_parts = []
    imag_parts = []
    for channel in range(CHANNELS):
        fields = product_fields(scatter_vectors[:, :, channel:channel + 1])
        padded = jnp.pad(fields, ((0, 0), (0, 0), (RADIUS, RADIUS), (RADIUS, RADIUS)))
        window_sums = row_window(column_window(padded, RADIUS), RADIUS)
        coherence_re, coherence_im = coherence_pair(window_sums)
        real_parts.append(coherence_re)
        imag_parts.append(coherence_im)
    coherence_re = jnp.concatenate(real_parts, axis=0)
    coherence_im = jnp.concatenate(imag_parts, axis=0)
    weighted_re, weighted_im, weight_total, offset_total, confidence = channel_summary(coherence_re, coherence_im, ground_ratio)
    phase_height, extinction_depth = gauss_newton(initial_phase, initial_extinction, weighted_re, weighted_im, weight_total, offset_total)
    start_height = phase_height / vertical_wavenumber
    solution = start_height
    residual = confidence * start_height - apply_operator(start_height, confidence)
    direction = residual
    norm_now = jnp.sum(residual * residual)
    for iteration in range(ITERS):
        image_field = apply_operator(direction, confidence)
        step_length = norm_now / jnp.sum(direction * image_field)
        solution = solution + step_length * direction
        residual = residual - step_length * image_field
        norm_next = jnp.sum(residual * residual)
        direction = residual + norm_next / norm_now * direction
        norm_now = norm_next
    return (solution, extinction_depth)
```

```python
import jax
import jax.numpy as jnp
from jax import lax
from jax.experimental import pallas as pl
from jax.experimental.pallas import tpu as pltpu
from jax.sharding import PartitionSpec as P

RADIUS = 9
LAYERS = 16
GAUSS_STEPS = 2
EPSILON = 1e-06
DAMPING = 0.002
SCALE = 4.5

H = 32
W = 512
EH = 40
EW = 640
FIELDS = 12
SEND_ROWS = FIELDS * 16 + 3 * 8
STRIPS = (FIELDS + 3) * (EH // 8)
PACK = -(-STRIPS // 8) * 8
VM = pl.BlockSpec(memory_space=pltpu.VMEM)
SM = pl.BlockSpec(memory_space=pltpu.SMEM)
ANY = pl.BlockSpec(memory_space=pl.ANY)
INTERPRET = False


def f32(*shape):
    return jax.ShapeDtypeStruct(shape, jnp.float32)


def call(kernel, outs, ins, scratch=(), name=None):
    return pl.pallas_call(
        kernel,
        out_shape=outs,
        in_specs=ins,
        out_specs=jax.tree.map(lambda _: VM, outs),
        scratch_shapes=scratch,
        name=name,
        interpret=INTERPRET,
    )


def edges_kernel(sv, vw, ip, ie, up, down, sems):
    copies = []
    for f in range(FIELDS):
        copies.append((sv.at[f, pl.ds(0, 16)], up.at[pl.ds(16 * f, 16)]))
        copies.append((sv.at[f, pl.ds(16, 16)], down.at[pl.ds(16 * f, 16)]))
    for j, ref in enumerate((vw, ip, ie)):
        at = FIELDS * 16 + 8 * j
        copies.append((ref.at[pl.ds(0, 8)], up.at[pl.ds(at, 8)]))
        copies.append((ref.at[pl.ds(24, 8)], down.at[pl.ds(at, 8)]))
    started = []
    for n, (src, dst) in enumerate(copies):
        copy = pltpu.make_async_copy(src, dst, sems.at[n])
        copy.start()
        started.append(copy)
    for copy in started:
        copy.wait()


def strip_source(rows, ext, strip):
    field, tile = divmod(strip, EH // 8)
    if field < FIELDS:
        return rows, field * EH + 8 * tile
    return ext, (field - FIELDS) * EH + 8 * tile


def rows_kernel(sv, vw, ip, ie, above, below, rows, ext, left, right, px, s4):
    sub = lax.broadcasted_iota(jnp.int32, (8, 128), 0)
    lane = lax.broadcasted_iota(jnp.int32, (8, 128), 1)

    def one(n, carry):
        k = n // 4
        b = n % 4
        cols = pl.ds(pl.multiple_of(b * 128, 128), 128)

        def parts(q):
            f = q * 3 + k
            return (
                above[pl.ds(pl.multiple_of(16 * f, 16), 16), cols],
                sv[f, :, cols],
                below[pl.ds(pl.multiple_of(16 * f, 16), 16), cols],
            )

        quads = [parts(q) for q in range(4)]
        for p, (at, size) in enumerate(((8, 16), (24, H), (24 + H, 16))):
            re1, im1, re2, im2 = (quad[p] for quad in quads)
            px[0, at : at + size] = re1 * re1 + im1 * im1
            px[1, at : at + size] = re2 * re2 + im2 * im2
            px[2, at : at + size] = re1 * re2 + im1 * im2
            px[3, at : at + size] = re1 * im2 - im1 * re2
        for j in range(4):
            two = px[j, 7:79] + px[j, 8:80]
            four = two[0:64] + (px[j, 9:73] + px[j, 10:74])
            s4[j, 0:64] = four
            eight = four[0:56] + s4[j, 4:60]
            sixteen = eight[0:48] + eight[8:56]
            total = sixteen + two[16:64] + px[j, 25:73]
            at = pl.multiple_of((j * 3 + k) * EH, 8)
            rows[pl.ds(at, H), cols] = total[8:40]
            rows[pl.ds(at + H, 8), cols] = jnp.where(sub < 4, total[40:48], total[0:8])
        return carry

    lax.fori_loop(0, 12, one, 0)
    for j, ref in enumerate((vw, ip, ie)):
        at = FIELDS * 16 + 8 * j
        ext[j * EH : j * EH + H] = ref[...]
        for b in range(4):
            cols = slice(128 * b, 128 * b + 128)
            ext[j * EH + H : j * EH + EH, cols] = jnp.where(
                sub < 4, below[at : at + 8, cols], above[at : at + 8, cols]
            )
    for v in range(PACK // 8):
        low = jnp.zeros((8, 128), jnp.float32)
        high = jnp.zeros((8, 128), jnp.float32)
        for g in range(8):
            strip = 8 * v + g
            if strip >= STRIPS:
                break
            ref, at = strip_source(rows, ext, strip)
            here = (lane >= 16 * g) & (lane < 16 * g + 16)
            first = ref[at : at + 8, 0:128]
            last = ref[at : at + 8, W - 128 : W]
            if g:
                first = pltpu.roll(first, 16 * g, 1)
            if g != 7:
                last = pltpu.roll(last, (16 * g + 16) % 128, 1)
            low = jnp.where(here, first, low)
            high = jnp.where(here, last, high)
        left[8 * v : 8 * v + 8] = low
        right[8 * v : 8 * v + 8] = high


def sincos(x):
    turns = jnp.floor(x * 0.3183098861837907 + 0.5)
    y = x - turns * 3.140625
    y = y - turns * 9.67502593994140625e-4
    y = y - turns * 1.509957990978376432e-7
    odd = turns - 2.0 * jnp.floor(turns * 0.5)
    sign = 1.0 - 2.0 * odd
    z = y * y
    s = -2.3889859e-08
    s = s * z + 2.7525562e-06
    s = s * z - 1.9840874e-04
    s = s * z + 8.3333310e-03
    s = s * z - 1.6666667e-01
    s = y + y * z * s
    c = 2.0875723e-09
    c = c * z - 2.7557319e-07
    c = c * z + 2.4801587e-05
    c = c * z - 1.3888889e-03
    c = c * z + 4.1666667e-02
    c = 1.0 + z * (c * z - 0.5)
    return sign * s, sign * c


def cmul(ar, ai, br, bi):
    return ar * br - ai * bi, ar * bi + ai * br


def moments(phase, atten):
    half_s, half_c = sincos(phase * (0.5 / LAYERS))
    r = jnp.exp(atten * (1.0 / LAYERS))
    zr = r * (half_c * half_c - half_s * half_s)
    zi = r * (2.0 * half_c * half_s)
    n_sum, n_dep = 1.0 + r, r
    sr, si = 1.0 + zr, zi
    dr, di = zr, zi
    count = 2.0
    while count < LAYERS:
        r = r * r
        zr, zi = zr * zr - zi * zi, 2.0 * zr * zi
        n_dep = n_dep + r * (n_dep + count * n_sum)
        n_sum = n_sum + r * n_sum
        tr, ti = cmul(zr, zi, dr + count * sr, di + count * si)
        dr, di = dr + tr, di + ti
        tr, ti = cmul(zr, zi, sr, si)
        sr, si = sr + tr, si + ti
        count = 2.0 * count
    norm = 1.0 / n_sum
    half_c = half_c * norm
    half_s = half_s * norm
    real, imag = cmul(sr, si, half_c, half_s)
    dr, di = cmul(dr, di, half_c, half_s)
    step = 1.0 / LAYERS
    return (
        (n_dep * norm + 0.5) * step,
        real,
        imag,
        (dr + 0.5 * real) * step,
        (di + 0.5 * imag) * step,
    )


def gauss_step(phase, atten, mom, wre, wim, weight, offset):
    mean_depth, real_part, imag_part, depth_cos, depth_sin = mom
    ra = depth_cos - mean_depth * real_part
    rt = -depth_sin
    ia = depth_sin - mean_depth * imag_part
    it = depth_cos
    er = wre - weight * real_part - offset
    ei = wim - weight * imag_part
    maa = weight * (ra * ra + ia * ia) + DAMPING
    map_ = weight * (ra * rt + ia * it)
    mpp = weight * (rt * rt + it * it) + DAMPING
    ga = ra * er + ia * ei
    gp = rt * er + it * ei
    inverse = 1.0 / (maa * mpp - map_ * map_)
    return (
        phase + (maa * gp - map_ * ga) * inverse,
        atten + (mpp * ga - map_ * gp) * inverse,
    )


def around(field):
    return (
        pltpu.roll(field, 1, 0)
        + pltpu.roll(field, EH - 1, 0)
        + pltpu.roll(field, 1, 1)
        + pltpu.roll(field, EW - 1, 1)
    )


def make_fit_kernel(row_count, col_count, group):
    def kernel(
        place, ground, rows, ext, from_left, from_right,
        depth, base, v0, v1, v2, sums,
        hi, mid, lo, win, wide, conf,
    ):
        lane = lax.broadcasted_iota(jnp.int32, (8, 128), 1)

        def halo_tile(strip):
            v, g = divmod(strip, 8)
            lo_part = from_right[8 * v : 8 * v + 8]
            hi_part = from_left[8 * v : 8 * v + 8]
            if g:
                lo_part = pltpu.roll(lo_part, 128 - 16 * g, 1)
            if g != 7:
                hi_part = pltpu.roll(hi_part, 112 - 16 * g, 1)
            return jnp.where(lane < 16, lo_part, jnp.where(lane >= 112, hi_part, 0.0))

        def split(value, at, cols):
            first = value.astype(jnp.bfloat16)
            rest = value - first.astype(jnp.float32)
            second = rest.astype(jnp.bfloat16)
            third = (rest - second.astype(jnp.float32)).astype(jnp.bfloat16)
            for c in cols:
                end = c + value.shape[1]
                hi[at : at + value.shape[0], c:end] = first
                mid[at : at + value.shape[0], c:end] = second
                lo[at : at + value.shape[0], c:end] = third

        for f in range(FIELDS):
            at = f * EH
            halo = jnp.concatenate([halo_tile(f * 5 + i) for i in range(5)], axis=0)
            wide[0, 0:EH, 0:128] = halo
            split(wide[0, 0:EH, 0:128], at, (0, 640))
            split(rows[at : at + EH, 0:128], at, (128, 768))
            for b in range(1, 4):
                split(rows[at : at + EH, 128 * b : 128 * b + 128], at, (128 + 128 * b,))
        for j in range(3):
            wide[j, :, 0:W] = ext[j * EH : j * EH + EH]
            for i in range(5):
                wide[j, 8 * i : 8 * i + 8, W:EW] = halo_tile((FIELDS + j) * 5 + i)

        up = lax.broadcasted_iota(jnp.int32, (384, 128), 0) - 128
        across = lax.broadcasted_iota(jnp.int32, (384, 128), 1)
        band = (jnp.abs(up - across) <= RADIUS).astype(jnp.float32).astype(jnp.bfloat16)

        def dot(a):
            return jnp.dot(a, band, preferred_element_type=jnp.float32)

        for b in range(5):
            cols = slice(128 * b, 128 * b + 384)
            win[:, 128 * b : 128 * b + 128] = dot(hi[:, cols]) + (dot(mid[:, cols]) + dot(lo[:, cols]))

        ratios = [jnp.full((8, 128), ground[k], jnp.float32) for k in range(3)]
        weights = [1.0 / (1.0 + g) for g in ratios]
        weight = weights[0] * weights[0] + weights[1] * weights[1] + weights[2] * weights[2]
        offset = (
            ratios[0] * weights[0] * weights[0]
            + ratios[1] * weights[1] * weights[1]
            + ratios[2] * weights[2] * weights[2]
        )

        def fit(i, carry):
            def tile(f, b):
                return win[pl.ds(pl.multiple_of(f * EH + 8 * i, 8), 8), 128 * b : 128 * b + 128]

            here = pl.ds(pl.multiple_of(8 * i, 8), 8)
            for b in range(5):
                cols = slice(128 * b, 128 * b + 128)
                wre = wim = power = None
                for k in range(3):
                    scale = lax.rsqrt(tile(k, b) * tile(3 + k, b) + EPSILON)
                    cre = tile(6 + k, b) * scale
                    cim = tile(9 + k, b) * scale
                    square = cre * cre + cim * cim
                    if k:
                        wre = wre + cre * weights[k]
                        wim = wim + cim * weights[k]
                        power = power + square
                    else:
                        wre = cre * weights[k]
                        wim = cim * weights[k]
                        power = square
                conf[here, cols] = power * (1.0 / 3.0)
                phase = wide[1, here, cols]
                atten = wide[2, here, cols]
                for _ in range(GAUSS_STEPS):
                    phase, atten = gauss_step(
                        phase, atten, moments(phase, atten), wre, wim, weight, offset
                    )
                wide[2, here, cols] = atten
                wide[0, here, cols] = phase / wide[0, here, cols]
            return carry

        lax.fori_loop(0, 5, fit, 0)

        r = lax.broadcasted_iota(jnp.int32, (EH, EW), 0)
        c = lax.broadcasted_iota(jnp.int32, (EH, EW), 1)
        row_low = jnp.where(place[0] == 0, EH - 4, EH)
        row_high = jnp.where(place[0] == row_count - 1, H, EH - 4)
        col_low = jnp.where(place[1] == 0, EW, EW - 4)
        col_high = jnp.where(place[1] == col_count - 1, W, W + 4)
        row_bad = ((r >= row_high) & (r < EH - 4)) | (r >= row_low)
        col_bad = (c >= col_high) & (c < col_low)
        inside = jnp.logical_not(row_bad | col_bad)

        start = jnp.where(inside, wide[0], 0.0)
        confidence = conf[...] - 0.5
        depth[...] = wide[2, 0:H, 0:W]
        base[...] = start[0:H, 0:W]
        first = jnp.where(inside, around(start) - 4.0 * start, 0.0)
        v0[...] = first[0:H, 0:W]

        def advance(field):
            return jnp.where(inside, (confidence * field - around(field)) * (1.0 / SCALE), 0.0)

        second = advance(first)
        v1[...] = second[0:H, 0:W]
        third = advance(second)
        v2[...] = third[0:H, 0:W]
        fourth = advance(third)
        a0, a1, a2, a3 = (x[0:H, 0:W] for x in (first, second, third, fourth))
        spots = lax.broadcasted_iota(jnp.int32, (1, 128), 1)
        line = jnp.zeros((1, 128), jnp.float32)
        for n, (p, q) in enumerate(((a0, a0), (a0, a1), (a1, a1), (a1, a2), (a2, a2), (a2, a3))):
            product = p * q
            total = jnp.sum(jnp.sum(product, axis=0, keepdims=True), axis=1, keepdims=True)
            line = jnp.where(spots == n, total, line)
        sums[...] = jnp.broadcast_to(line, (group, 128))

    return kernel


def make_relay_kernel(out_group):
    def kernel(parts, out):
        out[...] = jnp.broadcast_to(jnp.sum(parts[...], axis=0, keepdims=True), (out_group, 128))

    return kernel


def form(p, q, b):
    total = None
    for i, x in enumerate(p):
        for j, y in enumerate(q):
            term = x * y * b[i + j]
            total = term if total is None else total + term
    return total


def final_kernel(parts, base, v0, v1, v2, heights):
    line = jnp.sum(parts[...], axis=0, keepdims=True)
    spots = lax.broadcasted_iota(jnp.int32, (1, 128), 1)
    b = [
        jnp.sum(jnp.where(spots == n, line, 0.0), axis=1, keepdims=True) for n in range(6)
    ]

    def times_a(p):
        out = [SCALE * p[0]]
        for low, high in zip(p[:-1], p[1:]):
            out.append(SCALE * (low + high))
        return out + [SCALE * p[-1]]

    one = jnp.ones((1, 1), jnp.float32)
    zero = jnp.zeros((1, 1), jnp.float32)
    residual = [one]
    direction = [one]
    answer = [zero, zero, zero]
    now = b[0]
    for iteration in range(3):
        image = times_a(direction)
        alpha = now / form(direction, image, b)
        for n, x in enumerate(direction):
            answer[n] = answer[n] + alpha * x
        if iteration == 2:
            break
        residual = [
            (residual[n] if n < len(residual) else 0.0) - alpha * x for n, x in enumerate(image)
        ]
        after = form(residual, residual, b)
        beta = after / now
        direction = [
            x + (beta * direction[n] if n < len(direction) else 0.0)
            for n, x in enumerate(residual)
        ]
        now = after
    heights[...] = base[...] + (answer[0] * v0[...] + (answer[1] * v1[...] + answer[2] * v2[...]))


def solution(mesh):
    row_count = mesh.shape["row"]
    col_count = mesh.shape["col"]
    near = 2 * col_count
    far = row_count // 2

    def index(r, c):
        return r * col_count + c

    near_groups = [
        [index(2 * y + core, c) for core in range(2) for c in range(col_count)] for y in range(far)
    ]
    far_groups = [
        [index(2 * y + core, c) for y in range(far)] for core in range(2) for c in range(col_count)
    ]
    both = ("row", "col")

    def chain(count, step):
        return [(i, i + step) for i in range(count) if 0 <= i + step < count]

    def local(scatter_vectors, ground_ratio, wavenumber, phase, extinction):
        sv = scatter_vectors.reshape(FIELDS, H, W)
        copies = 2 * (FIELDS + 3)
        up, down = call(
            edges_kernel,
            (f32(SEND_ROWS, W), f32(SEND_ROWS, W)),
            [ANY] * 4,
            [pltpu.SemaphoreType.DMA((copies,))],
            name="edges",
        )(sv, wavenumber, phase, extinction)
        below = lax.ppermute(up, "row", chain(row_count, -1))
        above = lax.ppermute(down, "row", chain(row_count, 1))
        rows, ext, left, right = call(
            rows_kernel,
            (f32(FIELDS * EH, W), f32(3 * EH, W), f32(PACK, 128), f32(PACK, 128)),
            [VM] * 6,
            [pltpu.VMEM((4, 88, 128), jnp.float32), pltpu.VMEM((4, 64, 128), jnp.float32)],
            name="rowsums",
        )(sv, wavenumber, phase, extinction, above, below)
        from_right = lax.ppermute(left, "col", chain(col_count, -1))
        from_left = lax.ppermute(right, "col", chain(col_count, 1))
        place = jnp.stack([lax.axis_index("row"), lax.axis_index("col")]).astype(jnp.int32)
        depth, base, v0, v1, v2, sums = call(
            make_fit_kernel(row_count, col_count, near),
            tuple(f32(H, W) for _ in range(5)) + (f32(near, 128),),
            [SM, SM] + [VM] * 4,
            [pltpu.VMEM((FIELDS * EH, 896), jnp.bfloat16)] * 3
            + [
                pltpu.VMEM((FIELDS * EH, EW), jnp.float32),
                pltpu.VMEM((3, EH, EW), jnp.float32),
                pltpu.VMEM((EH, EW), jnp.float32),
            ],
            name="fit",
        )(place, ground_ratio, rows, ext, from_left, from_right)
        parts = lax.all_to_all(
            sums.reshape(near, 1, 128), both, 0, 0, axis_index_groups=near_groups
        ).reshape(near, 128)
        parts = call(make_relay_kernel(far), f32(far, 128), [VM], name="relay")(parts)
        parts = lax.all_to_all(
            parts.reshape(far, 1, 128), both, 0, 0, axis_index_groups=far_groups
        ).reshape(far, 128)
        heights = call(final_kernel, f32(H, W), [VM] * 5, name="final")(parts, base, v0, v1, v2)
        return heights, depth

    placed = (P(None, None, None, "row", "col"), P(), P("row", "col"), P("row", "col"), P("row", "col"))
    return jax.shard_map(
        local,
        mesh=mesh,
        in_specs=placed,
        out_specs=(P("row", "col"), P("row", "col")),
        check_vma=False,
    )
```

```python
import jax
import jax.numpy as jnp
from jax import lax
from jax.experimental import pallas as pl
from jax.experimental.pallas import tpu as pltpu
from jax.sharding import PartitionSpec as P

RADIUS = 9
LAYERS = 16
GAUSS_STEPS = 2
EPSILON = 1e-06
DAMPING = 0.002
SCALE = 4.5

H = 32
W = 512
EH = 40
EW = 640
FIELDS = 12
SEND_ROWS = FIELDS * 16 + 3 * 8
STRIPS = (FIELDS + 3) * (EH // 8)
PACK = -(-STRIPS // 8) * 8
VM = pl.BlockSpec(memory_space=pltpu.VMEM)
SM = pl.BlockSpec(memory_space=pltpu.SMEM)
ANY = pl.BlockSpec(memory_space=pl.ANY)
INTERPRET = False


def f32(*shape):
    return jax.ShapeDtypeStruct(shape, jnp.float32)


def call(kernel, outs, ins, scratch=(), name=None, kept=(), far=(), leaves=(), plain=()):
    single = not isinstance(outs, tuple)
    shapes = (outs,) if single else outs
    specs = tuple(ANY if n in leaves else VM for n in range(len(shapes)))
    if not INTERPRET:
        shapes = tuple(
            x if n in leaves or n in plain else pltpu.VMEM(x.shape, x.dtype)
            for n, x in enumerate(shapes)
        )
    run = pl.pallas_call(
        kernel,
        out_shape=shapes[0] if single else shapes,
        in_specs=ins,
        out_specs=specs[0] if single else specs,
        scratch_shapes=scratch,
        name=name,
        interpret=INTERPRET,
        compiler_params=pltpu.CompilerParams(vmem_limit_bytes=16 << 20),
    )

    def apply(*args):
        if not INTERPRET:
            args = tuple(
                pltpu.with_memory_space_constraint(x, pltpu.VMEM if n in kept else pltpu.HBM)
                if n in kept or n in far
                else x
                for n, x in enumerate(args)
            )
        return run(*args)

    return apply


def edges_kernel(sv, vw, ip, ie, up, down, sems):
    copies = []
    for f in range(FIELDS):
        copies.append((sv.at[f, pl.ds(0, 16)], up.at[pl.ds(16 * f, 16)]))
        copies.append((sv.at[f, pl.ds(16, 16)], down.at[pl.ds(16 * f, 16)]))
    for j, ref in enumerate((vw, ip, ie)):
        at = FIELDS * 16 + 8 * j
        copies.append((ref.at[pl.ds(0, 8)], up.at[pl.ds(at, 8)]))
        copies.append((ref.at[pl.ds(24, 8)], down.at[pl.ds(at, 8)]))
    started = []
    for n, (src, dst) in enumerate(copies):
        copy = pltpu.make_async_copy(src, dst, sems.at[n])
        copy.start()
        started.append(copy)
    for copy in started:
        copy.wait()


def strip_source(rows, ext, strip):
    field, tile = divmod(strip, EH // 8)
    if field < FIELDS:
        return rows, field * EH + 8 * tile
    return ext, (field - FIELDS) * EH + 8 * tile


def rows_kernel(sv, vw, ip, ie, above, below, rows, ext, left, right, px, s4):
    sub = lax.broadcasted_iota(jnp.int32, (8, 128), 0)
    lane = lax.broadcasted_iota(jnp.int32, (8, 128), 1)

    def one(n, carry):
        k = n // 4
        b = n % 4
        cols = pl.ds(pl.multiple_of(b * 128, 128), 128)

        def parts(q):
            f = q * 3 + k
            return (
                above[pl.ds(pl.multiple_of(16 * f, 16), 16), cols],
                sv[f, :, cols],
                below[pl.ds(pl.multiple_of(16 * f, 16), 16), cols],
            )

        quads = [parts(q) for q in range(4)]
        for p, (at, size) in enumerate(((8, 16), (24, H), (24 + H, 16))):
            re1, im1, re2, im2 = (quad[p] for quad in quads)
            px[0, at : at + size] = re1 * re1 + im1 * im1
            px[1, at : at + size] = re2 * re2 + im2 * im2
            px[2, at : at + size] = re1 * re2 + im1 * im2
            px[3, at : at + size] = re1 * im2 - im1 * re2
        for j in range(4):
            two = px[j, 7:79] + px[j, 8:80]
            four = two[0:64] + (px[j, 9:73] + px[j, 10:74])
            s4[j, 0:64] = four
            eight = four[0:56] + s4[j, 4:60]
            sixteen = eight[0:48] + eight[8:56]
            total = sixteen + two[16:64] + px[j, 25:73]
            at = pl.multiple_of((j * 3 + k) * EH, 8)
            rows[pl.ds(at, H), cols] = total[8:40]
            rows[pl.ds(at + H, 8), cols] = jnp.where(sub < 4, total[40:48], total[0:8])
        return carry

    lax.fori_loop(0, 12, one, 0)
    for j, ref in enumerate((vw, ip, ie)):
        at = FIELDS * 16 + 8 * j
        ext[j * EH : j * EH + H] = ref[...]
        for b in range(4):
            cols = slice(128 * b, 128 * b + 128)
            ext[j * EH + H : j * EH + EH, cols] = jnp.where(
                sub < 4, below[at : at + 8, cols], above[at : at + 8, cols]
            )
    for v in range(PACK // 8):
        low = jnp.zeros((8, 128), jnp.float32)
        high = jnp.zeros((8, 128), jnp.float32)
        for g in range(8):
            strip = 8 * v + g
            if strip >= STRIPS:
                break
            ref, at = strip_source(rows, ext, strip)
            here = (lane >= 16 * g) & (lane < 16 * g + 16)
            first = ref[at : at + 8, 0:128]
            last = ref[at : at + 8, W - 128 : W]
            if g:
                first = pltpu.roll(first, 16 * g, 1)
            if g != 7:
                last = pltpu.roll(last, (16 * g + 16) % 128, 1)
            low = jnp.where(here, first, low)
            high = jnp.where(here, last, high)
        left[8 * v : 8 * v + 8] = low
        right[8 * v : 8 * v + 8] = high


def sincos(x):
    turns = jnp.floor(x * 0.3183098861837907 + 0.5)
    y = x - turns * 3.140625
    y = y - turns * 9.67502593994140625e-4
    y = y - turns * 1.509957990978376432e-7
    odd = turns - 2.0 * jnp.floor(turns * 0.5)
    sign = 1.0 - 2.0 * odd
    z = y * y
    s = -2.3889859e-08
    s = s * z + 2.7525562e-06
    s = s * z - 1.9840874e-04
    s = s * z + 8.3333310e-03
    s = s * z - 1.6666667e-01
    s = y + y * z * s
    c = 2.0875723e-09
    c = c * z - 2.7557319e-07
    c = c * z + 2.4801587e-05
    c = c * z - 1.3888889e-03
    c = c * z + 4.1666667e-02
    c = 1.0 + z * (c * z - 0.5)
    return sign * s, sign * c


def cmul(ar, ai, br, bi):
    return ar * br - ai * bi, ar * bi + ai * br


def moments(phase, atten):
    half_s, half_c = sincos(phase * (0.5 / LAYERS))
    r = jnp.exp(atten * (1.0 / LAYERS))
    zr = r * (half_c * half_c - half_s * half_s)
    zi = r * (2.0 * half_c * half_s)
    n_sum, n_dep = 1.0 + r, r
    sr, si = 1.0 + zr, zi
    dr, di = zr, zi
    count = 2.0
    while count < LAYERS:
        r = r * r
        zr, zi = zr * zr - zi * zi, 2.0 * zr * zi
        n_dep = n_dep + r * (n_dep + count * n_sum)
        n_sum = n_sum + r * n_sum
        tr, ti = cmul(zr, zi, dr + count * sr, di + count * si)
        dr, di = dr + tr, di + ti
        tr, ti = cmul(zr, zi, sr, si)
        sr, si = sr + tr, si + ti
        count = 2.0 * count
    norm = 1.0 / n_sum
    half_c = half_c * norm
    half_s = half_s * norm
    real, imag = cmul(sr, si, half_c, half_s)
    dr, di = cmul(dr, di, half_c, half_s)
    step = 1.0 / LAYERS
    return (
        (n_dep * norm + 0.5) * step,
        real,
        imag,
        (dr + 0.5 * real) * step,
        (di + 0.5 * imag) * step,
    )


def gauss_step(phase, atten, mom, wre, wim, weight, offset):
    mean_depth, real_part, imag_part, depth_cos, depth_sin = mom
    ra = depth_cos - mean_depth * real_part
    rt = -depth_sin
    ia = depth_sin - mean_depth * imag_part
    it = depth_cos
    er = wre - weight * real_part - offset
    ei = wim - weight * imag_part
    maa = weight * (ra * ra + ia * ia) + DAMPING
    map_ = weight * (ra * rt + ia * it)
    mpp = weight * (rt * rt + it * it) + DAMPING
    ga = ra * er + ia * ei
    gp = rt * er + it * ei
    inverse = 1.0 / (maa * mpp - map_ * map_)
    return (
        phase + (maa * gp - map_ * ga) * inverse,
        atten + (mpp * ga - map_ * gp) * inverse,
    )


def around(field):
    return (
        pltpu.roll(field, 1, 0)
        + pltpu.roll(field, EH - 1, 0)
        + pltpu.roll(field, 1, 1)
        + pltpu.roll(field, EW - 1, 1)
    )


def make_fit_kernel(row_count, col_count, group):
    def kernel(
        place, ground, rows, ext, from_left, from_right,
        depth, base, v0, v1, v2, sums,
        hi, mid, lo, win, wide, conf, sem,
    ):
        lane = lax.broadcasted_iota(jnp.int32, (8, 128), 1)

        def halo_tile(strip):
            v, g = divmod(strip, 8)
            lo_part = from_right[8 * v : 8 * v + 8]
            hi_part = from_left[8 * v : 8 * v + 8]
            if g:
                lo_part = pltpu.roll(lo_part, 128 - 16 * g, 1)
            if g != 7:
                hi_part = pltpu.roll(hi_part, 112 - 16 * g, 1)
            return jnp.where(lane < 16, lo_part, jnp.where(lane >= 112, hi_part, 0.0))

        def split(value, at, cols):
            first = value.astype(jnp.bfloat16)
            rest = value - first.astype(jnp.float32)
            second = rest.astype(jnp.bfloat16)
            third = (rest - second.astype(jnp.float32)).astype(jnp.bfloat16)
            for c in cols:
                end = c + value.shape[1]
                hi[at : at + value.shape[0], c:end] = first
                mid[at : at + value.shape[0], c:end] = second
                lo[at : at + value.shape[0], c:end] = third

        for f in range(FIELDS):
            at = f * EH
            halo = jnp.concatenate([halo_tile(f * 5 + i) for i in range(5)], axis=0)
            wide[0, 0:EH, 0:128] = halo
            split(wide[0, 0:EH, 0:128], at, (0, 640))
            split(rows[at : at + EH, 0:128], at, (128, 768))
            for b in range(1, 4):
                split(rows[at : at + EH, 128 * b : 128 * b + 128], at, (128 + 128 * b,))
        for j in range(3):
            wide[j, :, 0:W] = ext[j * EH : j * EH + EH]
            for i in range(5):
                wide[j, 8 * i : 8 * i + 8, W:EW] = halo_tile((FIELDS + j) * 5 + i)

        up = lax.broadcasted_iota(jnp.int32, (384, 128), 0) - 128
        across = lax.broadcasted_iota(jnp.int32, (384, 128), 1)
        band = (jnp.abs(up - across) <= RADIUS).astype(jnp.float32).astype(jnp.bfloat16)

        def dot(a):
            return jnp.dot(a, band, preferred_element_type=jnp.float32)

        for b in range(5):
            cols = slice(128 * b, 128 * b + 384)
            win[:, 128 * b : 128 * b + 128] = dot(hi[:, cols]) + (dot(mid[:, cols]) + dot(lo[:, cols]))

        ratios = [jnp.full((8, 128), ground[k], jnp.float32) for k in range(3)]
        weights = [1.0 / (1.0 + g) for g in ratios]
        weight = weights[0] * weights[0] + weights[1] * weights[1] + weights[2] * weights[2]
        offset = (
            ratios[0] * weights[0] * weights[0]
            + ratios[1] * weights[1] * weights[1]
            + ratios[2] * weights[2] * weights[2]
        )

        def fit(i, carry):
            def tile(f, b):
                return win[pl.ds(pl.multiple_of(f * EH + 8 * i, 8), 8), 128 * b : 128 * b + 128]

            here = pl.ds(pl.multiple_of(8 * i, 8), 8)
            for b in range(5):
                cols = slice(128 * b, 128 * b + 128)
                wre = wim = power = None
                for k in range(3):
                    scale = lax.rsqrt(tile(k, b) * tile(3 + k, b) + EPSILON)
                    cre = tile(6 + k, b) * scale
                    cim = tile(9 + k, b) * scale
                    square = cre * cre + cim * cim
                    if k:
                        wre = wre + cre * weights[k]
                        wim = wim + cim * weights[k]
                        power = power + square
                    else:
                        wre = cre * weights[k]
                        wim = cim * weights[k]
                        power = square
                conf[here, cols] = power * (1.0 / 3.0)
                phase = wide[1, here, cols]
                atten = wide[2, here, cols]
                for _ in range(GAUSS_STEPS):
                    phase, atten = gauss_step(
                        phase, atten, moments(phase, atten), wre, wim, weight, offset
                    )
                wide[2, here, cols] = atten
                wide[0, here, cols] = phase / wide[0, here, cols]
            return carry

        lax.fori_loop(0, 5, fit, 0)
        written = pltpu.make_async_copy(wide.at[2, pl.ds(0, H), pl.ds(0, W)], depth, sem)
        written.start()

        r = lax.broadcasted_iota(jnp.int32, (EH, EW), 0)
        c = lax.broadcasted_iota(jnp.int32, (EH, EW), 1)
        row_low = jnp.where(place[0] == 0, EH - 4, EH)
        row_high = jnp.where(place[0] == row_count - 1, H, EH - 4)
        col_low = jnp.where(place[1] == 0, EW, EW - 4)
        col_high = jnp.where(place[1] == col_count - 1, W, W + 4)
        row_bad = ((r >= row_high) & (r < EH - 4)) | (r >= row_low)
        col_bad = (c >= col_high) & (c < col_low)
        inside = jnp.logical_not(row_bad | col_bad)

        start = jnp.where(inside, wide[0], 0.0)
        confidence = conf[...] - 0.5
        base[...] = start[0:H, 0:W]
        first = jnp.where(inside, around(start) - 4.0 * start, 0.0)
        v0[...] = first[0:H, 0:W]

        def advance(field):
            return jnp.where(inside, (confidence * field - around(field)) * (1.0 / SCALE), 0.0)

        second = advance(first)
        v1[...] = second[0:H, 0:W]
        third = advance(second)
        v2[...] = third[0:H, 0:W]
        fourth = advance(third)
        a0, a1, a2, a3 = (x[0:H, 0:W] for x in (first, second, third, fourth))
        spots = lax.broadcasted_iota(jnp.int32, (1, 128), 1)
        line = jnp.zeros((1, 128), jnp.float32)
        for n, (p, q) in enumerate(((a0, a0), (a0, a1), (a1, a1), (a1, a2), (a2, a2), (a2, a3))):
            product = p * q
            total = jnp.sum(jnp.sum(product, axis=0, keepdims=True), axis=1, keepdims=True)
            line = jnp.where(spots == n, total, line)
        sums[...] = jnp.broadcast_to(line, (group, 128))
        written.wait()

    return kernel


def make_relay_kernel(out_group):
    def kernel(parts, out):
        out[...] = jnp.broadcast_to(jnp.sum(parts[...], axis=0, keepdims=True), (out_group, 128))

    return kernel


def form(p, q, b):
    total = None
    for i, x in enumerate(p):
        for j, y in enumerate(q):
            term = x * y * b[i + j]
            total = term if total is None else total + term
    return total


def final_kernel(parts, base, v0, v1, v2, heights):
    line = jnp.sum(parts[...], axis=0, keepdims=True)
    spots = lax.broadcasted_iota(jnp.int32, (1, 128), 1)
    b = [
        jnp.sum(jnp.where(spots == n, line, 0.0), axis=1, keepdims=True) for n in range(6)
    ]

    def times_a(p):
        out = [SCALE * p[0]]
        for low, high in zip(p[:-1], p[1:]):
            out.append(SCALE * (low + high))
        return out + [SCALE * p[-1]]

    one = jnp.ones((1, 1), jnp.float32)
    zero = jnp.zeros((1, 1), jnp.float32)
    residual = [one]
    direction = [one]
    answer = [zero, zero, zero]
    now = b[0]
    for iteration in range(3):
        image = times_a(direction)
        alpha = now / form(direction, image, b)
        for n, x in enumerate(direction):
            answer[n] = answer[n] + alpha * x
        if iteration == 2:
            break
        residual = [
            (residual[n] if n < len(residual) else 0.0) - alpha * x for n, x in enumerate(image)
        ]
        after = form(residual, residual, b)
        beta = after / now
        direction = [
            x + (beta * direction[n] if n < len(direction) else 0.0)
            for n, x in enumerate(residual)
        ]
        now = after
    heights[...] = base[...] + (answer[0] * v0[...] + (answer[1] * v1[...] + answer[2] * v2[...]))


def solution(mesh):
    row_count = mesh.shape["row"]
    col_count = mesh.shape["col"]
    near = 2 * col_count
    far = row_count // 2

    def index(r, c):
        return r * col_count + c

    near_groups = [
        [index(2 * y + core, c) for core in range(2) for c in range(col_count)] for y in range(far)
    ]
    far_groups = [
        [index(2 * y + core, c) for y in range(far)] for core in range(2) for c in range(col_count)
    ]
    both = ("row", "col")

    def chain(count, step):
        return [(i, i + step) for i in range(count) if 0 <= i + step < count]

    def local(scatter_vectors, ground_ratio, wavenumber, phase, extinction):
        sv = scatter_vectors.reshape(FIELDS, H, W)
        copies = 2 * (FIELDS + 3)
        up, down = call(
            edges_kernel,
            (f32(SEND_ROWS, W), f32(SEND_ROWS, W)),
            [ANY] * 4,
            [pltpu.SemaphoreType.DMA((copies,))],
            name="edges",
            far=range(4),
        )(sv, wavenumber, phase, extinction)
        below = lax.ppermute(up, "row", chain(row_count, -1))
        above = lax.ppermute(down, "row", chain(row_count, 1))
        rows, ext, left, right = call(
            rows_kernel,
            (f32(FIELDS * EH, W), f32(3 * EH, W), f32(PACK, 128), f32(PACK, 128)),
            [VM] * 6,
            [pltpu.VMEM((4, 88, 128), jnp.float32), pltpu.VMEM((4, 64, 128), jnp.float32)],
            name="rowsums",
            kept=range(6),
        )(sv, wavenumber, phase, extinction, above, below)
        from_right = lax.ppermute(left, "col", chain(col_count, -1))
        from_left = lax.ppermute(right, "col", chain(col_count, 1))
        place = jnp.stack([lax.axis_index("row"), lax.axis_index("col")]).astype(jnp.int32)
        depth, base, v0, v1, v2, sums = call(
            make_fit_kernel(row_count, col_count, near),
            tuple(f32(H, W) for _ in range(5)) + (f32(near, 128),),
            [SM, SM] + [VM] * 4,
            [pltpu.VMEM((FIELDS * EH, 896), jnp.bfloat16)] * 3
            + [
                pltpu.VMEM((FIELDS * EH, EW), jnp.float32),
                pltpu.VMEM((3, EH, EW), jnp.float32),
                pltpu.VMEM((EH, EW), jnp.float32),
                pltpu.SemaphoreType.DMA,
            ],
            name="fit",
            kept=(2, 3, 4, 5),
            leaves=(0,),
        )(place, ground_ratio, rows, ext, from_left, from_right)
        parts = lax.all_to_all(
            sums.reshape(near, 1, 128), both, 0, 0, axis_index_groups=near_groups
        ).reshape(near, 128)
        parts = call(make_relay_kernel(far), f32(far, 128), [VM], name="relay", kept=(0,))(parts)
        parts = lax.all_to_all(
            parts.reshape(far, 1, 128), both, 0, 0, axis_index_groups=far_groups
        ).reshape(far, 128)
        heights = call(final_kernel, f32(H, W), [VM] * 5, name="final", kept=range(5), plain=(0,))(parts, base, v0, v1, v2)
        return heights, depth

    placed = (P(None, None, None, "row", "col"), P(), P("row", "col"), P("row", "col"), P("row", "col"))
    return jax.shard_map(
        local,
        mesh=mesh,
        in_specs=placed,
        out_specs=(P("row", "col"), P("row", "col")),
        check_vma=False,
    )
```

```python
import jax
import jax.numpy as jnp
from jax import lax
from jax.experimental import pallas as pl
from jax.experimental.pallas import tpu as pltpu
from jax.sharding import PartitionSpec as P

RADIUS = 9
LAYERS = 16
GAUSS_STEPS = 2
EPSILON = 1e-06
DAMPING = 0.002
SCALE = 4.5

H = 32
W = 512
EH = 40
EW = 640
FIELDS = 12
SEND_ROWS = FIELDS * 16 + 3 * 8
STRIPS = (FIELDS + 3) * (EH // 8)
PACK = -(-STRIPS // 8) * 8
VM = pl.BlockSpec(memory_space=pltpu.VMEM)
SM = pl.BlockSpec(memory_space=pltpu.SMEM)
ANY = pl.BlockSpec(memory_space=pl.ANY)
INTERPRET = False


def f32(*shape):
    return jax.ShapeDtypeStruct(shape, jnp.float32)


def call(kernel, outs, ins, scratch=(), name=None, kept=(), far=(), leaves=(), plain=(), aliases=None, cost=None):
    single = not isinstance(outs, tuple)
    shapes = (outs,) if single else outs
    specs = tuple(ANY if n in leaves else VM for n in range(len(shapes)))
    if not INTERPRET:
        shapes = tuple(
            x if n in leaves or n in plain else pltpu.VMEM(x.shape, x.dtype)
            for n, x in enumerate(shapes)
        )
    run = pl.pallas_call(
        kernel,
        out_shape=shapes[0] if single else shapes,
        in_specs=ins,
        out_specs=specs[0] if single else specs,
        scratch_shapes=scratch,
        name=name,
        interpret=INTERPRET,
        input_output_aliases=aliases or {},
        cost_estimate=cost,
        compiler_params=pltpu.CompilerParams(vmem_limit_bytes=16 << 20),
    )

    def apply(*args):
        if not INTERPRET:
            args = tuple(
                pltpu.with_memory_space_constraint(x, pltpu.VMEM if n in kept else pltpu.HBM)
                if n in kept or n in far
                else x
                for n, x in enumerate(args)
            )
        return run(*args)

    return apply


def edges_kernel(lifts):
    def kernel(sv, vw, ip, ie, out, sems):
        low = lax.rem(lax.axis_index("row") + lifts, 2)
        copies = []
        for f in range(FIELDS):
            at = pl.ds(pl.multiple_of(16 * low, 16), 16)
            copies.append((sv.at[f, at], out.at[pl.ds(16 * f, 16)]))
        for j, ref in enumerate((vw, ip, ie)):
            at = pl.ds(pl.multiple_of(24 * low, 8), 8)
            copies.append((ref.at[at], out.at[pl.ds(FIELDS * 16 + 8 * j, 8)]))
        started = []
        for n, (src, dst) in enumerate(copies):
            copy = pltpu.make_async_copy(src, dst, sems.at[n])
            copy.start()
            started.append(copy)
        for copy in started:
            copy.wait()

    return kernel


def strip_source(rows, ext, strip):
    field, tile = divmod(strip, EH // 8)
    if field < FIELDS:
        return rows, field * EH + 8 * tile
    return ext, (field - FIELDS) * EH + 8 * tile


def rows_kernel(sv, vw, ip, ie, far, near, rows, ext, far_pack, near_pack, px, s4):
    sub = lax.broadcasted_iota(jnp.int32, (8, 128), 0)
    lane = lax.broadcasted_iota(jnp.int32, (8, 128), 1)
    odd_row = lax.rem(lax.axis_index("row"), 2) == 1
    odd_col = lax.rem(lax.axis_index("col"), 2) == 1

    def sides(at, size, cols):
        one = far[pl.ds(at, size), cols]
        two = near[pl.ds(at, size), cols]
        return jnp.where(odd_row, two, one), jnp.where(odd_row, one, two)

    def one(n, carry):
        k = n // 4
        b = n % 4
        cols = pl.ds(pl.multiple_of(b * 128, 128), 128)

        def parts(q):
            f = q * 3 + k
            above, below = sides(pl.multiple_of(16 * f, 16), 16, cols)
            return above, sv[f, :, cols], below

        quads = [parts(q) for q in range(4)]
        for p, (at, size) in enumerate(((8, 16), (24, H), (24 + H, 16))):
            re1, im1, re2, im2 = (quad[p] for quad in quads)
            px[0, at : at + size] = re1 * re1 + im1 * im1
            px[1, at : at + size] = re2 * re2 + im2 * im2
            px[2, at : at + size] = re1 * re2 + im1 * im2
            px[3, at : at + size] = re1 * im2 - im1 * re2
        for j in range(4):
            two = px[j, 7:79] + px[j, 8:80]
            four = two[0:64] + (px[j, 9:73] + px[j, 10:74])
            s4[j, 0:64] = four
            eight = four[0:56] + s4[j, 4:60]
            sixteen = eight[0:48] + eight[8:56]
            total = sixteen + two[16:64] + px[j, 25:73]
            at = pl.multiple_of((j * 3 + k) * EH, 8)
            rows[pl.ds(at, H), cols] = total[8:40]
            rows[pl.ds(at + H, 8), cols] = jnp.where(sub < 4, total[40:48], total[0:8])
        return carry

    lax.fori_loop(0, 12, one, 0)
    for j, ref in enumerate((vw, ip, ie)):
        ext[j * EH : j * EH + H] = ref[...]
        for b in range(4):
            cols = slice(128 * b, 128 * b + 128)
            above, below = sides(FIELDS * 16 + 8 * j, 8, cols)
            ext[j * EH + H : j * EH + EH, cols] = jnp.where(sub < 4, below, above)
    for v in range(PACK // 8):
        low = jnp.zeros((8, 128), jnp.float32)
        high = jnp.zeros((8, 128), jnp.float32)
        for g in range(8):
            strip = 8 * v + g
            if strip >= STRIPS:
                break
            ref, at = strip_source(rows, ext, strip)
            here = (lane >= 16 * g) & (lane < 16 * g + 16)
            first = ref[at : at + 8, 0:128]
            last = ref[at : at + 8, W - 128 : W]
            if g:
                first = pltpu.roll(first, 16 * g, 1)
            if g != 7:
                last = pltpu.roll(last, (16 * g + 16) % 128, 1)
            low = jnp.where(here, first, low)
            high = jnp.where(here, last, high)
        far_pack[8 * v : 8 * v + 8] = jnp.where(odd_col, high, low)
        near_pack[8 * v : 8 * v + 8] = jnp.where(odd_col, low, high)


def sincos(x):
    turns = jnp.floor(x * 0.3183098861837907 + 0.5)
    y = x - turns * 3.140625
    y = y - turns * 9.67502593994140625e-4
    y = y - turns * 1.509957990978376432e-7
    odd = turns - 2.0 * jnp.floor(turns * 0.5)
    sign = 1.0 - 2.0 * odd
    z = y * y
    s = -2.3889859e-08
    s = s * z + 2.7525562e-06
    s = s * z - 1.9840874e-04
    s = s * z + 8.3333310e-03
    s = s * z - 1.6666667e-01
    s = y + y * z * s
    c = 2.0875723e-09
    c = c * z - 2.7557319e-07
    c = c * z + 2.4801587e-05
    c = c * z - 1.3888889e-03
    c = c * z + 4.1666667e-02
    c = 1.0 + z * (c * z - 0.5)
    return sign * s, sign * c


def cmul(ar, ai, br, bi):
    return ar * br - ai * bi, ar * bi + ai * br


def moments(phase, atten):
    half_s, half_c = sincos(phase * (0.5 / LAYERS))
    r = jnp.exp(atten * (1.0 / LAYERS))
    zr = r * (half_c * half_c - half_s * half_s)
    zi = r * (2.0 * half_c * half_s)
    n_sum, n_dep = 1.0 + r, r
    sr, si = 1.0 + zr, zi
    dr, di = zr, zi
    count = 2.0
    while count < LAYERS:
        r = r * r
        zr, zi = zr * zr - zi * zi, 2.0 * zr * zi
        n_dep = n_dep + r * (n_dep + count * n_sum)
        n_sum = n_sum + r * n_sum
        tr, ti = cmul(zr, zi, dr + count * sr, di + count * si)
        dr, di = dr + tr, di + ti
        tr, ti = cmul(zr, zi, sr, si)
        sr, si = sr + tr, si + ti
        count = 2.0 * count
    norm = 1.0 / n_sum
    half_c = half_c * norm
    half_s = half_s * norm
    real, imag = cmul(sr, si, half_c, half_s)
    dr, di = cmul(dr, di, half_c, half_s)
    step = 1.0 / LAYERS
    return (
        (n_dep * norm + 0.5) * step,
        real,
        imag,
        (dr + 0.5 * real) * step,
        (di + 0.5 * imag) * step,
    )


def gauss_step(phase, atten, mom, wre, wim, weight, offset):
    mean_depth, real_part, imag_part, depth_cos, depth_sin = mom
    ra = depth_cos - mean_depth * real_part
    rt = -depth_sin
    ia = depth_sin - mean_depth * imag_part
    it = depth_cos
    er = wre - weight * real_part - offset
    ei = wim - weight * imag_part
    maa = weight * (ra * ra + ia * ia) + DAMPING
    map_ = weight * (ra * rt + ia * it)
    mpp = weight * (rt * rt + it * it) + DAMPING
    ga = ra * er + ia * ei
    gp = rt * er + it * ei
    inverse = 1.0 / (maa * mpp - map_ * map_)
    return (
        phase + (maa * gp - map_ * ga) * inverse,
        atten + (mpp * ga - map_ * gp) * inverse,
    )


def early_kernel(ground, ip, ie, mom, shares):
    ratios = [jnp.full((8, 128), ground[k], jnp.float32) for k in range(3)]
    weights = [1.0 / (1.0 + g) for g in ratios]
    weight = weights[0] * weights[0] + weights[1] * weights[1] + weights[2] * weights[2]
    offset = (
        ratios[0] * weights[0] * weights[0]
        + ratios[1] * weights[1] * weights[1]
        + ratios[2] * weights[2] * weights[2]
    )
    for n, value in enumerate((*weights, weight, offset)):
        shares[8 * n : 8 * n + 8] = value

    def tiles(i, carry):
        here = pl.ds(pl.multiple_of(8 * i, 8), 8)
        for b in range(4):
            cols = slice(128 * b, 128 * b + 128)
            for n, value in enumerate(moments(ip[here, cols], ie[here, cols])):
                mom[n, here, cols] = value
        return carry

    lax.fori_loop(0, H // 8, tiles, 0)


def split(value):
    first = value.astype(jnp.bfloat16)
    return first, (value - first.astype(jnp.float32)).astype(jnp.bfloat16)


def band(height, width, shift):
    up = lax.broadcasted_iota(jnp.int32, (height, width), 0) - shift
    across = lax.broadcasted_iota(jnp.int32, (height, width), 1)
    return (jnp.abs(up - across) <= RADIUS).astype(jnp.float32).astype(jnp.bfloat16)


def dot(a, b):
    return jnp.dot(a, b, preferred_element_type=jnp.float32)


def columns_kernel(rows, ext, held, win, mom, hi, lo):
    if INTERPRET:
        mom[:, 0:H] = held[:, 0:H]
    for n in range(6):
        here = slice(80 * n, 80 * n + 80)
        for b in range(4):
            cols = slice(128 * b, 128 * b + 128)
            hi[here, cols], lo[here, cols] = split(rows[here, cols])
    left = band(384, 256, 0)
    right = band(384, 256, 128)
    win[:, 0:256] = dot(hi[:, 0:384], left) + dot(lo[:, 0:384], left)
    win[:, 256:512] = dot(hi[:, 128:512], right) + dot(lo[:, 128:512], right)
    before = band(128, 128, 128)
    after = band(128, 128, -128)
    win[:, 512:640] = (dot(hi[:, 384:512], before) + dot(lo[:, 384:512], before)) + (
        dot(hi[:, 0:128], after) + dot(lo[:, 0:128], after)
    )
    for b in range(4):
        cols = slice(128 * b, 128 * b + 128)
        values = moments(ext[EH + H : EH + EH, cols], ext[2 * EH + H : 2 * EH + EH, cols])
        for n, value in enumerate(values):
            mom[n, H:EH, cols] = value


def around(field):
    return (
        pltpu.roll(field, 1, 0)
        + pltpu.roll(field, EH - 1, 0)
        + pltpu.roll(field, 1, 1)
        + pltpu.roll(field, EW - 1, 1)
    )


def make_fit_kernel(row_count, col_count, group):
    def kernel(
        win, ext, mom, shares, far, near,
        depth, base, v0, v1, v2, sums,
        hi, lo, rim, wide, conf, sem,
    ):
        lane = lax.broadcasted_iota(jnp.int32, (8, 128), 1)
        row = lax.axis_index("row")
        col = lax.axis_index("col")
        odd_col = lax.rem(col, 2) == 1
        packs = {}

        def halo_tile(strip):
            v, g = divmod(strip, 8)
            if v not in packs:
                one = far[8 * v : 8 * v + 8]
                two = near[8 * v : 8 * v + 8]
                packs[v] = (jnp.where(odd_col, one, two), jnp.where(odd_col, two, one))
            lo_part, hi_part = packs[v]
            if g:
                lo_part = pltpu.roll(lo_part, 128 - 16 * g, 1)
            if g != 7:
                hi_part = pltpu.roll(hi_part, 112 - 16 * g, 1)
            return jnp.where(lane < 16, lo_part, jnp.where(lane >= 112, hi_part, 0.0))

        for n in range(6):
            halo = jnp.concatenate([halo_tile(10 * n + i) for i in range(10)], axis=0)
            hi[80 * n : 80 * n + 80], lo[80 * n : 80 * n + 80] = split(halo)
        for j in range(3):
            for i in range(5):
                wide[j, 8 * i : 8 * i + 8, W:EW] = halo_tile((FIELDS + j) * 5 + i)
        for n, shift in enumerate((128, 0, -128)):
            part = band(128, 128, shift)
            rim[:, 128 * n : 128 * n + 128] = dot(hi[...], part) + dot(lo[...], part)
        rim_of = {0: 0, 4: 1, 3: 2}
        weights = [shares[8 * n : 8 * n + 8] for n in range(3)]
        weight = shares[24:32]
        offset = shares[32:40]

        def fit(i, carry):
            here = pl.ds(pl.multiple_of(8 * i, 8), 8)

            def tile(f, b):
                at = pl.ds(pl.multiple_of(f * EH + 8 * i, 8), 8)
                value = win[at, 128 * b : 128 * b + 128]
                if b in rim_of:
                    value = value + rim[at, 128 * rim_of[b] : 128 * rim_of[b] + 128]
                return value

            for b in range(5):
                cols = slice(128 * b, 128 * b + 128)
                wre = wim = power = None
                for k in range(3):
                    scale = lax.rsqrt(tile(k, b) * tile(3 + k, b) + EPSILON)
                    cre = tile(6 + k, b) * scale
                    cim = tile(9 + k, b) * scale
                    square = cre * cre + cim * cim
                    if k:
                        wre = wre + cre * weights[k]
                        wim = wim + cim * weights[k]
                        power = power + square
                    else:
                        wre = cre * weights[k]
                        wim = cim * weights[k]
                        power = square
                conf[here, cols] = power * (1.0 / 3.0)
                if b < 4:
                    kz, phase, atten = (
                        ext[pl.ds(pl.multiple_of(j * EH + 8 * i, 8), 8), cols] for j in range(3)
                    )
                else:
                    kz, phase, atten = (wide[j, here, cols] for j in range(3))
                for step in range(GAUSS_STEPS):
                    if step or b == 4:
                        now = moments(phase, atten)
                    else:
                        now = tuple(mom[n, here, cols] for n in range(5))
                    phase, atten = gauss_step(phase, atten, now, wre, wim, weight, offset)
                wide[2, here, cols] = atten
                wide[0, here, cols] = phase / kz
            return carry

        lax.fori_loop(0, 5, fit, 0)
        written = pltpu.make_async_copy(wide.at[2, pl.ds(0, H), pl.ds(0, W)], depth, sem)
        written.start()

        r = lax.broadcasted_iota(jnp.int32, (EH, EW), 0)
        c = lax.broadcasted_iota(jnp.int32, (EH, EW), 1)
        row_low = jnp.where(row == 0, EH - 4, EH)
        row_high = jnp.where(row == row_count - 1, H, EH - 4)
        col_low = jnp.where(col == 0, EW, EW - 4)
        col_high = jnp.where(col == col_count - 1, W, W + 4)
        row_bad = ((r >= row_high) & (r < EH - 4)) | (r >= row_low)
        col_bad = (c >= col_high) & (c < col_low)
        inside = jnp.logical_not(row_bad | col_bad)

        start = jnp.where(inside, wide[0], 0.0)
        confidence = conf[...] - 0.5
        base[...] = start[0:H, 0:W]
        first = jnp.where(inside, around(start) - 4.0 * start, 0.0)
        v0[...] = first[0:H, 0:W]

        def advance(field):
            return jnp.where(inside, (confidence * field - around(field)) * (1.0 / SCALE), 0.0)

        second = advance(first)
        v1[...] = second[0:H, 0:W]
        third = advance(second)
        v2[...] = third[0:H, 0:W]
        fourth = advance(third)
        a0, a1, a2, a3 = (x[0:H, 0:W] for x in (first, second, third, fourth))
        spots = lax.broadcasted_iota(jnp.int32, (1, 128), 1)
        line = jnp.zeros((1, 128), jnp.float32)
        for n, (p, q) in enumerate(((a0, a0), (a0, a1), (a1, a1), (a1, a2), (a2, a2), (a2, a3))):
            product = p * q
            total = jnp.sum(jnp.sum(product, axis=0, keepdims=True), axis=1, keepdims=True)
            line = jnp.where(spots == n, total, line)
        sums[...] = jnp.broadcast_to(line, (group, 128))
        written.wait()

    return kernel


def make_relay_kernel(out_group):
    def kernel(parts, out):
        out[...] = jnp.broadcast_to(jnp.sum(parts[...], axis=0, keepdims=True), (out_group, 128))

    return kernel


def form(p, q, b):
    total = None
    for i, x in enumerate(p):
        for j, y in enumerate(q):
            term = x * y * b[i + j]
            total = term if total is None else total + term
    return total


def final_kernel(parts, base, v0, v1, v2, heights):
    line = jnp.sum(parts[...], axis=0, keepdims=True)
    spots = lax.broadcasted_iota(jnp.int32, (1, 128), 1)
    b = [
        jnp.sum(jnp.where(spots == n, line, 0.0), axis=1, keepdims=True) for n in range(6)
    ]

    def times_a(p):
        out = [SCALE * p[0]]
        for low, high in zip(p[:-1], p[1:]):
            out.append(SCALE * (low + high))
        return out + [SCALE * p[-1]]

    one = jnp.ones((1, 1), jnp.float32)
    zero = jnp.zeros((1, 1), jnp.float32)
    residual = [one]
    direction = [one]
    answer = [zero, zero, zero]
    now = b[0]
    for iteration in range(3):
        image = times_a(direction)
        alpha = now / form(direction, image, b)
        for n, x in enumerate(direction):
            answer[n] = answer[n] + alpha * x
        if iteration == 2:
            break
        residual = [
            (residual[n] if n < len(residual) else 0.0) - alpha * x for n, x in enumerate(image)
        ]
        after = form(residual, residual, b)
        beta = after / now
        direction = [
            x + (beta * direction[n] if n < len(direction) else 0.0)
            for n, x in enumerate(residual)
        ]
        now = after
    heights[...] = base[...] + (answer[0] * v0[...] + (answer[1] * v1[...] + answer[2] * v2[...]))


def solution(mesh):
    row_count = mesh.shape["row"]
    col_count = mesh.shape["col"]
    near_count = 2 * col_count
    far_count = row_count // 2

    def index(r, c):
        return r * col_count + c

    near_groups = [
        [index(2 * y + core, c) for core in range(2) for c in range(col_count)] for y in range(far_count)
    ]
    far_groups = [
        [index(2 * y + core, c) for y in range(far_count)] for core in range(2) for c in range(col_count)
    ]
    both = ("row", "col")

    def swap(count, start):
        pairs = [(i, i + 1) for i in range(start, count - 1, 2)]
        return pairs + [(j, i) for i, j in pairs]

    def local(scatter_vectors, ground_ratio, wavenumber, phase, extinction):
        sv = scatter_vectors.reshape(FIELDS, H, W)
        inputs = (sv, wavenumber, phase, extinction)

        def edges(lifts, name):
            return call(
                edges_kernel(lifts),
                f32(SEND_ROWS, W),
                [ANY] * 4,
                [pltpu.SemaphoreType.DMA((FIELDS + 3,))],
                name=name,
                far=range(4),
            )(*inputs)

        busy = pl.CostEstimate(flops=6000000, transcendentals=0, bytes_accessed=0)
        far = lax.ppermute(edges(0, "faredges"), "row", swap(row_count, 1))
        near = lax.ppermute(edges(1, "nearedges"), "row", swap(row_count, 0))
        mom, shares = call(
            early_kernel,
            (f32(5, EH, W), f32(40, 128)),
            [SM, VM, VM],
            name="early",
            kept=(1, 2),
            cost=busy,
        )(ground_ratio, phase, extinction)
        far, near, mom, shares = lax.optimization_barrier((far, near, mom, shares))
        rows, ext, left, right = call(
            rows_kernel,
            (f32(FIELDS * EH, W), f32(3 * EH, W), f32(PACK, 128), f32(PACK, 128)),
            [VM] * 6,
            [pltpu.VMEM((4, 88, 128), jnp.float32), pltpu.VMEM((4, 64, 128), jnp.float32)],
            name="rowsums",
            kept=range(6),
        )(*inputs, far, near)
        far = lax.ppermute(left, "col", swap(col_count, 1))
        near = lax.ppermute(right, "col", swap(col_count, 0))
        win, mom = call(
            columns_kernel,
            (f32(FIELDS * EH, EW), f32(5, EH, W)),
            [VM] * 3,
            [pltpu.VMEM((FIELDS * EH, W), jnp.bfloat16)] * 2,
            name="colsums",
            kept=range(3),
            aliases={2: 1},
            cost=busy,
        )(rows, ext, mom)
        depth, base, v0, v1, v2, sums = call(
            make_fit_kernel(row_count, col_count, near_count),
            tuple(f32(H, W) for _ in range(5)) + (f32(near_count, 128),),
            [VM] * 6,
            [pltpu.VMEM((FIELDS * EH, 128), jnp.bfloat16)] * 2
            + [
                pltpu.VMEM((FIELDS * EH, 384), jnp.float32),
                pltpu.VMEM((3, EH, EW), jnp.float32),
                pltpu.VMEM((EH, EW), jnp.float32),
                pltpu.SemaphoreType.DMA,
            ],
            name="fit",
            kept=range(6),
            leaves=(0,),
        )(win, ext, mom, shares, far, near)
        parts = lax.all_to_all(
            sums.reshape(near_count, 1, 128), both, 0, 0, axis_index_groups=near_groups
        ).reshape(near_count, 128)
        parts = call(make_relay_kernel(far_count), f32(far_count, 128), [VM], name="relay", kept=(0,))(parts)
        parts = lax.all_to_all(
            parts.reshape(far_count, 1, 128), both, 0, 0, axis_index_groups=far_groups
        ).reshape(far_count, 128)
        heights = call(final_kernel, f32(H, W), [VM] * 5, name="final", kept=range(5), plain=(0,))(parts, base, v0, v1, v2)
        return heights, depth

    placed = (P(None, None, None, "row", "col"), P(), P("row", "col"), P("row", "col"), P("row", "col"))
    return jax.shard_map(
        local,
        mesh=mesh,
        in_specs=placed,
        out_specs=(P("row", "col"), P("row", "col")),
        check_vma=False,
    )
```

```python
import jax
import jax.numpy as jnp
from jax import lax
from jax.experimental import pallas as pl
from jax.experimental.pallas import tpu as pltpu
from jax.sharding import PartitionSpec as P

RADIUS = 9
LAYERS = 16
GAUSS_STEPS = 2
EPSILON = 1e-06
DAMPING = 0.002
SCALE = 4.5

H = 32
W = 512
EH = 40
EW = 640
FIELDS = 12
SIDE = RADIUS + 4
REST = SIDE - 8
REST_AT = FIELDS * 8
EXTRA_AT = REST_AT + FIELDS * REST
SEND_ROWS = EXTRA_AT + 3 * 4
GROUPS = 128 // SIDE
PACK = 8 * (-(-FIELDS * 5 // GROUPS) + 1)
VM = pl.BlockSpec(memory_space=pltpu.VMEM)
SM = pl.BlockSpec(memory_space=pltpu.SMEM)
ANY = pl.BlockSpec(memory_space=pl.ANY)
INTERPRET = False


def f32(*shape):
    return jax.ShapeDtypeStruct(shape, jnp.float32)


def call(kernel, outs, ins, scratch=(), name=None, kept=(), far=(), leaves=(), plain=(), aliases=None, cost=None):
    single = not isinstance(outs, tuple)
    shapes = (outs,) if single else outs
    specs = tuple(ANY if n in leaves else VM for n in range(len(shapes)))
    if not INTERPRET:
        shapes = tuple(
            x if n in leaves or n in plain else pltpu.VMEM(x.shape, x.dtype)
            for n, x in enumerate(shapes)
        )
    run = pl.pallas_call(
        kernel,
        out_shape=shapes[0] if single else shapes,
        in_specs=ins,
        out_specs=specs[0] if single else specs,
        scratch_shapes=scratch,
        name=name,
        interpret=INTERPRET,
        input_output_aliases=aliases or {},
        cost_estimate=cost,
        compiler_params=pltpu.CompilerParams(vmem_limit_bytes=16 << 20),
    )

    def apply(*args):
        if not INTERPRET:
            args = tuple(
                pltpu.with_memory_space_constraint(x, pltpu.VMEM if n in kept else pltpu.HBM)
                if n in kept or n in far
                else x
                for n, x in enumerate(args)
            )
        return run(*args)

    return apply


def edges_kernel(lifts):
    def kernel(sv, vw, ip, ie, out, tiles, rest, extra, sems):
        low = lax.rem(lax.axis_index("row") + lifts, 2)
        edge = pl.ds(pl.multiple_of(24 * low, 8), 8)
        inner = pl.ds(pl.multiple_of(8 + 8 * low, 8), 8)
        started = [
            pltpu.make_async_copy(sv.at[:, inner], rest, sems.at[0]),
            pltpu.make_async_copy(sv.at[:, edge], tiles, sems.at[1]),
        ]
        for j, ref in enumerate((vw, ip, ie)):
            started.append(pltpu.make_async_copy(ref.at[edge], extra.at[j], sems.at[2 + j]))
        for copy in started:
            copy.start()
        for copy in started:
            copy.wait()
        bottom = low == 1
        for f in range(FIELDS):
            out[8 * f : 8 * f + 8] = tiles[f]
            at = REST_AT + REST * f
            out[at : at + REST] = jnp.where(bottom, rest[f, 8 - REST : 8], rest[f, 0:REST])
        for j in range(3):
            at = EXTRA_AT + 4 * j
            out[at : at + 4] = jnp.where(bottom, extra[j, 4:8], extra[j, 0:4])

    return kernel


def strips():
    out = []
    for n in range(FIELDS * 5):
        out.append((n // GROUPS, SIDE * (n % GROUPS), SIDE))
    for n in range(3 * 5):
        out.append((PACK // 8 - 1, 4 * n, 4))
    return out


def rows_kernel(sv, vw, ip, ie, far, near, rows, ext, far_pack, near_pack, px, s4):
    sub = lax.broadcasted_iota(jnp.int32, (8, 128), 0)
    lane = lax.broadcasted_iota(jnp.int32, (8, 128), 1)
    odd_row = lax.rem(lax.axis_index("row"), 2) == 1
    odd_col = lax.rem(lax.axis_index("col"), 2) == 1

    def sides(at, size, cols):
        one = far[at : at + size, cols]
        two = near[at : at + size, cols]
        return jnp.where(odd_row, two, one), jnp.where(odd_row, one, two)

    for k in range(3):

        def block(b, carry, k=k):
            cols = pl.ds(pl.multiple_of(b * 128, 128), 128)

            def parts(q):
                f = q * 3 + k
                above, below = sides(8 * f, 8, cols)
                above_rest, below_rest = sides(REST_AT + REST * f, REST, cols)
                return above_rest, above, sv[f, :, cols], below, below_rest

            quads = [parts(q) for q in range(4)]
            at = 24 - SIDE
            for p, size in enumerate((REST, 8, H, 8, REST)):
                re1, im1, re2, im2 = (quad[p] for quad in quads)
                px[0, at : at + size] = re1 * re1 + im1 * im1
                px[1, at : at + size] = re2 * re2 + im2 * im2
                px[2, at : at + size] = re1 * re2 + im1 * im2
                px[3, at : at + size] = re1 * im2 - im1 * re2
                at += size
            for j in range(4):
                two = px[j, 7:79] + px[j, 8:80]
                four = two[0:64] + (px[j, 9:73] + px[j, 10:74])
                s4[j, 0:64] = four
                eight = four[0:56] + s4[j, 4:60]
                sixteen = eight[0:48] + eight[8:56]
                total = sixteen + two[16:64] + px[j, 25:73]
                at = (j * 3 + k) * EH
                rows[at : at + H, cols] = total[8:40]
                rows[at + H : at + EH, cols] = jnp.where(sub < 4, total[40:48], total[0:8])
            return carry

        lax.fori_loop(0, 4, block, 0)
    for j, ref in enumerate((vw, ip, ie)):
        ext[j * EH : j * EH + H] = ref[...]
        above, below = sides(EXTRA_AT + 4 * j, 4, slice(0, W))
        ext[j * EH + H : j * EH + H + 4] = below
        ext[j * EH + H + 4 : j * EH + EH] = above
    low = [jnp.zeros((8, 128), jnp.float32)] * (PACK // 8)
    high = list(low)
    for n, (v, at, width) in enumerate(strips()):
        here = (lane >= at) & (lane < at + width)
        ref = rows if n < FIELDS * 5 else ext
        top = 8 * n if n < FIELDS * 5 else 8 * n - FIELDS * EH
        first = ref[top : top + 8, 0:128]
        last = ref[top : top + 8, W - 128 : W]
        if at:
            first = pltpu.roll(first, at, 1)
        last = pltpu.roll(last, at + width, 1)
        low[v] = jnp.where(here, first, low[v])
        high[v] = jnp.where(here, last, high[v])
    for v in range(PACK // 8):
        far_pack[8 * v : 8 * v + 8] = jnp.where(odd_col, high[v], low[v])
        near_pack[8 * v : 8 * v + 8] = jnp.where(odd_col, low[v], high[v])


def sincos(x):
    turns = jnp.floor(x * 0.3183098861837907 + 0.5)
    y = x - turns * 3.140625
    y = y - turns * 9.67502593994140625e-4
    y = y - turns * 1.509957990978376432e-7
    odd = turns - 2.0 * jnp.floor(turns * 0.5)
    sign = 1.0 - 2.0 * odd
    z = y * y
    s = -2.3889859e-08
    s = s * z + 2.7525562e-06
    s = s * z - 1.9840874e-04
    s = s * z + 8.3333310e-03
    s = s * z - 1.6666667e-01
    s = y + y * z * s
    c = 2.0875723e-09
    c = c * z - 2.7557319e-07
    c = c * z + 2.4801587e-05
    c = c * z - 1.3888889e-03
    c = c * z + 4.1666667e-02
    c = 1.0 + z * (c * z - 0.5)
    return sign * s, sign * c


def cmul(ar, ai, br, bi):
    return ar * br - ai * bi, ar * bi + ai * br


def moments(phase, atten):
    half_s, half_c = sincos(phase * (0.5 / LAYERS))
    r = jnp.exp(atten * (1.0 / LAYERS))
    zr = r * (half_c * half_c - half_s * half_s)
    zi = r * (2.0 * half_c * half_s)
    n_sum, n_dep = 1.0 + r, r
    sr, si = 1.0 + zr, zi
    dr, di = zr, zi
    count = 2.0
    while count < LAYERS:
        r = r * r
        zr, zi = zr * zr - zi * zi, 2.0 * zr * zi
        n_dep = n_dep + r * (n_dep + count * n_sum)
        n_sum = n_sum + r * n_sum
        tr, ti = cmul(zr, zi, dr + count * sr, di + count * si)
        dr, di = dr + tr, di + ti
        tr, ti = cmul(zr, zi, sr, si)
        sr, si = sr + tr, si + ti
        count = 2.0 * count
    norm = 1.0 / n_sum
    half_c = half_c * norm
    half_s = half_s * norm
    real, imag = cmul(sr, si, half_c, half_s)
    dr, di = cmul(dr, di, half_c, half_s)
    step = 1.0 / LAYERS
    return (
        (n_dep * norm + 0.5) * step,
        real,
        imag,
        (dr + 0.5 * real) * step,
        (di + 0.5 * imag) * step,
    )


def gauss_step(phase, atten, mom, wre, wim, weight, offset):
    mean_depth, real_part, imag_part, depth_cos, depth_sin = mom
    ra = depth_cos - mean_depth * real_part
    rt = -depth_sin
    ia = depth_sin - mean_depth * imag_part
    it = depth_cos
    er = wre - weight * real_part - offset
    ei = wim - weight * imag_part
    maa = weight * (ra * ra + ia * ia) + DAMPING
    map_ = weight * (ra * rt + ia * it)
    mpp = weight * (rt * rt + it * it) + DAMPING
    ga = ra * er + ia * ei
    gp = rt * er + it * ei
    inverse = 1.0 / (maa * mpp - map_ * map_)
    return (
        phase + (maa * gp - map_ * ga) * inverse,
        atten + (mpp * ga - map_ * gp) * inverse,
    )


def fit_tile(sums, weights, weight, offset, phase, atten, first):
    wre = wim = power = None
    for k in range(3):
        scale = lax.rsqrt(sums(k) * sums(3 + k) + EPSILON)
        cre = sums(6 + k) * scale
        cim = sums(9 + k) * scale
        square = cre * cre + cim * cim
        if k:
            wre = wre + cre * weights[k]
            wim = wim + cim * weights[k]
            power = power + square
        else:
            wre = cre * weights[k]
            wim = cim * weights[k]
            power = square
    for step in range(GAUSS_STEPS):
        now = moments(phase, atten) if step or first is None else first
        phase, atten = gauss_step(phase, atten, now, wre, wim, weight, offset)
    return phase, atten, power * (1.0 / 3.0)


def early_kernel(ground, ip, ie, mom, shares):
    ratios = [jnp.full((8, 128), ground[k], jnp.float32) for k in range(3)]
    weights = [1.0 / (1.0 + g) for g in ratios]
    weight = weights[0] * weights[0] + weights[1] * weights[1] + weights[2] * weights[2]
    offset = (
        ratios[0] * weights[0] * weights[0]
        + ratios[1] * weights[1] * weights[1]
        + ratios[2] * weights[2] * weights[2]
    )
    for n, value in enumerate((*weights, weight, offset)):
        shares[8 * n : 8 * n + 8] = value

    def tiles(i, carry):
        here = pl.ds(pl.multiple_of(8 * i, 8), 8)
        for b in range(4):
            cols = slice(128 * b, 128 * b + 128)
            for n, value in enumerate(moments(ip[here, cols], ie[here, cols])):
                mom[n, here, cols] = value
        return carry

    lax.fori_loop(0, H // 8, tiles, 0)


def split(value):
    first = value.astype(jnp.bfloat16)
    return first, (value - first.astype(jnp.float32)).astype(jnp.bfloat16)


def band(height, width, shift):
    up = lax.broadcasted_iota(jnp.int32, (height, width), 0) - shift
    across = lax.broadcasted_iota(jnp.int32, (height, width), 1)
    return (jnp.abs(up - across) <= RADIUS).astype(jnp.float32).astype(jnp.bfloat16)


def dot(a, b):
    return jnp.dot(a, b, preferred_element_type=jnp.float32)


def columns_kernel(rows, ext, shares, held, win, mom, mid, hi, lo):
    if INTERPRET:
        mom[:, 0:H] = held[:, 0:H]
    for n in range(6):
        here = slice(80 * n, 80 * n + 80)
        for b in range(4):
            cols = slice(128 * b, 128 * b + 128)
            hi[here, cols], lo[here, cols] = split(rows[here, cols])
    left = band(384, 256, 0)
    right = band(384, 256, 128)
    win[:, 0:256] = dot(hi[:, 0:384], left) + dot(lo[:, 0:384], left)
    win[:, 256:512] = dot(hi[:, 128:512], right) + dot(lo[:, 128:512], right)
    before = band(128, 128, 128)
    after = band(128, 128, -128)
    win[:, 512:640] = (dot(hi[:, 384:512], before) + dot(lo[:, 384:512], before)) + (
        dot(hi[:, 0:128], after) + dot(lo[:, 0:128], after)
    )
    for b in range(4):
        cols = slice(128 * b, 128 * b + 128)
        values = moments(ext[EH + H : EH + EH, cols], ext[2 * EH + H : 2 * EH + EH, cols])
        for n, value in enumerate(values):
            mom[n, H:EH, cols] = value
    weights = [shares[8 * n : 8 * n + 8] for n in range(3)]
    weight = shares[24:32]
    offset = shares[32:40]

    def fit(i, carry):
        here = pl.ds(pl.multiple_of(8 * i, 8), 8)
        for b in (1, 2):
            cols = slice(128 * b, 128 * b + 128)

            def sums(f):
                return win[pl.ds(pl.multiple_of(f * EH + 8 * i, 8), 8), cols]

            kz, phase, atten = (
                ext[pl.ds(pl.multiple_of(j * EH + 8 * i, 8), 8), cols] for j in range(3)
            )
            first = tuple(mom[n, here, cols] for n in range(5))
            phase, atten, power = fit_tile(sums, weights, weight, offset, phase, atten, first)
            spot = slice(128 * b - 128, 128 * b)
            mid[0, here, spot] = phase / kz
            mid[1, here, spot] = atten
            mid[2, here, spot] = power
        return carry

    lax.fori_loop(0, 5, fit, 0)


def around(field):
    return (
        pltpu.roll(field, 1, 0)
        + pltpu.roll(field, EH - 1, 0)
        + pltpu.roll(field, 1, 1)
        + pltpu.roll(field, EW - 1, 1)
    )


def make_fit_kernel(row_count, col_count, group):
    def kernel(
        win, ext, mom, shares, mid, far, near,
        depth, base, v0, v1, v2, sums,
        hi, lo, rim, wide, sem,
    ):
        lane = lax.broadcasted_iota(jnp.int32, (8, 128), 1)
        row = lax.axis_index("row")
        col = lax.axis_index("col")
        odd_col = lax.rem(col, 2) == 1
        places = strips()
        packs = []
        for v in range(PACK // 8):
            one = far[8 * v : 8 * v + 8]
            two = near[8 * v : 8 * v + 8]
            packs.append((jnp.where(odd_col, one, two), jnp.where(odd_col, two, one)))

        def halo_tile(strip):
            v, at, width = places[strip]
            low, high = packs[v]
            if at:
                low = pltpu.roll(low, 128 - at, 1)
            high = pltpu.roll(high, 128 - at - width, 1)
            return jnp.where(lane < width, low, jnp.where(lane >= 128 - width, high, 0.0))

        for n in range(6):
            halo = jnp.concatenate([halo_tile(10 * n + i) for i in range(10)], axis=0)
            hi[80 * n : 80 * n + 80], lo[80 * n : 80 * n + 80] = split(halo)
        for n, shift in enumerate((128, 0, -128)):
            part = band(128, 128, shift)
            rim[:, 128 * n : 128 * n + 128] = dot(hi[...], part) + dot(lo[...], part)
        rim_of = {0: 0, 4: 1, 3: 2}
        weights = [shares[8 * n : 8 * n + 8] for n in range(3)]
        weight = shares[24:32]
        offset = shares[32:40]

        def tile(f, i, b):
            at = f * EH + 8 * i
            value = win[at : at + 8, 128 * b : 128 * b + 128]
            return value + rim[at : at + 8, 128 * rim_of[b] : 128 * rim_of[b] + 128]

        def gathered(parts):
            out = jnp.zeros((8, 128), jnp.float32)
            for i, part in enumerate(parts):
                here = (lane >= 8 * i) & (lane < 8 * i + 8)
                out = jnp.where(here, pltpu.roll(part, 8 * i + 4, 1), out)
            return out

        def rim_sums(f):
            return gathered([tile(f, i, 4) for i in range(5)])

        kz, phase, atten = (
            gathered([halo_tile((FIELDS + j) * 5 + i) for i in range(5)]) for j in range(3)
        )
        phase, _, power = fit_tile(rim_sums, weights, weight, offset, phase, atten, None)
        phase = phase / kz
        for i in range(5):
            here = slice(8 * i, 8 * i + 8)
            wide[0, here, W:EW] = pltpu.roll(phase, 124 - 8 * i, 1)
            wide[2, here, W:EW] = pltpu.roll(power, 124 - 8 * i, 1)
        for i in range(5):
            here = slice(8 * i, 8 * i + 8)
            for b in (0, 3):
                cols = slice(128 * b, 128 * b + 128)
                kz, phase, atten = (
                    ext[j * EH + 8 * i : j * EH + 8 * i + 8, cols] for j in range(3)
                )
                first = tuple(mom[n, here, cols] for n in range(5))
                phase, atten, power = fit_tile(
                    lambda f: tile(f, i, b), weights, weight, offset, phase, atten, first
                )
                wide[0, here, cols] = phase / kz
                wide[1, here, cols] = atten
                wide[2, here, cols] = power
        for n in range(3):
            wide[n, :, 128:384] = mid[n]
        written = pltpu.make_async_copy(wide.at[1, pl.ds(0, H), pl.ds(0, W)], depth, sem)
        written.start()

        r = lax.broadcasted_iota(jnp.int32, (EH, EW), 0)
        c = lax.broadcasted_iota(jnp.int32, (EH, EW), 1)
        row_low = jnp.where(row == 0, EH - 4, EH)
        row_high = jnp.where(row == row_count - 1, H, EH - 4)
        col_low = jnp.where(col == 0, EW, EW - 4)
        col_high = jnp.where(col == col_count - 1, W, W + 4)
        row_bad = ((r >= row_high) & (r < EH - 4)) | (r >= row_low)
        col_bad = (c >= col_high) & (c < col_low)
        inside = jnp.logical_not(row_bad | col_bad)

        start = jnp.where(inside, wide[0], 0.0)
        confidence = wide[2] - 0.5
        base[...] = start[0:H, 0:W]
        first = jnp.where(inside, around(start) - 4.0 * start, 0.0)
        v0[...] = first[0:H, 0:W]

        def advance(field):
            return jnp.where(inside, (confidence * field - around(field)) * (1.0 / SCALE), 0.0)

        second = advance(first)
        v1[...] = second[0:H, 0:W]
        third = advance(second)
        v2[...] = third[0:H, 0:W]
        fourth = advance(third)
        a0, a1, a2, a3 = (x[0:H, 0:W] for x in (first, second, third, fourth))
        spots = lax.broadcasted_iota(jnp.int32, (1, 128), 1)
        line = jnp.zeros((1, 128), jnp.float32)
        for n, (p, q) in enumerate(((a0, a0), (a0, a1), (a1, a1), (a1, a2), (a2, a2), (a2, a3))):
            product = p * q
            total = jnp.sum(jnp.sum(product, axis=0, keepdims=True), axis=1, keepdims=True)
            line = jnp.where(spots == n, total, line)
        sums[...] = jnp.broadcast_to(line, (group, 128))
        written.wait()

    return kernel


def make_relay_kernel(out_group):
    def kernel(parts, out):
        out[...] = jnp.broadcast_to(jnp.sum(parts[...], axis=0, keepdims=True), (out_group, 128))

    return kernel


def form(p, q, b):
    total = None
    for i, x in enumerate(p):
        for j, y in enumerate(q):
            term = x * y * b[i + j]
            total = term if total is None else total + term
    return total


def final_kernel(parts, base, v0, v1, v2, heights):
    line = jnp.sum(parts[...], axis=0, keepdims=True)
    spots = lax.broadcasted_iota(jnp.int32, (1, 128), 1)
    b = [
        jnp.sum(jnp.where(spots == n, line, 0.0), axis=1, keepdims=True) for n in range(6)
    ]

    def times_a(p):
        out = [SCALE * p[0]]
        for low, high in zip(p[:-1], p[1:]):
            out.append(SCALE * (low + high))
        return out + [SCALE * p[-1]]

    one = jnp.ones((1, 1), jnp.float32)
    zero = jnp.zeros((1, 1), jnp.float32)
    residual = [one]
    direction = [one]
    answer = [zero, zero, zero]
    now = b[0]
    for iteration in range(3):
        image = times_a(direction)
        alpha = now / form(direction, image, b)
        for n, x in enumerate(direction):
            answer[n] = answer[n] + alpha * x
        if iteration == 2:
            break
        residual = [
            (residual[n] if n < len(residual) else 0.0) - alpha * x for n, x in enumerate(image)
        ]
        after = form(residual, residual, b)
        beta = after / now
        direction = [
            x + (beta * direction[n] if n < len(direction) else 0.0)
            for n, x in enumerate(residual)
        ]
        now = after
    heights[...] = base[...] + (answer[0] * v0[...] + (answer[1] * v1[...] + answer[2] * v2[...]))


def solution(mesh):
    row_count = mesh.shape["row"]
    col_count = mesh.shape["col"]
    near_count = 2 * col_count
    far_count = row_count // 2

    def index(r, c):
        return r * col_count + c

    near_groups = [
        [index(2 * y + core, c) for core in range(2) for c in range(col_count)] for y in range(far_count)
    ]
    far_groups = [
        [index(2 * y + core, c) for y in range(far_count)] for core in range(2) for c in range(col_count)
    ]
    both = ("row", "col")

    def swap(count, start):
        pairs = [(i, i + 1) for i in range(start, count - 1, 2)]
        return pairs + [(j, i) for i, j in pairs]

    def local(scatter_vectors, ground_ratio, wavenumber, phase, extinction):
        sv = scatter_vectors.reshape(FIELDS, H, W)
        inputs = (sv, wavenumber, phase, extinction)

        def edges(lifts, name):
            return call(
                edges_kernel(lifts),
                f32(SEND_ROWS, W),
                [ANY] * 4,
                [
                    pltpu.VMEM((FIELDS, 8, W), jnp.float32),
                    pltpu.VMEM((FIELDS, 8, W), jnp.float32),
                    pltpu.VMEM((3, 8, W), jnp.float32),
                    pltpu.SemaphoreType.DMA((5,)),
                ],
                name=name,
                far=range(4),
            )(*inputs)

        busy = pl.CostEstimate(flops=6000000, transcendentals=0, bytes_accessed=0)
        far = lax.ppermute(edges(0, "faredges"), "row", swap(row_count, 1))
        near = lax.ppermute(edges(1, "nearedges"), "row", swap(row_count, 0))
        mom, shares = call(
            early_kernel,
            (f32(5, EH, W), f32(40, 128)),
            [SM, VM, VM],
            name="early",
            kept=(1, 2),
            cost=busy,
        )(ground_ratio, phase, extinction)
        far, near, mom, shares = lax.optimization_barrier((far, near, mom, shares))
        rows, ext, left, right = call(
            rows_kernel,
            (f32(FIELDS * EH, W), f32(3 * EH, W), f32(PACK, 128), f32(PACK, 128)),
            [VM] * 6,
            [pltpu.VMEM((4, 88, 128), jnp.float32), pltpu.VMEM((4, 64, 128), jnp.float32)],
            name="rowsums",
            kept=range(6),
        )(*inputs, far, near)
        far = lax.ppermute(left, "col", swap(col_count, 1))
        near = lax.ppermute(right, "col", swap(col_count, 0))
        win, mom, mid = call(
            columns_kernel,
            (f32(FIELDS * EH, EW), f32(5, EH, W), f32(3, EH, 256)),
            [VM] * 4,
            [pltpu.VMEM((FIELDS * EH, W), jnp.bfloat16)] * 2,
            name="colsums",
            kept=range(4),
            aliases={3: 1},
            cost=busy,
        )(rows, ext, shares, mom)
        depth, base, v0, v1, v2, sums = call(
            make_fit_kernel(row_count, col_count, near_count),
            tuple(f32(H, W) for _ in range(5)) + (f32(near_count, 128),),
            [VM] * 7,
            [pltpu.VMEM((FIELDS * EH, 128), jnp.bfloat16)] * 2
            + [
                pltpu.VMEM((FIELDS * EH, 384), jnp.float32),
                pltpu.VMEM((3, EH, EW), jnp.float32),
                pltpu.SemaphoreType.DMA,
            ],
            name="fit",
            kept=range(7),
            leaves=(0,),
        )(win, ext, mom, shares, mid, far, near)
        parts = lax.all_to_all(
            sums.reshape(near_count, 1, 128), both, 0, 0, axis_index_groups=near_groups
        ).reshape(near_count, 128)
        parts = call(make_relay_kernel(far_count), f32(far_count, 128), [VM], name="relay", kept=(0,))(parts)
        parts = lax.all_to_all(
            parts.reshape(far_count, 1, 128), both, 0, 0, axis_index_groups=far_groups
        ).reshape(far_count, 128)
        heights = call(final_kernel, f32(H, W), [VM] * 5, name="final", kept=range(5), plain=(0,))(parts, base, v0, v1, v2)
        return heights, depth

    placed = (P(None, None, None, "row", "col"), P(), P("row", "col"), P("row", "col"), P("row", "col"))
    return jax.shard_map(
        local,
        mesh=mesh,
        in_specs=placed,
        out_specs=(P("row", "col"), P("row", "col")),
        check_vma=False,
    )
```

```python
import jax
import jax.numpy as jnp
from jax import lax
from jax.experimental import pallas as pl
from jax.experimental.pallas import tpu as pltpu
from jax.sharding import PartitionSpec as P

RADIUS = 9
LAYERS = 16
GAUSS_STEPS = 2
EPSILON = 1e-06
DAMPING = 0.002
SCALE = 4.5

H = 32
W = 512
EH = 40
EW = 640
FIELDS = 12
SIDE = RADIUS + 4
REST = SIDE - 8
REST_AT = FIELDS * 8
EXTRA_AT = REST_AT + FIELDS * REST
SEND_ROWS = EXTRA_AT + 3 * 4
GROUPS = 128 // SIDE
PACK = 8 * (-(-FIELDS * 5 // GROUPS) + 1)
VM = pl.BlockSpec(memory_space=pltpu.VMEM)
SM = pl.BlockSpec(memory_space=pltpu.SMEM)
ANY = pl.BlockSpec(memory_space=pl.ANY)
INTERPRET = False


def f32(*shape):
    return jax.ShapeDtypeStruct(shape, jnp.float32)


def call(kernel, outs, ins, scratch=(), name=None, kept=(), far=(), leaves=(), plain=(), aliases=None, cost=None):
    single = not isinstance(outs, tuple)
    shapes = (outs,) if single else outs
    specs = tuple(ANY if n in leaves else VM for n in range(len(shapes)))
    if not INTERPRET:
        shapes = tuple(
            x if n in leaves or n in plain else pltpu.VMEM(x.shape, x.dtype)
            for n, x in enumerate(shapes)
        )
    run = pl.pallas_call(
        kernel,
        out_shape=shapes[0] if single else shapes,
        in_specs=ins,
        out_specs=specs[0] if single else specs,
        scratch_shapes=scratch,
        name=name,
        interpret=INTERPRET,
        input_output_aliases=aliases or {},
        cost_estimate=cost,
        compiler_params=pltpu.CompilerParams(vmem_limit_bytes=16 << 20),
    )

    def apply(*args):
        if not INTERPRET:
            args = tuple(
                pltpu.with_memory_space_constraint(x, pltpu.VMEM if n in kept else pltpu.HBM)
                if n in kept or n in far
                else x
                for n, x in enumerate(args)
            )
        return run(*args)

    return apply


def pack_edges(low, out, tiles, rest, extra):
    bottom = low == 1
    for f in range(FIELDS):
        out[8 * f : 8 * f + 8] = tiles(f)
        at = REST_AT + REST * f
        value = rest(f)
        out[at : at + REST] = jnp.where(bottom, value[8 - REST : 8], value[0:REST])
    for j in range(3):
        at = EXTRA_AT + 4 * j
        value = extra(j)
        out[at : at + 4] = jnp.where(bottom, value[4:8], value[0:4])


def far_edges_kernel(sv, vw, ip, ie, out, tiles, rest, extra, sems):
    low = lax.rem(lax.axis_index("row"), 2)
    edge = pl.ds(pl.multiple_of(24 * low, 8), 8)
    inner = pl.ds(pl.multiple_of(8 + 8 * low, 8), 8)
    started = [
        pltpu.make_async_copy(sv.at[:, inner], rest, sems.at[0]),
        pltpu.make_async_copy(sv.at[:, edge], tiles, sems.at[1]),
    ]
    for j, ref in enumerate((vw, ip, ie)):
        started.append(pltpu.make_async_copy(ref.at[edge], extra.at[j], sems.at[2 + j]))
    for copy in started:
        copy.start()
    for copy in started:
        copy.wait()
    pack_edges(low, out, lambda f: tiles[f], lambda f: rest[f], lambda j: extra[j])


def near_edges_kernel(sv, vw, ip, ie, out):
    low = 1 - lax.rem(lax.axis_index("row"), 2)
    edge = pl.ds(pl.multiple_of(24 * low, 8), 8)
    inner = pl.ds(pl.multiple_of(8 + 8 * low, 8), 8)
    fields = (vw, ip, ie)
    pack_edges(low, out, lambda f: sv[f, edge], lambda f: sv[f, inner], lambda j: fields[j][edge])


def strips():
    out = []
    for n in range(FIELDS * 5):
        out.append((n // GROUPS, SIDE * (n % GROUPS), SIDE))
    for n in range(3 * 5):
        out.append((PACK // 8 - 1, 4 * n, 4))
    return out


def products(re1, im1, re2, im2):
    return (
        re1 * re1 + im1 * im1,
        re2 * re2 + im2 * im2,
        re1 * re2 + im1 * im2,
        re1 * im2 - im1 * re2,
    )


def own_rows_kernel(sv, rows, px, s4):
    sub = lax.broadcasted_iota(jnp.int32, (8, 128), 0)
    for j in range(4):
        px[j, 0:24] = jnp.zeros((24, 128), jnp.float32)
        px[j, 24 + H : 88] = jnp.zeros((64 - H, 128), jnp.float32)
    for k in range(3):

        def block(b, carry, k=k):
            cols = pl.ds(pl.multiple_of(b * 128, 128), 128)
            for j, value in enumerate(products(*(sv[q * 3 + k, :, cols] for q in range(4)))):
                px[j, 24 : 24 + H] = value
            for j in range(4):
                two = px[j, 7:79] + px[j, 8:80]
                four = two[0:64] + (px[j, 9:73] + px[j, 10:74])
                s4[j, 0:64] = four
                eight = four[0:56] + s4[j, 4:60]
                sixteen = eight[0:48] + eight[8:56]
                total = sixteen + two[16:64] + px[j, 25:73]
                at = (j * 3 + k) * EH
                rows[at : at + H, cols] = total[8:40]
                rows[at + H : at + EH, cols] = jnp.where(sub < 4, total[40:48], total[0:8])
            return carry

        lax.fori_loop(0, 4, block, 0)


HALO_SCRATCH = [pltpu.VMEM((4, 32, 128), jnp.float32)] * 4 + [pltpu.VMEM((4, 56, 128), jnp.float32)]


def halo_rows(far, near, blocks, scratch, put):
    odd_row = lax.rem(lax.axis_index("row"), 2) == 1
    sub = lax.broadcasted_iota(jnp.int32, (8, 128), 0)
    xa, xb, ta, tb, out = scratch
    zeros = jnp.zeros((16, 128), jnp.float32)
    for j in range(4):
        xa[j, 8:24] = zeros
        xa[j, 16:32] = zeros
        xb[j, 0:16] = zeros
        xb[j, 16:32] = zeros
        ta[j, 16:32] = zeros
        tb[j, 0:16] = zeros
        out[j, 0:16] = zeros
        out[j, 16:32] = zeros
        out[j, 24:40] = zeros

    def sides(at, size, cols):
        one = far[at : at + size, cols]
        two = near[at : at + size, cols]
        return jnp.where(odd_row, two, one), jnp.where(odd_row, one, two)

    for b in blocks:
        cols = slice(128 * b, 128 * b + 128)
        for k in range(3):
            tiles = [sides(8 * (q * 3 + k), 8, cols) for q in range(4)]
            rests = [sides(REST_AT + REST * (q * 3 + k), REST, cols) for q in range(4)]
            for j, value in enumerate(products(*(x[0] for x in rests))):
                xa[j, 0:REST] = value
            for j, value in enumerate(products(*(x[0] for x in tiles))):
                xa[j, REST:SIDE] = value
            for j, value in enumerate(products(*(x[1] for x in tiles))):
                xb[j, 16:24] = value
            for j, value in enumerate(products(*(x[1] for x in rests))):
                xb[j, 24 : 24 + REST] = value
            for j in range(4):
                four = (xa[j, 0:16] + xa[j, 1:17]) + (xa[j, 2:18] + xa[j, 3:19])
                ta[j, 0:16] = four
                total = (four + ta[j, 4:20]) + (ta[j, 8:24] + ta[j, 12:28])
                out[j, 8:24] = total
                four = (xb[j, 16:32] + xb[j, 15:31]) + (xb[j, 14:30] + xb[j, 13:29])
                tb[j, 16:32] = four
                total = (four + tb[j, 12:28]) + (tb[j, 8:24] + tb[j, 4:20])
                out[j, 39:55] = total
                put(
                    j * 3 + k,
                    b,
                    (
                        out[j, 12:20],
                        out[j, 20:28],
                        out[j, 32:40],
                        out[j, 40:48],
                        jnp.where(sub < 4, out[j, 48:56], out[j, 4:12]),
                    ),
                )


def sides_kernel(sums, vw, ip, ie, far, near, outer, ext, far_pack, near_pack, *scratch):
    lane = lax.broadcasted_iota(jnp.int32, (8, 128), 1)
    odd_row = lax.rem(lax.axis_index("row"), 2) == 1
    odd_col = lax.rem(lax.axis_index("col"), 2) == 1

    def put(f, b, parts):
        for i, part in enumerate(parts):
            at = f * EH + 8 * i
            spot = slice(0, 128) if b == 0 else slice(128, 256)
            outer[at : at + 8, spot] = sums[at : at + 8, 128 * b : 128 * b + 128] + part

    halo_rows(far, near, (0, 3), scratch, put)
    for j, ref in enumerate((vw, ip, ie)):
        at = EXTRA_AT + 4 * j
        one = far[at : at + 4]
        two = near[at : at + 4]
        ext[j * EH : j * EH + H] = ref[...]
        ext[j * EH + H : j * EH + H + 4] = jnp.where(odd_row, one, two)
        ext[j * EH + H + 4 : j * EH + EH] = jnp.where(odd_row, two, one)
    low = [jnp.zeros((8, 128), jnp.float32)] * (PACK // 8)
    high = list(low)
    for n, (v, at, width) in enumerate(strips()):
        here = (lane >= at) & (lane < at + width)
        if n < FIELDS * 5:
            first = outer[8 * n : 8 * n + 8, 0:128]
            last = outer[8 * n : 8 * n + 8, 128:256]
        else:
            top = 8 * n - FIELDS * EH
            first = ext[top : top + 8, 0:128]
            last = ext[top : top + 8, W - 128 : W]
        if at:
            first = pltpu.roll(first, at, 1)
        last = pltpu.roll(last, at + width, 1)
        low[v] = jnp.where(here, first, low[v])
        high[v] = jnp.where(here, last, high[v])
    for v in range(PACK // 8):
        far_pack[8 * v : 8 * v + 8] = jnp.where(odd_col, high[v], low[v])
        near_pack[8 * v : 8 * v + 8] = jnp.where(odd_col, low[v], high[v])


def sincos(x):
    turns = jnp.floor(x * 0.3183098861837907 + 0.5)
    y = x - turns * 3.140625
    y = y - turns * 9.67502593994140625e-4
    y = y - turns * 1.509957990978376432e-7
    odd = turns - 2.0 * jnp.floor(turns * 0.5)
    sign = 1.0 - 2.0 * odd
    z = y * y
    s = -2.3889859e-08
    s = s * z + 2.7525562e-06
    s = s * z - 1.9840874e-04
    s = s * z + 8.3333310e-03
    s = s * z - 1.6666667e-01
    s = y + y * z * s
    c = 2.0875723e-09
    c = c * z - 2.7557319e-07
    c = c * z + 2.4801587e-05
    c = c * z - 1.3888889e-03
    c = c * z + 4.1666667e-02
    c = 1.0 + z * (c * z - 0.5)
    return sign * s, sign * c


def cmul(ar, ai, br, bi):
    return ar * br - ai * bi, ar * bi + ai * br


def moments(phase, atten):
    half_s, half_c = sincos(phase * (0.5 / LAYERS))
    r = jnp.exp(atten * (1.0 / LAYERS))
    zr = r * (half_c * half_c - half_s * half_s)
    zi = r * (2.0 * half_c * half_s)
    n_sum, n_dep = 1.0 + r, r
    sr, si = 1.0 + zr, zi
    dr, di = zr, zi
    count = 2.0
    while count < LAYERS:
        r = r * r
        zr, zi = zr * zr - zi * zi, 2.0 * zr * zi
        n_dep = n_dep + r * (n_dep + count * n_sum)
        n_sum = n_sum + r * n_sum
        tr, ti = cmul(zr, zi, dr + count * sr, di + count * si)
        dr, di = dr + tr, di + ti
        tr, ti = cmul(zr, zi, sr, si)
        sr, si = sr + tr, si + ti
        count = 2.0 * count
    norm = 1.0 / n_sum
    half_c = half_c * norm
    half_s = half_s * norm
    real, imag = cmul(sr, si, half_c, half_s)
    dr, di = cmul(dr, di, half_c, half_s)
    step = 1.0 / LAYERS
    return (
        (n_dep * norm + 0.5) * step,
        real,
        imag,
        (dr + 0.5 * real) * step,
        (di + 0.5 * imag) * step,
    )


def gauss_step(phase, atten, mom, wre, wim, weight, offset):
    mean_depth, real_part, imag_part, depth_cos, depth_sin = mom
    ra = depth_cos - mean_depth * real_part
    rt = -depth_sin
    ia = depth_sin - mean_depth * imag_part
    it = depth_cos
    er = wre - weight * real_part - offset
    ei = wim - weight * imag_part
    maa = weight * (ra * ra + ia * ia) + DAMPING
    map_ = weight * (ra * rt + ia * it)
    mpp = weight * (rt * rt + it * it) + DAMPING
    ga = ra * er + ia * ei
    gp = rt * er + it * ei
    inverse = 1.0 / (maa * mpp - map_ * map_)
    return (
        phase + (maa * gp - map_ * ga) * inverse,
        atten + (mpp * ga - map_ * gp) * inverse,
    )


def fit_tile(sums, weights, weight, offset, phase, atten, first):
    wre = wim = power = None
    for k in range(3):
        scale = lax.rsqrt(sums(k) * sums(3 + k) + EPSILON)
        cre = sums(6 + k) * scale
        cim = sums(9 + k) * scale
        square = cre * cre + cim * cim
        if k:
            wre = wre + cre * weights[k]
            wim = wim + cim * weights[k]
            power = power + square
        else:
            wre = cre * weights[k]
            wim = cim * weights[k]
            power = square
    for step in range(GAUSS_STEPS):
        now = moments(phase, atten) if step or first is None else first
        phase, atten = gauss_step(phase, atten, now, wre, wim, weight, offset)
    return phase, atten, power * (1.0 / 3.0)


def early_kernel(ground, ip, ie, mom, shares):
    ratios = [jnp.full((8, 128), ground[k], jnp.float32) for k in range(3)]
    weights = [1.0 / (1.0 + g) for g in ratios]
    weight = weights[0] * weights[0] + weights[1] * weights[1] + weights[2] * weights[2]
    offset = (
        ratios[0] * weights[0] * weights[0]
        + ratios[1] * weights[1] * weights[1]
        + ratios[2] * weights[2] * weights[2]
    )
    for n, value in enumerate((*weights, weight, offset)):
        shares[8 * n : 8 * n + 8] = value

    def tiles(i, carry):
        here = pl.ds(pl.multiple_of(8 * i, 8), 8)
        for b in range(4):
            cols = slice(128 * b, 128 * b + 128)
            for n, value in enumerate(moments(ip[here, cols], ie[here, cols])):
                mom[n, here, cols] = value
        return carry

    lax.fori_loop(0, H // 8, tiles, 0)


def split(value):
    first = value.astype(jnp.bfloat16)
    return first, (value - first.astype(jnp.float32)).astype(jnp.bfloat16)


def band(height, width, shift):
    up = lax.broadcasted_iota(jnp.int32, (height, width), 0) - shift
    across = lax.broadcasted_iota(jnp.int32, (height, width), 1)
    return (jnp.abs(up - across) <= RADIUS).astype(jnp.float32).astype(jnp.bfloat16)


def dot(a, b):
    return jnp.dot(a, b, preferred_element_type=jnp.float32)


def columns_kernel(rows, outer, far, near, ext, shares, held, win, mom, mid, hi, lo, sums, *scratch):
    if INTERPRET:
        mom[:, 0:H] = held[:, 0:H]

    def put(f, b, parts):
        for i, part in enumerate(parts):
            at = f * EH + 8 * i
            spot = slice(128 * b - 128, 128 * b)
            sums[at : at + 8, spot] = rows[at : at + 8, 128 * b : 128 * b + 128] + part

    halo_rows(far, near, (1, 2), scratch, put)
    for n in range(6):
        here = slice(80 * n, 80 * n + 80)
        hi[here, 0:128], lo[here, 0:128] = split(outer[here, 0:128])
        hi[here, 384:512], lo[here, 384:512] = split(outer[here, 128:256])
        for b in range(2):
            cols = slice(128 * b + 128, 128 * b + 256)
            hi[here, cols], lo[here, cols] = split(sums[here, 128 * b : 128 * b + 128])
    left = band(384, 256, 0)
    right = band(384, 256, 128)
    win[:, 0:256] = dot(hi[:, 0:384], left) + dot(lo[:, 0:384], left)
    win[:, 256:512] = dot(hi[:, 128:512], right) + dot(lo[:, 128:512], right)
    before = band(128, 128, 128)
    after = band(128, 128, -128)
    win[:, 512:640] = (dot(hi[:, 384:512], before) + dot(lo[:, 384:512], before)) + (
        dot(hi[:, 0:128], after) + dot(lo[:, 0:128], after)
    )
    for b in range(4):
        cols = slice(128 * b, 128 * b + 128)
        values = moments(ext[EH + H : EH + EH, cols], ext[2 * EH + H : 2 * EH + EH, cols])
        for n, value in enumerate(values):
            mom[n, H:EH, cols] = value
    weights = [shares[8 * n : 8 * n + 8] for n in range(3)]
    weight = shares[24:32]
    offset = shares[32:40]

    def fit(i, carry):
        here = pl.ds(pl.multiple_of(8 * i, 8), 8)
        for b in (1, 2):
            cols = slice(128 * b, 128 * b + 128)

            def sums(f):
                return win[pl.ds(pl.multiple_of(f * EH + 8 * i, 8), 8), cols]

            kz, phase, atten = (
                ext[pl.ds(pl.multiple_of(j * EH + 8 * i, 8), 8), cols] for j in range(3)
            )
            first = tuple(mom[n, here, cols] for n in range(5))
            phase, atten, power = fit_tile(sums, weights, weight, offset, phase, atten, first)
            spot = slice(128 * b - 128, 128 * b)
            mid[0, here, spot] = phase / kz
            mid[1, here, spot] = atten
            mid[2, here, spot] = power
        return carry

    lax.fori_loop(0, 5, fit, 0)


def around(field):
    return (
        pltpu.roll(field, 1, 0)
        + pltpu.roll(field, EH - 1, 0)
        + pltpu.roll(field, 1, 1)
        + pltpu.roll(field, EW - 1, 1)
    )


def make_fit_kernel(row_count, col_count, group):
    def kernel(
        win, ext, mom, shares, mid, far, near,
        depth, base, v0, v1, v2, sums,
        hi, lo, rim, wide,
    ):
        lane = lax.broadcasted_iota(jnp.int32, (8, 128), 1)
        row = lax.axis_index("row")
        col = lax.axis_index("col")
        odd_col = lax.rem(col, 2) == 1
        places = strips()
        packs = []
        for v in range(PACK // 8):
            one = far[8 * v : 8 * v + 8]
            two = near[8 * v : 8 * v + 8]
            packs.append((jnp.where(odd_col, one, two), jnp.where(odd_col, two, one)))

        def halo_tile(strip):
            v, at, width = places[strip]
            low, high = packs[v]
            if at:
                low = pltpu.roll(low, 128 - at, 1)
            high = pltpu.roll(high, 128 - at - width, 1)
            return jnp.where(lane < width, low, jnp.where(lane >= 128 - width, high, 0.0))

        for n in range(6):
            halo = jnp.concatenate([halo_tile(10 * n + i) for i in range(10)], axis=0)
            hi[80 * n : 80 * n + 80], lo[80 * n : 80 * n + 80] = split(halo)
        for n, shift in enumerate((128, 0, -128)):
            part = band(128, 128, shift)
            rim[:, 128 * n : 128 * n + 128] = dot(hi[...], part) + dot(lo[...], part)
        rim_of = {0: 0, 4: 1, 3: 2}
        weights = [shares[8 * n : 8 * n + 8] for n in range(3)]
        weight = shares[24:32]
        offset = shares[32:40]

        def tile(f, i, b):
            at = f * EH + 8 * i
            value = win[at : at + 8, 128 * b : 128 * b + 128]
            return value + rim[at : at + 8, 128 * rim_of[b] : 128 * rim_of[b] + 128]

        def gathered(parts):
            out = jnp.zeros((8, 128), jnp.float32)
            for i, part in enumerate(parts):
                here = (lane >= 8 * i) & (lane < 8 * i + 8)
                out = jnp.where(here, pltpu.roll(part, 8 * i + 4, 1), out)
            return out

        def rim_sums(f):
            return gathered([tile(f, i, 4) for i in range(5)])

        kz, phase, atten = (
            gathered([halo_tile((FIELDS + j) * 5 + i) for i in range(5)]) for j in range(3)
        )
        phase, _, power = fit_tile(rim_sums, weights, weight, offset, phase, atten, None)
        phase = phase / kz
        for i in range(5):
            here = slice(8 * i, 8 * i + 8)
            wide[0, here, W:EW] = pltpu.roll(phase, 124 - 8 * i, 1)
            wide[2, here, W:EW] = pltpu.roll(power, 124 - 8 * i, 1)
        for i in range(5):
            here = slice(8 * i, 8 * i + 8)
            for b in (0, 3):
                cols = slice(128 * b, 128 * b + 128)
                kz, phase, atten = (
                    ext[j * EH + 8 * i : j * EH + 8 * i + 8, cols] for j in range(3)
                )
                first = tuple(mom[n, here, cols] for n in range(5))
                phase, atten, power = fit_tile(
                    lambda f: tile(f, i, b), weights, weight, offset, phase, atten, first
                )
                wide[0, here, cols] = phase / kz
                wide[1, here, cols] = atten
                wide[2, here, cols] = power
        for n in range(3):
            wide[n, :, 128:384] = mid[n]
        depth[...] = wide[1, 0:H, 0:W]

        r = lax.broadcasted_iota(jnp.int32, (EH, EW), 0)
        c = lax.broadcasted_iota(jnp.int32, (EH, EW), 1)
        row_low = jnp.where(row == 0, EH - 4, EH)
        row_high = jnp.where(row == row_count - 1, H, EH - 4)
        col_low = jnp.where(col == 0, EW, EW - 4)
        col_high = jnp.where(col == col_count - 1, W, W + 4)
        row_bad = ((r >= row_high) & (r < EH - 4)) | (r >= row_low)
        col_bad = (c >= col_high) & (c < col_low)
        inside = jnp.logical_not(row_bad | col_bad)

        start = jnp.where(inside, wide[0], 0.0)
        confidence = wide[2] - 0.5
        base[...] = start[0:H, 0:W]
        first = jnp.where(inside, around(start) - 4.0 * start, 0.0)
        v0[...] = first[0:H, 0:W]

        def advance(field):
            return jnp.where(inside, (confidence * field - around(field)) * (1.0 / SCALE), 0.0)

        second = advance(first)
        v1[...] = second[0:H, 0:W]
        third = advance(second)
        v2[...] = third[0:H, 0:W]
        fourth = advance(third)
        a0, a1, a2, a3 = (x[0:H, 0:W] for x in (first, second, third, fourth))
        spots = lax.broadcasted_iota(jnp.int32, (1, 128), 1)
        line = jnp.zeros((1, 128), jnp.float32)
        for n, (p, q) in enumerate(((a0, a0), (a0, a1), (a1, a1), (a1, a2), (a2, a2), (a2, a3))):
            product = p * q
            total = jnp.sum(jnp.sum(product, axis=0, keepdims=True), axis=1, keepdims=True)
            line = jnp.where(spots == n, total, line)
        sums[...] = jnp.broadcast_to(line, (group, 128))

    return kernel


def make_relay_kernel(out_group):
    def kernel(parts, out):
        out[...] = jnp.broadcast_to(jnp.sum(parts[...], axis=0, keepdims=True), (out_group, 128))

    return kernel


def form(p, q, b):
    total = None
    for i, x in enumerate(p):
        for j, y in enumerate(q):
            term = x * y * b[i + j]
            total = term if total is None else total + term
    return total


def final_kernel(parts, base, v0, v1, v2, fitted, heights, depth, result, sems):
    first = pltpu.make_async_copy(fitted, depth, sems.at[0])
    first.start()
    line = jnp.sum(parts[...], axis=0, keepdims=True)
    spots = lax.broadcasted_iota(jnp.int32, (1, 128), 1)
    b = [
        jnp.sum(jnp.where(spots == n, line, 0.0), axis=1, keepdims=True) for n in range(6)
    ]

    def times_a(p):
        out = [SCALE * p[0]]
        for low, high in zip(p[:-1], p[1:]):
            out.append(SCALE * (low + high))
        return out + [SCALE * p[-1]]

    one = jnp.ones((1, 1), jnp.float32)
    zero = jnp.zeros((1, 1), jnp.float32)
    residual = [one]
    direction = [one]
    answer = [zero, zero, zero]
    now = b[0]
    for iteration in range(3):
        image = times_a(direction)
        alpha = now / form(direction, image, b)
        for n, x in enumerate(direction):
            answer[n] = answer[n] + alpha * x
        if iteration == 2:
            break
        residual = [
            (residual[n] if n < len(residual) else 0.0) - alpha * x for n, x in enumerate(image)
        ]
        after = form(residual, residual, b)
        beta = after / now
        direction = [
            x + (beta * direction[n] if n < len(direction) else 0.0)
            for n, x in enumerate(residual)
        ]
        now = after
    result[...] = base[...] + (answer[0] * v0[...] + (answer[1] * v1[...] + answer[2] * v2[...]))
    second = pltpu.make_async_copy(result, heights, sems.at[1])
    second.start()
    first.wait()
    second.wait()


def solution(mesh):
    row_count = mesh.shape["row"]
    col_count = mesh.shape["col"]

    def index(r, c):
        return r * col_count + c

    ring = max(col_count // 8, 1)
    near_groups = [
        [index(2 * y + core, x + ring * z) for core in range(2) for z in range(col_count // ring)]
        for y in range(row_count // 2)
        for x in range(ring)
    ]
    far_groups = [
        [index(2 * y + core, x + ring * z) for y in range(row_count // 2) for x in range(ring)]
        for core in range(2)
        for z in range(col_count // ring)
    ]
    near_count = len(near_groups[0])
    far_count = len(far_groups[0])
    both = ("row", "col")

    def swap(count, start):
        pairs = [(i, i + 1) for i in range(start, count - 1, 2)]
        return pairs + [(j, i) for i, j in pairs]

    def local(scatter_vectors, ground_ratio, wavenumber, phase, extinction):
        sv = scatter_vectors.reshape(FIELDS, H, W)
        inputs = (sv, wavenumber, phase, extinction)

        tile = pltpu.VMEM((FIELDS, 8, W), jnp.float32)
        edge = call(
            far_edges_kernel,
            f32(SEND_ROWS, W),
            [ANY] * 4,
            [tile, tile, pltpu.VMEM((3, 8, W), jnp.float32), pltpu.SemaphoreType.DMA((5,))],
            name="faredges",
            far=range(4),
        )(*inputs)
        busy = pl.CostEstimate(flops=6000000, transcendentals=0, bytes_accessed=0)
        far = lax.ppermute(edge, "row", swap(row_count, 1))
        edge = call(near_edges_kernel, f32(SEND_ROWS, W), [VM] * 4, name="nearedges", kept=range(4))(*inputs)
        near = lax.ppermute(edge, "row", swap(row_count, 0))
        mom, shares = call(
            early_kernel,
            (f32(5, EH, W), f32(40, 128)),
            [SM, VM, VM],
            name="early",
            kept=(1, 2),
            cost=busy,
        )(ground_ratio, phase, extinction)
        rows = call(
            own_rows_kernel,
            f32(FIELDS * EH, W),
            [VM],
            [pltpu.VMEM((4, 88, 128), jnp.float32), pltpu.VMEM((4, 64, 128), jnp.float32)],
            name="ownrows",
            kept=(0,),
            cost=busy,
        )(sv)
        far, near, mom, shares, rows = lax.optimization_barrier((far, near, mom, shares, rows))
        outer, ext, left, right = call(
            sides_kernel,
            (f32(FIELDS * EH, 256), f32(3 * EH, W), f32(PACK, 128), f32(PACK, 128)),
            [VM] * 6,
            HALO_SCRATCH,
            name="sides",
            kept=range(6),
        )(rows, wavenumber, phase, extinction, far, near)
        far_side = lax.ppermute(left, "col", swap(col_count, 1))
        near_side = lax.ppermute(right, "col", swap(col_count, 0))
        win, mom, mid = call(
            columns_kernel,
            (f32(FIELDS * EH, EW), f32(5, EH, W), f32(3, EH, 256)),
            [VM] * 7,
            [pltpu.VMEM((FIELDS * EH, W), jnp.bfloat16)] * 2
            + [pltpu.VMEM((FIELDS * EH, 256), jnp.float32)]
            + HALO_SCRATCH,
            name="colsums",
            kept=range(7),
            aliases={6: 1},
            cost=busy,
        )(rows, outer, far, near, ext, shares, mom)
        depth, base, v0, v1, v2, sums = call(
            make_fit_kernel(row_count, col_count, near_count),
            tuple(f32(H, W) for _ in range(5)) + (f32(near_count, 128),),
            [VM] * 7,
            [pltpu.VMEM((FIELDS * EH, 128), jnp.bfloat16)] * 2
            + [
                pltpu.VMEM((FIELDS * EH, 384), jnp.float32),
                pltpu.VMEM((3, EH, EW), jnp.float32),
            ],
            name="fit",
            kept=range(7),
        )(win, ext, mom, shares, mid, far_side, near_side)
        parts = lax.all_to_all(
            sums.reshape(near_count, 1, 128), both, 0, 0, axis_index_groups=near_groups
        ).reshape(near_count, 128)
        parts = call(make_relay_kernel(far_count), f32(far_count, 128), [VM], name="relay", kept=(0,))(parts)
        parts = lax.all_to_all(
            parts.reshape(far_count, 1, 128), both, 0, 0, axis_index_groups=far_groups
        ).reshape(far_count, 128)
        return call(
            final_kernel,
            (f32(H, W), f32(H, W)),
            [VM] * 6,
            [pltpu.VMEM((H, W), jnp.float32), pltpu.SemaphoreType.DMA((2,))],
            name="final",
            kept=range(6),
            leaves=(0, 1),
        )(parts, base, v0, v1, v2, depth)

    placed = (P(None, None, None, "row", "col"), P(), P("row", "col"), P("row", "col"), P("row", "col"))
    return jax.shard_map(
        local,
        mesh=mesh,
        in_specs=placed,
        out_specs=(P("row", "col"), P("row", "col")),
        check_vma=False,
    )
```

```python
import jax
import jax.numpy as jnp
from jax import lax
from jax.experimental import pallas as pl
from jax.experimental.pallas import tpu as pltpu
from jax.sharding import PartitionSpec as P

RADIUS = 9
LAYERS = 16
GAUSS_STEPS = 2
EPSILON = 1e-06
DAMPING = 0.002
SCALE = 4.5

H = 32
W = 512
EH = 40
EW = 640
FIELDS = 12
SIDE = RADIUS + 4
REST = SIDE - 8
SENT = 9
REST_AT = SENT * 8
EXTRA_AT = REST_AT + SENT * REST
SEND_ROWS = EXTRA_AT + 3 * 4
GROUPS = 128 // SIDE
PACK = 8 * (-(-FIELDS * 5 // GROUPS) + 1)
VM = pl.BlockSpec(memory_space=pltpu.VMEM)
SM = pl.BlockSpec(memory_space=pltpu.SMEM)
ANY = pl.BlockSpec(memory_space=pl.ANY)
INTERPRET = False


def f32(*shape):
    return jax.ShapeDtypeStruct(shape, jnp.float32)


def call(kernel, outs, ins, scratch=(), name=None, kept=(), far=(), leaves=(), plain=(), aliases=None, cost=None):
    single = not isinstance(outs, tuple)
    shapes = (outs,) if single else outs
    specs = tuple(ANY if n in leaves else VM for n in range(len(shapes)))
    if not INTERPRET:
        shapes = tuple(
            x if n in leaves or n in plain else pltpu.VMEM(x.shape, x.dtype)
            for n, x in enumerate(shapes)
        )
    run = pl.pallas_call(
        kernel,
        out_shape=shapes[0] if single else shapes,
        in_specs=ins,
        out_specs=specs[0] if single else specs,
        scratch_shapes=scratch,
        name=name,
        interpret=INTERPRET,
        input_output_aliases=aliases or {},
        cost_estimate=cost,
        compiler_params=pltpu.CompilerParams(vmem_limit_bytes=16 << 20),
    )

    def apply(*args):
        if not INTERPRET:
            args = tuple(
                pltpu.with_memory_space_constraint(x, pltpu.VMEM if n in kept else pltpu.HBM)
                if n in kept or n in far
                else x
                for n, x in enumerate(args)
            )
        return run(*args)

    return apply


def turned(re1, im1, re2, im2):
    square = re1 * re1 + im1 * im1
    inverse = lax.rsqrt(square)
    none = square == 0.0
    cos = jnp.where(none, 1.0, re1 * inverse)
    sin = jnp.where(none, 0.0, im1 * inverse)
    return re1 * cos + im1 * sin, re2 * cos + im2 * sin, im2 * cos - re2 * sin


def pack_edges(low, out, tiles, rest, extra):
    bottom = low == 1
    for k in range(3):
        for m, value in enumerate(turned(*(tiles(q * 3 + k) for q in range(4)))):
            at = 8 * (m * 3 + k)
            out[at : at + 8] = value
        for m, value in enumerate(turned(*(rest(q * 3 + k) for q in range(4)))):
            at = REST_AT + REST * (m * 3 + k)
            out[at : at + REST] = jnp.where(bottom, value[8 - REST : 8], value[0:REST])
    for j in range(3):
        at = EXTRA_AT + 4 * j
        value = extra(j)
        out[at : at + 4] = jnp.where(bottom, value[4:8], value[0:4])


def far_edges_kernel(sv, vw, ip, ie, out, tiles, rest, extra, sems):
    low = lax.rem(lax.axis_index("row"), 2)
    edge = pl.ds(pl.multiple_of(24 * low, 8), 8)
    inner = pl.ds(pl.multiple_of(8 + 8 * low, 8), 8)
    started = [
        pltpu.make_async_copy(sv.at[:, inner], rest, sems.at[0]),
        pltpu.make_async_copy(sv.at[:, edge], tiles, sems.at[1]),
    ]
    for j, ref in enumerate((vw, ip, ie)):
        started.append(pltpu.make_async_copy(ref.at[edge], extra.at[j], sems.at[2 + j]))
    for copy in started:
        copy.start()
    for copy in started:
        copy.wait()
    pack_edges(low, out, lambda f: tiles[f], lambda f: rest[f], lambda j: extra[j])


def near_edges_kernel(sv, vw, ip, ie, out):
    low = 1 - lax.rem(lax.axis_index("row"), 2)
    edge = pl.ds(pl.multiple_of(24 * low, 8), 8)
    inner = pl.ds(pl.multiple_of(8 + 8 * low, 8), 8)
    fields = (vw, ip, ie)
    pack_edges(low, out, lambda f: sv[f, edge], lambda f: sv[f, inner], lambda j: fields[j][edge])


def strips():
    out = []
    for n in range(FIELDS * 5):
        out.append((n // GROUPS, SIDE * (n % GROUPS), SIDE))
    for n in range(3 * 5):
        out.append((PACK // 8 - 1, 4 * n, 4))
    return out


def products(re1, im1, re2, im2):
    return (
        re1 * re1 + im1 * im1,
        re2 * re2 + im2 * im2,
        re1 * re2 + im1 * im2,
        re1 * im2 - im1 * re2,
    )


def turned_products(one, re2, im2):
    return one * one, re2 * re2 + im2 * im2, one * re2, one * im2


def own_rows_kernel(sv, rows, px, s4):
    sub = lax.broadcasted_iota(jnp.int32, (8, 128), 0)
    for j in range(4):
        px[j, 0:24] = jnp.zeros((24, 128), jnp.float32)
        px[j, 24 + H : 88] = jnp.zeros((64 - H, 128), jnp.float32)
    for k in range(3):

        def block(b, carry, k=k):
            cols = pl.ds(pl.multiple_of(b * 128, 128), 128)
            for j, value in enumerate(products(*(sv[q * 3 + k, :, cols] for q in range(4)))):
                px[j, 24 : 24 + H] = value
            for j in range(4):
                two = px[j, 7:79] + px[j, 8:80]
                four = two[0:64] + (px[j, 9:73] + px[j, 10:74])
                s4[j, 0:64] = four
                eight = four[0:56] + s4[j, 4:60]
                sixteen = eight[0:48] + eight[8:56]
                total = sixteen + two[16:64] + px[j, 25:73]
                at = (j * 3 + k) * EH
                rows[at : at + H, cols] = total[8:40]
                rows[at + H : at + EH, cols] = jnp.where(sub < 4, total[40:48], total[0:8])
            return carry

        lax.fori_loop(0, 4, block, 0)


HALO_SCRATCH = [pltpu.VMEM((4, 32, 128), jnp.float32)] * 4 + [pltpu.VMEM((4, 56, 128), jnp.float32)]


def halo_rows(far, near, blocks, scratch, put):
    odd_row = lax.rem(lax.axis_index("row"), 2) == 1
    sub = lax.broadcasted_iota(jnp.int32, (8, 128), 0)
    xa, xb, ta, tb, out = scratch
    zeros = jnp.zeros((16, 128), jnp.float32)
    for j in range(4):
        xa[j, 8:24] = zeros
        xa[j, 16:32] = zeros
        xb[j, 0:16] = zeros
        xb[j, 16:32] = zeros
        ta[j, 16:32] = zeros
        tb[j, 0:16] = zeros
        out[j, 0:16] = zeros
        out[j, 16:32] = zeros
        out[j, 24:40] = zeros

    def sides(at, size, cols):
        one = far[at : at + size, cols]
        two = near[at : at + size, cols]
        return jnp.where(odd_row, two, one), jnp.where(odd_row, one, two)

    for b in blocks:
        cols = slice(128 * b, 128 * b + 128)
        for k in range(3):
            tiles = [sides(8 * (m * 3 + k), 8, cols) for m in range(3)]
            rests = [sides(REST_AT + REST * (m * 3 + k), REST, cols) for m in range(3)]
            for j, value in enumerate(turned_products(*(x[0] for x in rests))):
                xa[j, 0:REST] = value
            for j, value in enumerate(turned_products(*(x[0] for x in tiles))):
                xa[j, REST:SIDE] = value
            for j, value in enumerate(turned_products(*(x[1] for x in tiles))):
                xb[j, 16:24] = value
            for j, value in enumerate(turned_products(*(x[1] for x in rests))):
                xb[j, 24 : 24 + REST] = value
            for j in range(4):
                four = (xa[j, 0:16] + xa[j, 1:17]) + (xa[j, 2:18] + xa[j, 3:19])
                ta[j, 0:16] = four
                total = (four + ta[j, 4:20]) + (ta[j, 8:24] + ta[j, 12:28])
                out[j, 8:24] = total
                four = (xb[j, 16:32] + xb[j, 15:31]) + (xb[j, 14:30] + xb[j, 13:29])
                tb[j, 16:32] = four
                total = (four + tb[j, 12:28]) + (tb[j, 8:24] + tb[j, 4:20])
                out[j, 39:55] = total
                put(
                    j * 3 + k,
                    b,
                    (
                        out[j, 12:20],
                        out[j, 20:28],
                        out[j, 32:40],
                        out[j, 40:48],
                        jnp.where(sub < 4, out[j, 48:56], out[j, 4:12]),
                    ),
                )


def sides_kernel(sums, vw, ip, ie, far, near, outer, ext, far_pack, near_pack, *scratch):
    lane = lax.broadcasted_iota(jnp.int32, (8, 128), 1)
    odd_row = lax.rem(lax.axis_index("row"), 2) == 1
    odd_col = lax.rem(lax.axis_index("col"), 2) == 1

    def put(f, b, parts):
        for i, part in enumerate(parts):
            at = f * EH + 8 * i
            spot = slice(0, 128) if b == 0 else slice(128, 256)
            outer[at : at + 8, spot] = sums[at : at + 8, 128 * b : 128 * b + 128] + part

    halo_rows(far, near, (0, 3), scratch, put)
    for j, ref in enumerate((vw, ip, ie)):
        at = EXTRA_AT + 4 * j
        one = far[at : at + 4]
        two = near[at : at + 4]
        ext[j * EH : j * EH + H] = ref[...]
        ext[j * EH + H : j * EH + H + 4] = jnp.where(odd_row, one, two)
        ext[j * EH + H + 4 : j * EH + EH] = jnp.where(odd_row, two, one)
    low = [jnp.zeros((8, 128), jnp.float32)] * (PACK // 8)
    high = list(low)
    for n, (v, at, width) in enumerate(strips()):
        here = (lane >= at) & (lane < at + width)
        if n < FIELDS * 5:
            first = outer[8 * n : 8 * n + 8, 0:128]
            last = outer[8 * n : 8 * n + 8, 128:256]
        else:
            top = 8 * n - FIELDS * EH
            first = ext[top : top + 8, 0:128]
            last = ext[top : top + 8, W - 128 : W]
        if at:
            first = pltpu.roll(first, at, 1)
        last = pltpu.roll(last, at + width, 1)
        low[v] = jnp.where(here, first, low[v])
        high[v] = jnp.where(here, last, high[v])
    for v in range(PACK // 8):
        far_pack[8 * v : 8 * v + 8] = jnp.where(odd_col, high[v], low[v])
        near_pack[8 * v : 8 * v + 8] = jnp.where(odd_col, low[v], high[v])


def sincos(x):
    turns = jnp.floor(x * 0.3183098861837907 + 0.5)
    y = x - turns * 3.140625
    y = y - turns * 9.67502593994140625e-4
    y = y - turns * 1.509957990978376432e-7
    odd = turns - 2.0 * jnp.floor(turns * 0.5)
    sign = 1.0 - 2.0 * odd
    z = y * y
    s = -2.3889859e-08
    s = s * z + 2.7525562e-06
    s = s * z - 1.9840874e-04
    s = s * z + 8.3333310e-03
    s = s * z - 1.6666667e-01
    s = y + y * z * s
    c = 2.0875723e-09
    c = c * z - 2.7557319e-07
    c = c * z + 2.4801587e-05
    c = c * z - 1.3888889e-03
    c = c * z + 4.1666667e-02
    c = 1.0 + z * (c * z - 0.5)
    return sign * s, sign * c


def cmul(ar, ai, br, bi):
    return ar * br - ai * bi, ar * bi + ai * br


def moments(phase, atten):
    half_s, half_c = sincos(phase * (0.5 / LAYERS))
    r = jnp.exp(atten * (1.0 / LAYERS))
    zr = r * (half_c * half_c - half_s * half_s)
    zi = r * (2.0 * half_c * half_s)
    n_sum, n_dep = 1.0 + r, r
    sr, si = 1.0 + zr, zi
    dr, di = zr, zi
    count = 2.0
    while count < LAYERS:
        r = r * r
        zr, zi = zr * zr - zi * zi, 2.0 * zr * zi
        n_dep = n_dep + r * (n_dep + count * n_sum)
        n_sum = n_sum + r * n_sum
        tr, ti = cmul(zr, zi, dr + count * sr, di + count * si)
        dr, di = dr + tr, di + ti
        tr, ti = cmul(zr, zi, sr, si)
        sr, si = sr + tr, si + ti
        count = 2.0 * count
    norm = 1.0 / n_sum
    half_c = half_c * norm
    half_s = half_s * norm
    real, imag = cmul(sr, si, half_c, half_s)
    dr, di = cmul(dr, di, half_c, half_s)
    step = 1.0 / LAYERS
    return (
        (n_dep * norm + 0.5) * step,
        real,
        imag,
        (dr + 0.5 * real) * step,
        (di + 0.5 * imag) * step,
    )


def gauss_step(phase, atten, mom, wre, wim, weight, offset):
    mean_depth, real_part, imag_part, depth_cos, depth_sin = mom
    ra = depth_cos - mean_depth * real_part
    rt = -depth_sin
    ia = depth_sin - mean_depth * imag_part
    it = depth_cos
    er = wre - weight * real_part - offset
    ei = wim - weight * imag_part
    maa = weight * (ra * ra + ia * ia) + DAMPING
    map_ = weight * (ra * rt + ia * it)
    mpp = weight * (rt * rt + it * it) + DAMPING
    ga = ra * er + ia * ei
    gp = rt * er + it * ei
    inverse = 1.0 / (maa * mpp - map_ * map_)
    return (
        phase + (maa * gp - map_ * ga) * inverse,
        atten + (mpp * ga - map_ * gp) * inverse,
    )


def fit_tile(sums, weights, weight, offset, phase, atten, first):
    wre = wim = power = None
    for k in range(3):
        scale = lax.rsqrt(sums(k) * sums(3 + k) + EPSILON)
        cre = sums(6 + k) * scale
        cim = sums(9 + k) * scale
        square = cre * cre + cim * cim
        if k:
            wre = wre + cre * weights[k]
            wim = wim + cim * weights[k]
            power = power + square
        else:
            wre = cre * weights[k]
            wim = cim * weights[k]
            power = square
    for step in range(GAUSS_STEPS):
        now = moments(phase, atten) if step or first is None else first
        phase, atten = gauss_step(phase, atten, now, wre, wim, weight, offset)
    return phase, atten, power * (1.0 / 3.0)


def early_kernel(ground, ip, ie, mom, shares):
    ratios = [jnp.full((8, 128), ground[k], jnp.float32) for k in range(3)]
    weights = [1.0 / (1.0 + g) for g in ratios]
    weight = weights[0] * weights[0] + weights[1] * weights[1] + weights[2] * weights[2]
    offset = (
        ratios[0] * weights[0] * weights[0]
        + ratios[1] * weights[1] * weights[1]
        + ratios[2] * weights[2] * weights[2]
    )
    for n, value in enumerate((*weights, weight, offset)):
        shares[8 * n : 8 * n + 8] = value

    def tiles(i, carry):
        here = pl.ds(pl.multiple_of(8 * i, 8), 8)
        for b in range(4):
            cols = slice(128 * b, 128 * b + 128)
            for n, value in enumerate(moments(ip[here, cols], ie[here, cols])):
                mom[n, here, cols] = value
        return carry

    lax.fori_loop(0, H // 8, tiles, 0)


def split(value):
    first = value.astype(jnp.bfloat16)
    return first, (value - first.astype(jnp.float32)).astype(jnp.bfloat16)


def band(height, width, shift):
    up = lax.broadcasted_iota(jnp.int32, (height, width), 0) - shift
    across = lax.broadcasted_iota(jnp.int32, (height, width), 1)
    return (jnp.abs(up - across) <= RADIUS).astype(jnp.float32).astype(jnp.bfloat16)


def dot(a, b):
    return jnp.dot(a, b, preferred_element_type=jnp.float32)


def columns_kernel(rows, outer, far, near, ext, shares, held, win, mom, mid, hi, lo, sums, *scratch):
    if INTERPRET:
        mom[:, 0:H] = held[:, 0:H]

    def put(f, b, parts):
        for i, part in enumerate(parts):
            at = f * EH + 8 * i
            spot = slice(128 * b - 128, 128 * b)
            sums[at : at + 8, spot] = rows[at : at + 8, 128 * b : 128 * b + 128] + part

    halo_rows(far, near, (1, 2), scratch, put)
    for n in range(6):
        here = slice(80 * n, 80 * n + 80)
        hi[here, 0:128], lo[here, 0:128] = split(outer[here, 0:128])
        hi[here, 384:512], lo[here, 384:512] = split(outer[here, 128:256])
        for b in range(2):
            cols = slice(128 * b + 128, 128 * b + 256)
            hi[here, cols], lo[here, cols] = split(sums[here, 128 * b : 128 * b + 128])
    left = band(384, 256, 0)
    right = band(384, 256, 128)
    win[:, 0:256] = dot(hi[:, 0:384], left) + dot(lo[:, 0:384], left)
    win[:, 256:512] = dot(hi[:, 128:512], right) + dot(lo[:, 128:512], right)
    before = band(128, 128, 128)
    after = band(128, 128, -128)
    win[:, 512:640] = (dot(hi[:, 384:512], before) + dot(lo[:, 384:512], before)) + (
        dot(hi[:, 0:128], after) + dot(lo[:, 0:128], after)
    )
    for b in range(4):
        cols = slice(128 * b, 128 * b + 128)
        values = moments(ext[EH + H : EH + EH, cols], ext[2 * EH + H : 2 * EH + EH, cols])
        for n, value in enumerate(values):
            mom[n, H:EH, cols] = value
    weights = [shares[8 * n : 8 * n + 8] for n in range(3)]
    weight = shares[24:32]
    offset = shares[32:40]

    def fit(i, carry):
        here = pl.ds(pl.multiple_of(8 * i, 8), 8)
        for b in (1, 2):
            cols = slice(128 * b, 128 * b + 128)

            def sums(f):
                return win[pl.ds(pl.multiple_of(f * EH + 8 * i, 8), 8), cols]

            kz, phase, atten = (
                ext[pl.ds(pl.multiple_of(j * EH + 8 * i, 8), 8), cols] for j in range(3)
            )
            first = tuple(mom[n, here, cols] for n in range(5))
            phase, atten, power = fit_tile(sums, weights, weight, offset, phase, atten, first)
            spot = slice(128 * b - 128, 128 * b)
            mid[0, here, spot] = phase / kz
            mid[1, here, spot] = atten
            mid[2, here, spot] = power
        return carry

    lax.fori_loop(0, 5, fit, 0)


def around(field):
    return (
        pltpu.roll(field, 1, 0)
        + pltpu.roll(field, EH - 1, 0)
        + pltpu.roll(field, 1, 1)
        + pltpu.roll(field, EW - 1, 1)
    )


def make_fit_kernel(row_count, col_count, group):
    def kernel(
        win, ext, mom, shares, mid, far, near,
        depth, base, v0, v1, v2, sums,
        hi, lo, rim, wide,
    ):
        lane = lax.broadcasted_iota(jnp.int32, (8, 128), 1)
        row = lax.axis_index("row")
        col = lax.axis_index("col")
        odd_col = lax.rem(col, 2) == 1
        places = strips()
        packs = []
        for v in range(PACK // 8):
            one = far[8 * v : 8 * v + 8]
            two = near[8 * v : 8 * v + 8]
            packs.append((jnp.where(odd_col, one, two), jnp.where(odd_col, two, one)))

        def halo_tile(strip):
            v, at, width = places[strip]
            low, high = packs[v]
            if at:
                low = pltpu.roll(low, 128 - at, 1)
            high = pltpu.roll(high, 128 - at - width, 1)
            return jnp.where(lane < width, low, jnp.where(lane >= 128 - width, high, 0.0))

        for n in range(6):
            halo = jnp.concatenate([halo_tile(10 * n + i) for i in range(10)], axis=0)
            hi[80 * n : 80 * n + 80], lo[80 * n : 80 * n + 80] = split(halo)
        for n, shift in enumerate((128, 0, -128)):
            part = band(128, 128, shift)
            rim[:, 128 * n : 128 * n + 128] = dot(hi[...], part) + dot(lo[...], part)
        rim_of = {0: 0, 4: 1, 3: 2}
        weights = [shares[8 * n : 8 * n + 8] for n in range(3)]
        weight = shares[24:32]
        offset = shares[32:40]

        def tile(f, i, b):
            at = f * EH + 8 * i
            value = win[at : at + 8, 128 * b : 128 * b + 128]
            return value + rim[at : at + 8, 128 * rim_of[b] : 128 * rim_of[b] + 128]

        def gathered(parts):
            out = jnp.zeros((8, 128), jnp.float32)
            for i, part in enumerate(parts):
                here = (lane >= 8 * i) & (lane < 8 * i + 8)
                out = jnp.where(here, pltpu.roll(part, 8 * i + 4, 1), out)
            return out

        def rim_sums(f):
            return gathered([tile(f, i, 4) for i in range(5)])

        kz, phase, atten = (
            gathered([halo_tile((FIELDS + j) * 5 + i) for i in range(5)]) for j in range(3)
        )
        phase, _, power = fit_tile(rim_sums, weights, weight, offset, phase, atten, None)
        phase = phase / kz
        for i in range(5):
            here = slice(8 * i, 8 * i + 8)
            wide[0, here, W:EW] = pltpu.roll(phase, 124 - 8 * i, 1)
            wide[2, here, W:EW] = pltpu.roll(power, 124 - 8 * i, 1)
        for i in range(5):
            here = slice(8 * i, 8 * i + 8)
            for b in (0, 3):
                cols = slice(128 * b, 128 * b + 128)
                kz, phase, atten = (
                    ext[j * EH + 8 * i : j * EH + 8 * i + 8, cols] for j in range(3)
                )
                first = tuple(mom[n, here, cols] for n in range(5))
                phase, atten, power = fit_tile(
                    lambda f: tile(f, i, b), weights, weight, offset, phase, atten, first
                )
                wide[0, here, cols] = phase / kz
                wide[1, here, cols] = atten
                wide[2, here, cols] = power
        for n in range(3):
            wide[n, :, 128:384] = mid[n]
        depth[...] = wide[1, 0:H, 0:W]

        r = lax.broadcasted_iota(jnp.int32, (EH, EW), 0)
        c = lax.broadcasted_iota(jnp.int32, (EH, EW), 1)
        row_low = jnp.where(row == 0, EH - 4, EH)
        row_high = jnp.where(row == row_count - 1, H, EH - 4)
        col_low = jnp.where(col == 0, EW, EW - 4)
        col_high = jnp.where(col == col_count - 1, W, W + 4)
        row_bad = ((r >= row_high) & (r < EH - 4)) | (r >= row_low)
        col_bad = (c >= col_high) & (c < col_low)
        inside = jnp.logical_not(row_bad | col_bad)

        start = jnp.where(inside, wide[0], 0.0)
        confidence = wide[2] - 0.5
        base[...] = start[0:H, 0:W]
        first = jnp.where(inside, around(start) - 4.0 * start, 0.0)
        v0[...] = first[0:H, 0:W]

        def advance(field):
            return jnp.where(inside, (confidence * field - around(field)) * (1.0 / SCALE), 0.0)

        second = advance(first)
        v1[...] = second[0:H, 0:W]
        third = advance(second)
        v2[...] = third[0:H, 0:W]
        fourth = advance(third)
        a0, a1, a2, a3 = (x[0:H, 0:W] for x in (first, second, third, fourth))
        spots = lax.broadcasted_iota(jnp.int32, (1, 128), 1)
        line = jnp.zeros((1, 128), jnp.float32)
        for n, (p, q) in enumerate(((a0, a0), (a0, a1), (a1, a1), (a1, a2), (a2, a2), (a2, a3))):
            product = p * q
            total = jnp.sum(jnp.sum(product, axis=0, keepdims=True), axis=1, keepdims=True)
            line = jnp.where(spots == n, total, line)
        sums[...] = jnp.broadcast_to(line, (group, 128))

    return kernel


def make_relay_kernel(out_group):
    def kernel(parts, out):
        out[...] = jnp.broadcast_to(jnp.sum(parts[...], axis=0, keepdims=True), (out_group, 128))

    return kernel


def form(p, q, b):
    total = None
    for i, x in enumerate(p):
        for j, y in enumerate(q):
            term = x * y * b[i + j]
            total = term if total is None else total + term
    return total


def final_kernel(parts, base, v0, v1, v2, fitted, heights, depth, result, sems):
    first = pltpu.make_async_copy(fitted, depth, sems.at[0])
    first.start()
    line = jnp.sum(parts[...], axis=0, keepdims=True)
    spots = lax.broadcasted_iota(jnp.int32, (1, 128), 1)
    b = [
        jnp.sum(jnp.where(spots == n, line, 0.0), axis=1, keepdims=True) for n in range(6)
    ]

    def times_a(p):
        out = [SCALE * p[0]]
        for low, high in zip(p[:-1], p[1:]):
            out.append(SCALE * (low + high))
        return out + [SCALE * p[-1]]

    one = jnp.ones((1, 1), jnp.float32)
    zero = jnp.zeros((1, 1), jnp.float32)
    residual = [one]
    direction = [one]
    answer = [zero, zero, zero]
    now = b[0]
    for iteration in range(3):
        image = times_a(direction)
        alpha = now / form(direction, image, b)
        for n, x in enumerate(direction):
            answer[n] = answer[n] + alpha * x
        if iteration == 2:
            break
        residual = [
            (residual[n] if n < len(residual) else 0.0) - alpha * x for n, x in enumerate(image)
        ]
        after = form(residual, residual, b)
        beta = after / now
        direction = [
            x + (beta * direction[n] if n < len(direction) else 0.0)
            for n, x in enumerate(residual)
        ]
        now = after
    result[...] = base[...] + (answer[0] * v0[...] + (answer[1] * v1[...] + answer[2] * v2[...]))
    second = pltpu.make_async_copy(result, heights, sems.at[1])
    second.start()
    first.wait()
    second.wait()


def solution(mesh):
    row_count = mesh.shape["row"]
    col_count = mesh.shape["col"]

    def index(r, c):
        return r * col_count + c

    ring = max(col_count // 8, 1)
    near_groups = [
        [index(2 * y + core, x + ring * z) for core in range(2) for z in range(col_count // ring)]
        for y in range(row_count // 2)
        for x in range(ring)
    ]
    far_groups = [
        [index(2 * y + core, x + ring * z) for y in range(row_count // 2) for x in range(ring)]
        for core in range(2)
        for z in range(col_count // ring)
    ]
    near_count = len(near_groups[0])
    far_count = len(far_groups[0])
    both = ("row", "col")

    def swap(count, start):
        pairs = [(i, i + 1) for i in range(start, count - 1, 2)]
        return pairs + [(j, i) for i, j in pairs]

    def local(scatter_vectors, ground_ratio, wavenumber, phase, extinction):
        sv = scatter_vectors.reshape(FIELDS, H, W)
        inputs = (sv, wavenumber, phase, extinction)

        tile = pltpu.VMEM((FIELDS, 8, W), jnp.float32)
        edge = call(
            far_edges_kernel,
            f32(SEND_ROWS, W),
            [ANY] * 4,
            [tile, tile, pltpu.VMEM((3, 8, W), jnp.float32), pltpu.SemaphoreType.DMA((5,))],
            name="faredges",
            far=range(4),
        )(*inputs)
        busy = pl.CostEstimate(flops=6000000, transcendentals=0, bytes_accessed=0)
        far = lax.ppermute(edge, "row", swap(row_count, 1))
        edge = call(near_edges_kernel, f32(SEND_ROWS, W), [VM] * 4, name="nearedges", kept=range(4))(*inputs)
        near = lax.ppermute(edge, "row", swap(row_count, 0))
        mom, shares = call(
            early_kernel,
            (f32(5, EH, W), f32(40, 128)),
            [SM, VM, VM],
            name="early",
            kept=(1, 2),
            cost=busy,
        )(ground_ratio, phase, extinction)
        rows = call(
            own_rows_kernel,
            f32(FIELDS * EH, W),
            [VM],
            [pltpu.VMEM((4, 88, 128), jnp.float32), pltpu.VMEM((4, 64, 128), jnp.float32)],
            name="ownrows",
            kept=(0,),
            cost=busy,
        )(sv)
        far, near, mom, shares, rows = lax.optimization_barrier((far, near, mom, shares, rows))
        outer, ext, left, right = call(
            sides_kernel,
            (f32(FIELDS * EH, 256), f32(3 * EH, W), f32(PACK, 128), f32(PACK, 128)),
            [VM] * 6,
            HALO_SCRATCH,
            name="sides",
            kept=range(6),
        )(rows, wavenumber, phase, extinction, far, near)
        far_side = lax.ppermute(left, "col", swap(col_count, 1))
        near_side = lax.ppermute(right, "col", swap(col_count, 0))
        win, mom, mid = call(
            columns_kernel,
            (f32(FIELDS * EH, EW), f32(5, EH, W), f32(3, EH, 256)),
            [VM] * 7,
            [pltpu.VMEM((FIELDS * EH, W), jnp.bfloat16)] * 2
            + [pltpu.VMEM((FIELDS * EH, 256), jnp.float32)]
            + HALO_SCRATCH,
            name="colsums",
            kept=range(7),
            aliases={6: 1},
            cost=busy,
        )(rows, outer, far, near, ext, shares, mom)
        depth, base, v0, v1, v2, sums = call(
            make_fit_kernel(row_count, col_count, near_count),
            tuple(f32(H, W) for _ in range(5)) + (f32(near_count, 128),),
            [VM] * 7,
            [pltpu.VMEM((FIELDS * EH, 128), jnp.bfloat16)] * 2
            + [
                pltpu.VMEM((FIELDS * EH, 384), jnp.float32),
                pltpu.VMEM((3, EH, EW), jnp.float32),
            ],
            name="fit",
            kept=range(7),
        )(win, ext, mom, shares, mid, far_side, near_side)
        parts = lax.all_to_all(
            sums.reshape(near_count, 1, 128), both, 0, 0, axis_index_groups=near_groups
        ).reshape(near_count, 128)
        parts = call(make_relay_kernel(far_count), f32(far_count, 128), [VM], name="relay", kept=(0,))(parts)
        parts = lax.all_to_all(
            parts.reshape(far_count, 1, 128), both, 0, 0, axis_index_groups=far_groups
        ).reshape(far_count, 128)
        return call(
            final_kernel,
            (f32(H, W), f32(H, W)),
            [VM] * 6,
            [pltpu.VMEM((H, W), jnp.float32), pltpu.SemaphoreType.DMA((2,))],
            name="final",
            kept=range(6),
            leaves=(0, 1),
        )(parts, base, v0, v1, v2, depth)

    placed = (P(None, None, None, "row", "col"), P(), P("row", "col"), P("row", "col"), P("row", "col"))
    return jax.shard_map(
        local,
        mesh=mesh,
        in_specs=placed,
        out_specs=(P("row", "col"), P("row", "col")),
        check_vma=False,
    )
```

```python
import jax
import jax.numpy as jnp
from jax import lax
from jax.experimental import pallas as pl
from jax.experimental.pallas import tpu as pltpu
from jax.sharding import PartitionSpec as P

RADIUS = 9
LAYERS = 16
GAUSS_STEPS = 2
EPSILON = 1e-06
DAMPING = 0.002
SCALE = 4.5

H = 32
W = 512
EH = 40
EW = 640
FIELDS = 12
SIDE = RADIUS + 4
REST = SIDE - 8
SENT = 9
REST_AT = SENT * 8
EXTRA_AT = REST_AT + SENT * REST
SEND_ROWS = EXTRA_AT + 3 * 4
GROUPS = 128 // SIDE
PACK = 8 * (-(-FIELDS * 5 // GROUPS) + 1)
VM = pl.BlockSpec(memory_space=pltpu.VMEM)
SM = pl.BlockSpec(memory_space=pltpu.SMEM)
ANY = pl.BlockSpec(memory_space=pl.ANY)
INTERPRET = False


def f32(*shape):
    return jax.ShapeDtypeStruct(shape, jnp.float32)


def call(kernel, outs, ins, scratch=(), name=None, kept=(), far=(), leaves=(), plain=(), aliases=None, cost=None):
    single = not isinstance(outs, tuple)
    shapes = (outs,) if single else outs
    specs = tuple(ANY if n in leaves else VM for n in range(len(shapes)))
    if not INTERPRET:
        shapes = tuple(
            x if n in leaves or n in plain else pltpu.VMEM(x.shape, x.dtype)
            for n, x in enumerate(shapes)
        )
    run = pl.pallas_call(
        kernel,
        out_shape=shapes[0] if single else shapes,
        in_specs=ins,
        out_specs=specs[0] if single else specs,
        scratch_shapes=scratch,
        name=name,
        interpret=INTERPRET,
        input_output_aliases=aliases or {},
        cost_estimate=cost,
        compiler_params=pltpu.CompilerParams(vmem_limit_bytes=16 << 20),
    )

    def apply(*args):
        if not INTERPRET:
            args = tuple(
                pltpu.with_memory_space_constraint(x, pltpu.VMEM if n in kept else pltpu.HBM)
                if n in kept or n in far
                else x
                for n, x in enumerate(args)
            )
        return run(*args)

    return apply


def turned(re1, im1, re2, im2):
    square = re1 * re1 + im1 * im1
    inverse = lax.rsqrt(square)
    none = square == 0.0
    cos = jnp.where(none, 1.0, re1 * inverse)
    sin = jnp.where(none, 0.0, im1 * inverse)
    return re1 * cos + im1 * sin, re2 * cos + im2 * sin, im2 * cos - re2 * sin


def pack_edges(low, out, tiles, rest, extra):
    bottom = low == 1
    for k in range(3):
        for m, value in enumerate(turned(*(tiles(q * 3 + k) for q in range(4)))):
            at = 8 * (m * 3 + k)
            out[at : at + 8] = value
        for m, value in enumerate(turned(*(rest(q * 3 + k) for q in range(4)))):
            at = REST_AT + REST * (m * 3 + k)
            out[at : at + REST] = jnp.where(bottom, value[8 - REST : 8], value[0:REST])
    for j in range(3):
        at = EXTRA_AT + 4 * j
        value = extra(j)
        out[at : at + 4] = jnp.where(bottom, value[4:8], value[0:4])


def far_edges_kernel(sv, vw, ip, ie, out, tiles, rest, extra, sems):
    low = lax.rem(lax.axis_index("row"), 2)
    edge = pl.ds(pl.multiple_of(24 * low, 8), 8)
    inner = pl.ds(pl.multiple_of(8 + 8 * low, 8), 8)
    started = [
        pltpu.make_async_copy(sv.at[:, inner], rest, sems.at[0]),
        pltpu.make_async_copy(sv.at[:, edge], tiles, sems.at[1]),
    ]
    for j, ref in enumerate((vw, ip, ie)):
        started.append(pltpu.make_async_copy(ref.at[edge], extra.at[j], sems.at[2 + j]))
    for copy in started:
        copy.start()
    for copy in started:
        copy.wait()
    pack_edges(low, out, lambda f: tiles[f], lambda f: rest[f], lambda j: extra[j])


def near_edges_kernel(sv, vw, ip, ie, out):
    low = 1 - lax.rem(lax.axis_index("row"), 2)
    edge = pl.ds(pl.multiple_of(24 * low, 8), 8)
    inner = pl.ds(pl.multiple_of(8 + 8 * low, 8), 8)
    fields = (vw, ip, ie)
    pack_edges(low, out, lambda f: sv[f, edge], lambda f: sv[f, inner], lambda j: fields[j][edge])


def strips():
    out = []
    for n in range(FIELDS * 5):
        out.append((n // GROUPS, SIDE * (n % GROUPS), SIDE))
    for n in range(3 * 5):
        out.append((PACK // 8 - 1, 4 * n, 4))
    return out


def products(re1, im1, re2, im2):
    return (
        re1 * re1 + im1 * im1,
        re2 * re2 + im2 * im2,
        re1 * re2 + im1 * im2,
        re1 * im2 - im1 * re2,
    )


def turned_products(one, re2, im2):
    return one * one, re2 * re2 + im2 * im2, one * re2, one * im2


def own_rows_kernel(sv, rows, px, s4):
    sub = lax.broadcasted_iota(jnp.int32, (8, 128), 0)
    for j in range(4):
        px[j, 0:24] = jnp.zeros((24, 128), jnp.float32)
        px[j, 24 + H : 88] = jnp.zeros((64 - H, 128), jnp.float32)
    for k in range(3):

        def block(b, carry, k=k):
            cols = pl.ds(pl.multiple_of(b * 128, 128), 128)
            for j, value in enumerate(products(*(sv[q * 3 + k, :, cols] for q in range(4)))):
                px[j, 24 : 24 + H] = value
            for j in range(4):
                two = px[j, 7:79] + px[j, 8:80]
                four = two[0:64] + (px[j, 9:73] + px[j, 10:74])
                s4[j, 0:64] = four
                eight = four[0:56] + s4[j, 4:60]
                sixteen = eight[0:48] + eight[8:56]
                total = sixteen + two[16:64] + px[j, 25:73]
                at = (j * 3 + k) * EH
                rows[at : at + H, cols] = total[8:40]
                rows[at + H : at + EH, cols] = jnp.where(sub < 4, total[40:48], total[0:8])
            return carry

        lax.fori_loop(0, 4, block, 0)


HALO_SCRATCH = [pltpu.VMEM((4, 32, 128), jnp.float32)] * 4 + [pltpu.VMEM((4, 56, 128), jnp.float32)]


def halo_rows(far, near, blocks, scratch, put):
    odd_row = lax.rem(lax.axis_index("row"), 2) == 1
    sub = lax.broadcasted_iota(jnp.int32, (8, 128), 0)
    xa, xb, ta, tb, out = scratch
    zeros = jnp.zeros((16, 128), jnp.float32)
    for j in range(4):
        xa[j, 8:24] = zeros
        xa[j, 16:32] = zeros
        xb[j, 0:16] = zeros
        xb[j, 16:32] = zeros
        ta[j, 16:32] = zeros
        tb[j, 0:16] = zeros
        out[j, 0:16] = zeros
        out[j, 16:32] = zeros
        out[j, 24:40] = zeros

    def sides(at, size, cols):
        one = far[at : at + size, cols]
        two = near[at : at + size, cols]
        return jnp.where(odd_row, two, one), jnp.where(odd_row, one, two)

    for b in blocks:
        cols = slice(128 * b, 128 * b + 128)
        for k in range(3):
            tiles = [sides(8 * (m * 3 + k), 8, cols) for m in range(3)]
            rests = [sides(REST_AT + REST * (m * 3 + k), REST, cols) for m in range(3)]
            for j, value in enumerate(turned_products(*(x[0] for x in rests))):
                xa[j, 0:REST] = value
            for j, value in enumerate(turned_products(*(x[0] for x in tiles))):
                xa[j, REST:SIDE] = value
            for j, value in enumerate(turned_products(*(x[1] for x in tiles))):
                xb[j, 16:24] = value
            for j, value in enumerate(turned_products(*(x[1] for x in rests))):
                xb[j, 24 : 24 + REST] = value
            for j in range(4):
                four = (xa[j, 0:16] + xa[j, 1:17]) + (xa[j, 2:18] + xa[j, 3:19])
                ta[j, 0:16] = four
                total = (four + ta[j, 4:20]) + (ta[j, 8:24] + ta[j, 12:28])
                out[j, 8:24] = total
                four = (xb[j, 16:32] + xb[j, 15:31]) + (xb[j, 14:30] + xb[j, 13:29])
                tb[j, 16:32] = four
                total = (four + tb[j, 12:28]) + (tb[j, 8:24] + tb[j, 4:20])
                out[j, 39:55] = total
                put(
                    j * 3 + k,
                    b,
                    (
                        out[j, 12:20],
                        out[j, 20:28],
                        out[j, 32:40],
                        out[j, 40:48],
                        jnp.where(sub < 4, out[j, 48:56], out[j, 4:12]),
                    ),
                )


def sides_kernel(sums, vw, ip, ie, far, near, outer, ext, far_pack, near_pack, *scratch):
    lane = lax.broadcasted_iota(jnp.int32, (8, 128), 1)
    odd_row = lax.rem(lax.axis_index("row"), 2) == 1
    odd_col = lax.rem(lax.axis_index("col"), 2) == 1

    def put(f, b, parts):
        for i, part in enumerate(parts):
            at = f * EH + 8 * i
            spot = slice(0, 128) if b == 0 else slice(128, 256)
            outer[at : at + 8, spot] = sums[at : at + 8, 128 * b : 128 * b + 128] + part

    halo_rows(far, near, (0, 3), scratch, put)
    for j, ref in enumerate((vw, ip, ie)):
        at = EXTRA_AT + 4 * j
        one = far[at : at + 4]
        two = near[at : at + 4]
        ext[j * EH : j * EH + H] = ref[...]
        ext[j * EH + H : j * EH + H + 4] = jnp.where(odd_row, one, two)
        ext[j * EH + H + 4 : j * EH + EH] = jnp.where(odd_row, two, one)
    low = [jnp.zeros((8, 128), jnp.float32)] * (PACK // 8)
    high = list(low)
    for n, (v, at, width) in enumerate(strips()):
        here = (lane >= at) & (lane < at + width)
        if n < FIELDS * 5:
            first = outer[8 * n : 8 * n + 8, 0:128]
            last = outer[8 * n : 8 * n + 8, 128:256]
        else:
            top = 8 * n - FIELDS * EH
            first = ext[top : top + 8, 0:128]
            last = ext[top : top + 8, W - 128 : W]
        if at:
            first = pltpu.roll(first, at, 1)
        last = pltpu.roll(last, at + width, 1)
        low[v] = jnp.where(here, first, low[v])
        high[v] = jnp.where(here, last, high[v])
    for v in range(PACK // 8):
        far_pack[8 * v : 8 * v + 8] = jnp.where(odd_col, high[v], low[v])
        near_pack[8 * v : 8 * v + 8] = jnp.where(odd_col, low[v], high[v])


def sincos(x):
    turns = jnp.floor(x * 0.3183098861837907 + 0.5)
    y = x - turns * 3.140625
    y = y - turns * 9.67502593994140625e-4
    y = y - turns * 1.509957990978376432e-7
    odd = turns - 2.0 * jnp.floor(turns * 0.5)
    sign = 1.0 - 2.0 * odd
    z = y * y
    s = -2.3889859e-08
    s = s * z + 2.7525562e-06
    s = s * z - 1.9840874e-04
    s = s * z + 8.3333310e-03
    s = s * z - 1.6666667e-01
    s = y + y * z * s
    c = 2.0875723e-09
    c = c * z - 2.7557319e-07
    c = c * z + 2.4801587e-05
    c = c * z - 1.3888889e-03
    c = c * z + 4.1666667e-02
    c = 1.0 + z * (c * z - 0.5)
    return sign * s, sign * c


def cmul(ar, ai, br, bi):
    return ar * br - ai * bi, ar * bi + ai * br


def moments(phase, atten):
    half_s, half_c = sincos(phase * (0.5 / LAYERS))
    r = jnp.exp(atten * (1.0 / LAYERS))
    zr = r * (half_c * half_c - half_s * half_s)
    zi = r * (2.0 * half_c * half_s)
    n_sum, n_dep = 1.0 + r, r
    sr, si = 1.0 + zr, zi
    dr, di = zr, zi
    count = 2.0
    while count < LAYERS:
        r = r * r
        zr, zi = zr * zr - zi * zi, 2.0 * zr * zi
        n_dep = n_dep + r * (n_dep + count * n_sum)
        n_sum = n_sum + r * n_sum
        tr, ti = cmul(zr, zi, dr + count * sr, di + count * si)
        dr, di = dr + tr, di + ti
        tr, ti = cmul(zr, zi, sr, si)
        sr, si = sr + tr, si + ti
        count = 2.0 * count
    norm = 1.0 / n_sum
    half_c = half_c * norm
    half_s = half_s * norm
    real, imag = cmul(sr, si, half_c, half_s)
    dr, di = cmul(dr, di, half_c, half_s)
    step = 1.0 / LAYERS
    return (
        (n_dep * norm + 0.5) * step,
        real,
        imag,
        (dr + 0.5 * real) * step,
        (di + 0.5 * imag) * step,
    )


def gauss_step(phase, atten, mom, wre, wim, weight, offset):
    mean_depth, real_part, imag_part, depth_cos, depth_sin = mom
    ra = depth_cos - mean_depth * real_part
    rt = -depth_sin
    ia = depth_sin - mean_depth * imag_part
    it = depth_cos
    er = wre - weight * real_part - offset
    ei = wim - weight * imag_part
    maa = weight * (ra * ra + ia * ia) + DAMPING
    map_ = weight * (ra * rt + ia * it)
    mpp = weight * (rt * rt + it * it) + DAMPING
    ga = ra * er + ia * ei
    gp = rt * er + it * ei
    inverse = 1.0 / (maa * mpp - map_ * map_)
    return (
        phase + (maa * gp - map_ * ga) * inverse,
        atten + (mpp * ga - map_ * gp) * inverse,
    )


def fit_tile(sums, weights, weight, offset, phase, atten, first):
    wre = wim = power = None
    for k in range(3):
        scale = lax.rsqrt(sums(k) * sums(3 + k) + EPSILON)
        cre = sums(6 + k) * scale
        cim = sums(9 + k) * scale
        square = cre * cre + cim * cim
        if k:
            wre = wre + cre * weights[k]
            wim = wim + cim * weights[k]
            power = power + square
        else:
            wre = cre * weights[k]
            wim = cim * weights[k]
            power = square
    for step in range(GAUSS_STEPS):
        now = moments(phase, atten) if step or first is None else first
        phase, atten = gauss_step(phase, atten, now, wre, wim, weight, offset)
    return phase, atten, power * (1.0 / 3.0)


def early_kernel(ground, ip, ie, mom, shares):
    ratios = [jnp.full((8, 128), ground[k], jnp.float32) for k in range(3)]
    weights = [1.0 / (1.0 + g) for g in ratios]
    weight = weights[0] * weights[0] + weights[1] * weights[1] + weights[2] * weights[2]
    offset = (
        ratios[0] * weights[0] * weights[0]
        + ratios[1] * weights[1] * weights[1]
        + ratios[2] * weights[2] * weights[2]
    )
    for n, value in enumerate((*weights, weight, offset)):
        shares[8 * n : 8 * n + 8] = value

    def tiles(i, carry):
        here = pl.ds(pl.multiple_of(8 * i, 8), 8)
        for b in range(4):
            cols = slice(128 * b, 128 * b + 128)
            for n, value in enumerate(moments(ip[here, cols], ie[here, cols])):
                mom[n, here, cols] = value
        return carry

    lax.fori_loop(0, H // 8, tiles, 0)


def split(value):
    first = value.astype(jnp.bfloat16)
    return first, (value - first.astype(jnp.float32)).astype(jnp.bfloat16)


def band(height, width, shift):
    up = lax.broadcasted_iota(jnp.int32, (height, width), 0) - shift
    across = lax.broadcasted_iota(jnp.int32, (height, width), 1)
    return (jnp.abs(up - across) <= RADIUS).astype(jnp.float32).astype(jnp.bfloat16)


def dot(a, b):
    return jnp.dot(a, b, preferred_element_type=jnp.float32)


def columns_kernel(rows, outer, far, near, ext, shares, held, win, mom, mid, hi, lo, sums, *scratch):
    if INTERPRET:
        mom[:, 0:H] = held[:, 0:H]

    def put(f, b, parts):
        for i, part in enumerate(parts):
            at = f * EH + 8 * i
            spot = slice(128 * b - 128, 128 * b)
            sums[at : at + 8, spot] = rows[at : at + 8, 128 * b : 128 * b + 128] + part

    halo_rows(far, near, (1, 2), scratch, put)
    for n in range(6):
        here = slice(80 * n, 80 * n + 80)
        hi[here, 0:128], lo[here, 0:128] = split(outer[here, 0:128])
        hi[here, 384:512], lo[here, 384:512] = split(outer[here, 128:256])
        for b in range(2):
            cols = slice(128 * b + 128, 128 * b + 256)
            hi[here, cols], lo[here, cols] = split(sums[here, 128 * b : 128 * b + 128])
    left = band(384, 256, 0)
    right = band(384, 256, 128)
    win[:, 0:256] = dot(hi[:, 0:384], left) + dot(lo[:, 0:384], left)
    win[:, 256:512] = dot(hi[:, 128:512], right) + dot(lo[:, 128:512], right)
    before = band(128, 128, 128)
    after = band(128, 128, -128)
    win[:, 512:640] = (dot(hi[:, 384:512], before) + dot(lo[:, 384:512], before)) + (
        dot(hi[:, 0:128], after) + dot(lo[:, 0:128], after)
    )
    for b in range(4):
        cols = slice(128 * b, 128 * b + 128)
        values = moments(ext[EH + H : EH + EH, cols], ext[2 * EH + H : 2 * EH + EH, cols])
        for n, value in enumerate(values):
            mom[n, H:EH, cols] = value
    weights = [shares[8 * n : 8 * n + 8] for n in range(3)]
    weight = shares[24:32]
    offset = shares[32:40]

    def fit(i, carry):
        here = pl.ds(pl.multiple_of(8 * i, 8), 8)
        for b in (1, 2):
            cols = slice(128 * b, 128 * b + 128)

            def sums(f):
                return win[pl.ds(pl.multiple_of(f * EH + 8 * i, 8), 8), cols]

            kz, phase, atten = (
                ext[pl.ds(pl.multiple_of(j * EH + 8 * i, 8), 8), cols] for j in range(3)
            )
            first = tuple(mom[n, here, cols] for n in range(5))
            phase, atten, power = fit_tile(sums, weights, weight, offset, phase, atten, first)
            spot = slice(128 * b - 128, 128 * b)
            mid[0, here, spot] = phase / kz
            mid[1, here, spot] = atten
            mid[2, here, spot] = power
        return carry

    lax.fori_loop(0, 5, fit, 0)


def around(field):
    return (
        pltpu.roll(field, 1, 0)
        + pltpu.roll(field, EH - 1, 0)
        + pltpu.roll(field, 1, 1)
        + pltpu.roll(field, EW - 1, 1)
    )


def make_fit_kernel(row_count, col_count, group):
    def kernel(
        win, ext, mom, shares, mid, far, near,
        depth, base, v0, v1, v2, sums,
        hi, lo, rim, wide,
    ):
        lane = lax.broadcasted_iota(jnp.int32, (8, 128), 1)
        row = lax.axis_index("row")
        col = lax.axis_index("col")
        odd_col = lax.rem(col, 2) == 1
        places = strips()
        packs = []
        for v in range(PACK // 8):
            one = far[8 * v : 8 * v + 8]
            two = near[8 * v : 8 * v + 8]
            packs.append((jnp.where(odd_col, one, two), jnp.where(odd_col, two, one)))

        def halo_tile(strip):
            v, at, width = places[strip]
            low, high = packs[v]
            if at:
                low = pltpu.roll(low, 128 - at, 1)
            high = pltpu.roll(high, 128 - at - width, 1)
            return jnp.where(lane < width, low, jnp.where(lane >= 128 - width, high, 0.0))

        for n in range(6):
            halo = jnp.concatenate([halo_tile(10 * n + i) for i in range(10)], axis=0)
            hi[80 * n : 80 * n + 80], lo[80 * n : 80 * n + 80] = split(halo)
        for n, shift in enumerate((128, 0, -128)):
            part = band(128, 128, shift)
            rim[:, 128 * n : 128 * n + 128] = dot(hi[...], part) + dot(lo[...], part)
        rim_of = {0: 0, 4: 1, 3: 2}
        weights = [shares[8 * n : 8 * n + 8] for n in range(3)]
        weight = shares[24:32]
        offset = shares[32:40]

        def tile(f, i, b):
            at = f * EH + 8 * i
            value = win[at : at + 8, 128 * b : 128 * b + 128]
            return value + rim[at : at + 8, 128 * rim_of[b] : 128 * rim_of[b] + 128]

        def gathered(parts):
            out = jnp.zeros((8, 128), jnp.float32)
            for i, part in enumerate(parts):
                here = (lane >= 8 * i) & (lane < 8 * i + 8)
                out = jnp.where(here, pltpu.roll(part, 8 * i + 4, 1), out)
            return out

        def rim_sums(f):
            return gathered([tile(f, i, 4) for i in range(5)])

        kz, phase, atten = (
            gathered([halo_tile((FIELDS + j) * 5 + i) for i in range(5)]) for j in range(3)
        )
        phase, _, power = fit_tile(rim_sums, weights, weight, offset, phase, atten, None)
        phase = phase / kz
        for i in range(5):
            here = slice(8 * i, 8 * i + 8)
            wide[0, here, W:EW] = pltpu.roll(phase, 124 - 8 * i, 1)
            wide[2, here, W:EW] = pltpu.roll(power, 124 - 8 * i, 1)
        for i in range(5):
            here = slice(8 * i, 8 * i + 8)
            for b in (0, 3):
                cols = slice(128 * b, 128 * b + 128)
                kz, phase, atten = (
                    ext[j * EH + 8 * i : j * EH + 8 * i + 8, cols] for j in range(3)
                )
                first = tuple(mom[n, here, cols] for n in range(5))
                phase, atten, power = fit_tile(
                    lambda f: tile(f, i, b), weights, weight, offset, phase, atten, first
                )
                wide[0, here, cols] = phase / kz
                wide[1, here, cols] = atten
                wide[2, here, cols] = power
        for n in range(3):
            wide[n, :, 128:384] = mid[n]
        depth[...] = wide[1, 0:H, 0:W]

        r = lax.broadcasted_iota(jnp.int32, (EH, EW), 0)
        c = lax.broadcasted_iota(jnp.int32, (EH, EW), 1)
        row_low = jnp.where(row == 0, EH - 4, EH)
        row_high = jnp.where(row == row_count - 1, H, EH - 4)
        col_low = jnp.where(col == 0, EW, EW - 4)
        col_high = jnp.where(col == col_count - 1, W, W + 4)
        row_bad = ((r >= row_high) & (r < EH - 4)) | (r >= row_low)
        col_bad = (c >= col_high) & (c < col_low)
        inside = jnp.logical_not(row_bad | col_bad)

        start = jnp.where(inside, wide[0], 0.0)
        confidence = wide[2] - 0.5
        base[...] = start[0:H, 0:W]
        first = jnp.where(inside, around(start) - 4.0 * start, 0.0)
        v0[...] = first[0:H, 0:W]

        def advance(field):
            return jnp.where(inside, (confidence * field - around(field)) * (1.0 / SCALE), 0.0)

        second = advance(first)
        v1[...] = second[0:H, 0:W]
        third = advance(second)
        v2[...] = third[0:H, 0:W]
        fourth = advance(third)
        a0, a1, a2, a3 = (x[0:H, 0:W] for x in (first, second, third, fourth))
        spots = lax.broadcasted_iota(jnp.int32, (1, 128), 1)
        line = jnp.zeros((1, 128), jnp.float32)
        for n, (p, q) in enumerate(((a0, a0), (a0, a1), (a1, a1), (a1, a2), (a2, a2), (a2, a3))):
            product = p * q
            total = jnp.sum(jnp.sum(product, axis=0, keepdims=True), axis=1, keepdims=True)
            line = jnp.where(spots == n, total, line)
        sums[...] = jnp.broadcast_to(line, (group, 128))

    return kernel


def make_relay_kernel(out_group):
    def kernel(parts, out):
        out[...] = jnp.broadcast_to(jnp.sum(parts[...], axis=0, keepdims=True), (out_group, 128))

    return kernel


def form(p, q, b):
    total = None
    for i, x in enumerate(p):
        for j, y in enumerate(q):
            term = x * y * b[i + j]
            total = term if total is None else total + term
    return total


def final_kernel(parts, base, v0, v1, v2, fitted, heights, depth, result, sems):
    first = pltpu.make_async_copy(fitted, depth, sems.at[0])
    first.start()
    line = jnp.sum(parts[...], axis=0, keepdims=True)
    spots = lax.broadcasted_iota(jnp.int32, (1, 128), 1)
    b = [
        jnp.sum(jnp.where(spots == n, line, 0.0), axis=1, keepdims=True) for n in range(6)
    ]

    def times_a(p):
        out = [SCALE * p[0]]
        for low, high in zip(p[:-1], p[1:]):
            out.append(SCALE * (low + high))
        return out + [SCALE * p[-1]]

    one = jnp.ones((1, 1), jnp.float32)
    zero = jnp.zeros((1, 1), jnp.float32)
    residual = [one]
    direction = [one]
    answer = [zero, zero, zero]
    now = b[0]
    for iteration in range(3):
        image = times_a(direction)
        alpha = now / form(direction, image, b)
        for n, x in enumerate(direction):
            answer[n] = answer[n] + alpha * x
        if iteration == 2:
            break
        residual = [
            (residual[n] if n < len(residual) else 0.0) - alpha * x for n, x in enumerate(image)
        ]
        after = form(residual, residual, b)
        beta = after / now
        direction = [
            x + (beta * direction[n] if n < len(direction) else 0.0)
            for n, x in enumerate(residual)
        ]
        now = after
    result[...] = base[...] + (answer[0] * v0[...] + (answer[1] * v1[...] + answer[2] * v2[...]))
    second = pltpu.make_async_copy(result, heights, sems.at[1])
    second.start()
    first.wait()
    second.wait()


def solution(mesh):
    row_count = mesh.shape["row"]
    col_count = mesh.shape["col"]

    def index(r, c):
        return r * col_count + c

    def outward(count):
        return sorted(range(count), key=lambda i: (abs(i - count // 2), i))

    ring = max(col_count // 8, 1)
    cores, ys = outward(2), outward(row_count // 2)
    xs, zs = outward(ring), outward(col_count // ring)
    near_groups = [
        [index(2 * y + core, x + ring * z) for core in cores for z in zs] for y in ys for x in xs
    ]
    far_groups = [
        [index(2 * y + core, x + ring * z) for y in ys for x in xs] for core in cores for z in zs
    ]
    near_count = len(near_groups[0])
    far_count = len(far_groups[0])
    both = ("row", "col")

    def swap(count, start):
        pairs = [(i, i + 1) for i in range(start, count - 1, 2)]
        return pairs + [(j, i) for i, j in pairs]

    def local(scatter_vectors, ground_ratio, wavenumber, phase, extinction):
        sv = scatter_vectors.reshape(FIELDS, H, W)
        inputs = (sv, wavenumber, phase, extinction)

        tile = pltpu.VMEM((FIELDS, 8, W), jnp.float32)
        edge = call(
            far_edges_kernel,
            f32(SEND_ROWS, W),
            [ANY] * 4,
            [tile, tile, pltpu.VMEM((3, 8, W), jnp.float32), pltpu.SemaphoreType.DMA((5,))],
            name="faredges",
            far=range(4),
        )(*inputs)
        busy = pl.CostEstimate(flops=6000000, transcendentals=0, bytes_accessed=0)
        far = lax.ppermute(edge, "row", swap(row_count, 1))
        edge = call(near_edges_kernel, f32(SEND_ROWS, W), [VM] * 4, name="nearedges", kept=range(4))(*inputs)
        near = lax.ppermute(edge, "row", swap(row_count, 0))
        mom, shares = call(
            early_kernel,
            (f32(5, EH, W), f32(40, 128)),
            [SM, VM, VM],
            name="early",
            kept=(1, 2),
            cost=busy,
        )(ground_ratio, phase, extinction)
        rows = call(
            own_rows_kernel,
            f32(FIELDS * EH, W),
            [VM],
            [pltpu.VMEM((4, 88, 128), jnp.float32), pltpu.VMEM((4, 64, 128), jnp.float32)],
            name="ownrows",
            kept=(0,),
            cost=busy,
        )(sv)
        far, near, mom, shares, rows = lax.optimization_barrier((far, near, mom, shares, rows))
        outer, ext, left, right = call(
            sides_kernel,
            (f32(FIELDS * EH, 256), f32(3 * EH, W), f32(PACK, 128), f32(PACK, 128)),
            [VM] * 6,
            HALO_SCRATCH,
            name="sides",
            kept=range(6),
        )(rows, wavenumber, phase, extinction, far, near)
        far_side = lax.ppermute(left, "col", swap(col_count, 1))
        near_side = lax.ppermute(right, "col", swap(col_count, 0))
        win, mom, mid = call(
            columns_kernel,
            (f32(FIELDS * EH, EW), f32(5, EH, W), f32(3, EH, 256)),
            [VM] * 7,
            [pltpu.VMEM((FIELDS * EH, W), jnp.bfloat16)] * 2
            + [pltpu.VMEM((FIELDS * EH, 256), jnp.float32)]
            + HALO_SCRATCH,
            name="colsums",
            kept=range(7),
            aliases={6: 1},
            cost=busy,
        )(rows, outer, far, near, ext, shares, mom)
        depth, base, v0, v1, v2, sums = call(
            make_fit_kernel(row_count, col_count, near_count),
            tuple(f32(H, W) for _ in range(5)) + (f32(near_count, 128),),
            [VM] * 7,
            [pltpu.VMEM((FIELDS * EH, 128), jnp.bfloat16)] * 2
            + [
                pltpu.VMEM((FIELDS * EH, 384), jnp.float32),
                pltpu.VMEM((3, EH, EW), jnp.float32),
            ],
            name="fit",
            kept=range(7),
        )(win, ext, mom, shares, mid, far_side, near_side)
        parts = lax.all_to_all(
            sums.reshape(near_count, 1, 128), both, 0, 0, axis_index_groups=near_groups
        ).reshape(near_count, 128)
        parts = call(make_relay_kernel(far_count), f32(far_count, 128), [VM], name="relay", kept=(0,))(parts)
        parts = lax.all_to_all(
            parts.reshape(far_count, 1, 128), both, 0, 0, axis_index_groups=far_groups
        ).reshape(far_count, 128)
        return call(
            final_kernel,
            (f32(H, W), f32(H, W)),
            [VM] * 6,
            [pltpu.VMEM((H, W), jnp.float32), pltpu.SemaphoreType.DMA((2,))],
            name="final",
            kept=range(6),
            leaves=(0, 1),
        )(parts, base, v0, v1, v2, depth)

    placed = (P(None, None, None, "row", "col"), P(), P("row", "col"), P("row", "col"), P("row", "col"))
    return jax.shard_map(
        local,
        mesh=mesh,
        in_specs=placed,
        out_specs=(P("row", "col"), P("row", "col")),
        check_vma=False,
    )
```

```python
import jax
import jax.numpy as jnp
from jax import lax
from jax.experimental import pallas as pl
from jax.experimental.pallas import tpu as pltpu
from jax.sharding import PartitionSpec as P

RADIUS = 9
LAYERS = 16
GAUSS_STEPS = 2
EPSILON = 1e-06
DAMPING = 0.002
SCALE = 4.5

H = 32
W = 512
EH = 40
EW = 640
FIELDS = 12
SIDE = RADIUS + 4
REST = SIDE - 8
SENT = 9
REST_AT = SENT * 8
EXTRA_AT = REST_AT + SENT * REST
SEND_ROWS = EXTRA_AT + 3 * 4
GROUPS = 128 // SIDE
PACK = 8 * (-(-FIELDS * 5 // GROUPS) + 1)
VM = pl.BlockSpec(memory_space=pltpu.VMEM)
SM = pl.BlockSpec(memory_space=pltpu.SMEM)
ANY = pl.BlockSpec(memory_space=pl.ANY)
INTERPRET = False


def f32(*shape):
    return jax.ShapeDtypeStruct(shape, jnp.float32)


def call(kernel, outs, ins, scratch=(), name=None, kept=(), far=(), leaves=(), plain=(), aliases=None, cost=None):
    single = not isinstance(outs, tuple)
    shapes = (outs,) if single else outs
    specs = tuple(ANY if n in leaves else VM for n in range(len(shapes)))
    if not INTERPRET:
        shapes = tuple(
            x if n in leaves or n in plain else pltpu.VMEM(x.shape, x.dtype)
            for n, x in enumerate(shapes)
        )
    run = pl.pallas_call(
        kernel,
        out_shape=shapes[0] if single else shapes,
        in_specs=ins,
        out_specs=specs[0] if single else specs,
        scratch_shapes=scratch,
        name=name,
        interpret=INTERPRET,
        input_output_aliases=aliases or {},
        cost_estimate=cost,
        compiler_params=pltpu.CompilerParams(vmem_limit_bytes=16 << 20),
    )

    def apply(*args):
        if not INTERPRET:
            args = tuple(
                pltpu.with_memory_space_constraint(x, pltpu.VMEM if n in kept else pltpu.HBM)
                if n in kept or n in far
                else x
                for n, x in enumerate(args)
            )
        return run(*args)

    return apply


def turned(re1, im1, re2, im2):
    square = re1 * re1 + im1 * im1
    inverse = lax.rsqrt(square)
    none = square == 0.0
    cos = jnp.where(none, 1.0, re1 * inverse)
    sin = jnp.where(none, 0.0, im1 * inverse)
    return re1 * cos + im1 * sin, re2 * cos + im2 * sin, im2 * cos - re2 * sin


def pack_edges(low, out, tiles, rest, extra):
    bottom = low == 1
    for k in range(3):
        for m, value in enumerate(turned(*(tiles(q * 3 + k) for q in range(4)))):
            at = 8 * (m * 3 + k)
            out[at : at + 8] = value
        for m, value in enumerate(turned(*(rest(q * 3 + k) for q in range(4)))):
            at = REST_AT + REST * (m * 3 + k)
            out[at : at + REST] = jnp.where(bottom, value[8 - REST : 8], value[0:REST])
    for j in range(3):
        at = EXTRA_AT + 4 * j
        value = extra(j)
        out[at : at + 4] = jnp.where(bottom, value[4:8], value[0:4])


def far_edges_kernel(sv, vw, ip, ie, out, tiles, rest, extra, sems):
    low = lax.rem(lax.axis_index("row"), 2)
    edge = pl.ds(pl.multiple_of(24 * low, 8), 8)
    inner = pl.ds(pl.multiple_of(8 + 8 * low, 8), 8)
    started = [
        pltpu.make_async_copy(sv.at[:, inner], rest, sems.at[0]),
        pltpu.make_async_copy(sv.at[:, edge], tiles, sems.at[1]),
    ]
    for j, ref in enumerate((vw, ip, ie)):
        started.append(pltpu.make_async_copy(ref.at[edge], extra.at[j], sems.at[2 + j]))
    for copy in started:
        copy.start()
    for copy in started:
        copy.wait()
    pack_edges(low, out, lambda f: tiles[f], lambda f: rest[f], lambda j: extra[j])


def near_edges_kernel(sv, vw, ip, ie, out):
    low = 1 - lax.rem(lax.axis_index("row"), 2)
    edge = pl.ds(pl.multiple_of(24 * low, 8), 8)
    inner = pl.ds(pl.multiple_of(8 + 8 * low, 8), 8)
    fields = (vw, ip, ie)
    pack_edges(low, out, lambda f: sv[f, edge], lambda f: sv[f, inner], lambda j: fields[j][edge])


def strips():
    out = []
    for n in range(FIELDS * 5):
        out.append((n // GROUPS, SIDE * (n % GROUPS), SIDE))
    for n in range(3 * 5):
        out.append((PACK // 8 - 1, 4 * n, 4))
    return out


def products(re1, im1, re2, im2):
    return (
        re1 * re1 + im1 * im1,
        re2 * re2 + im2 * im2,
        re1 * re2 + im1 * im2,
        re1 * im2 - im1 * re2,
    )


def turned_products(one, re2, im2):
    return one * one, re2 * re2 + im2 * im2, one * re2, one * im2


def own_rows_kernel(sv, rows, px, s4):
    sub = lax.broadcasted_iota(jnp.int32, (8, 128), 0)
    for j in range(4):
        px[j, 0:24] = jnp.zeros((24, 128), jnp.float32)
        px[j, 24 + H : 88] = jnp.zeros((64 - H, 128), jnp.float32)
    for k in range(3):

        def block(b, carry, k=k):
            cols = pl.ds(pl.multiple_of(b * 128, 128), 128)
            for j, value in enumerate(products(*(sv[q * 3 + k, :, cols] for q in range(4)))):
                px[j, 24 : 24 + H] = value
            for j in range(4):
                two = px[j, 7:79] + px[j, 8:80]
                four = two[0:64] + (px[j, 9:73] + px[j, 10:74])
                s4[j, 0:64] = four
                eight = four[0:56] + s4[j, 4:60]
                sixteen = eight[0:48] + eight[8:56]
                total = sixteen + two[16:64] + px[j, 25:73]
                at = (j * 3 + k) * EH
                rows[at : at + H, cols] = total[8:40]
                rows[at + H : at + EH, cols] = jnp.where(sub < 4, total[40:48], total[0:8])
            return carry

        lax.fori_loop(0, 4, block, 0)


HALO_SCRATCH = [pltpu.VMEM((4, 32, 128), jnp.float32)] * 4 + [pltpu.VMEM((4, 56, 128), jnp.float32)]


def halo_rows(far, near, blocks, scratch, put):
    odd_row = lax.rem(lax.axis_index("row"), 2) == 1
    sub = lax.broadcasted_iota(jnp.int32, (8, 128), 0)
    xa, xb, ta, tb, out = scratch
    zeros = jnp.zeros((16, 128), jnp.float32)
    for j in range(4):
        xa[j, 8:24] = zeros
        xa[j, 16:32] = zeros
        xb[j, 0:16] = zeros
        xb[j, 16:32] = zeros
        ta[j, 16:32] = zeros
        tb[j, 0:16] = zeros
        out[j, 0:16] = zeros
        out[j, 16:32] = zeros
        out[j, 24:40] = zeros

    def sides(at, size, cols):
        one = far[at : at + size, cols]
        two = near[at : at + size, cols]
        return jnp.where(odd_row, two, one), jnp.where(odd_row, one, two)

    for b in blocks:
        cols = slice(128 * b, 128 * b + 128)
        for k in range(3):
            tiles = [sides(8 * (m * 3 + k), 8, cols) for m in range(3)]
            rests = [sides(REST_AT + REST * (m * 3 + k), REST, cols) for m in range(3)]
            for j, value in enumerate(turned_products(*(x[0] for x in rests))):
                xa[j, 0:REST] = value
            for j, value in enumerate(turned_products(*(x[0] for x in tiles))):
                xa[j, REST:SIDE] = value
            for j, value in enumerate(turned_products(*(x[1] for x in tiles))):
                xb[j, 16:24] = value
            for j, value in enumerate(turned_products(*(x[1] for x in rests))):
                xb[j, 24 : 24 + REST] = value
            for j in range(4):
                four = (xa[j, 0:16] + xa[j, 1:17]) + (xa[j, 2:18] + xa[j, 3:19])
                ta[j, 0:16] = four
                total = (four + ta[j, 4:20]) + (ta[j, 8:24] + ta[j, 12:28])
                out[j, 8:24] = total
                four = (xb[j, 16:32] + xb[j, 15:31]) + (xb[j, 14:30] + xb[j, 13:29])
                tb[j, 16:32] = four
                total = (four + tb[j, 12:28]) + (tb[j, 8:24] + tb[j, 4:20])
                out[j, 39:55] = total
                put(
                    j * 3 + k,
                    b,
                    (
                        out[j, 12:20],
                        out[j, 20:28],
                        out[j, 32:40],
                        out[j, 40:48],
                        jnp.where(sub < 4, out[j, 48:56], out[j, 4:12]),
                    ),
                )


def sides_kernel(sums, vw, ip, ie, far, near, outer, ext, far_pack, near_pack, *scratch):
    lane = lax.broadcasted_iota(jnp.int32, (8, 128), 1)
    odd_row = lax.rem(lax.axis_index("row"), 2) == 1
    odd_col = lax.rem(lax.axis_index("col"), 2) == 1

    def put(f, b, parts):
        for i, part in enumerate(parts):
            at = f * EH + 8 * i
            spot = slice(0, 128) if b == 0 else slice(128, 256)
            outer[at : at + 8, spot] = sums[at : at + 8, 128 * b : 128 * b + 128] + part

    halo_rows(far, near, (0, 3), scratch, put)
    for j, ref in enumerate((vw, ip, ie)):
        at = EXTRA_AT + 4 * j
        one = far[at : at + 4]
        two = near[at : at + 4]
        ext[j * EH : j * EH + H] = ref[...]
        ext[j * EH + H : j * EH + H + 4] = jnp.where(odd_row, one, two)
        ext[j * EH + H + 4 : j * EH + EH] = jnp.where(odd_row, two, one)
    low = [jnp.zeros((8, 128), jnp.float32)] * (PACK // 8)
    high = list(low)
    for n, (v, at, width) in enumerate(strips()):
        here = (lane >= at) & (lane < at + width)
        if n < FIELDS * 5:
            first = outer[8 * n : 8 * n + 8, 0:128]
            last = outer[8 * n : 8 * n + 8, 128:256]
        else:
            top = 8 * n - FIELDS * EH
            first = ext[top : top + 8, 0:128]
            last = ext[top : top + 8, W - 128 : W]
        if at:
            first = pltpu.roll(first, at, 1)
        last = pltpu.roll(last, at + width, 1)
        low[v] = jnp.where(here, first, low[v])
        high[v] = jnp.where(here, last, high[v])
    for v in range(PACK // 8):
        far_pack[8 * v : 8 * v + 8] = jnp.where(odd_col, high[v], low[v])
        near_pack[8 * v : 8 * v + 8] = jnp.where(odd_col, low[v], high[v])


def sincos(x):
    turns = jnp.floor(x * 0.3183098861837907 + 0.5)
    y = x - turns * 3.140625
    y = y - turns * 9.676535897932385e-4
    odd = turns - 2.0 * jnp.floor(turns * 0.5)
    sign = 1.0 - 2.0 * odd
    z = y * y
    s = -2.3889859e-08
    s = s * z + 2.7525562e-06
    s = s * z - 1.9840874e-04
    s = s * z + 8.3333310e-03
    s = s * z - 1.6666667e-01
    s = y + y * z * s
    c = 2.0875723e-09
    c = c * z - 2.7557319e-07
    c = c * z + 2.4801587e-05
    c = c * z - 1.3888889e-03
    c = c * z + 4.1666667e-02
    c = 1.0 + z * (c * z - 0.5)
    return sign * s, sign * c


def cmul(ar, ai, br, bi):
    return ar * br - ai * bi, ar * bi + ai * br


def moments(phase, atten):
    half_s, half_c = sincos(phase * (0.5 / LAYERS))
    r = jnp.exp(atten * (1.0 / LAYERS))
    zr = r * (half_c * half_c - half_s * half_s)
    zi = r * (2.0 * half_c * half_s)
    n_sum, n_dep = 1.0 + r, r
    sr, si = 1.0 + zr, zi
    dr, di = zr, zi
    count = 2.0
    while count < LAYERS:
        r = r * r
        zr, zi = zr * zr - zi * zi, 2.0 * zr * zi
        n_dep = n_dep + r * (n_dep + count * n_sum)
        n_sum = n_sum + r * n_sum
        tr, ti = cmul(zr, zi, dr + count * sr, di + count * si)
        dr, di = dr + tr, di + ti
        tr, ti = cmul(zr, zi, sr, si)
        sr, si = sr + tr, si + ti
        count = 2.0 * count
    norm = 1.0 / n_sum
    half_c = half_c * norm
    half_s = half_s * norm
    real, imag = cmul(sr, si, half_c, half_s)
    dr, di = cmul(dr, di, half_c, half_s)
    step = 1.0 / LAYERS
    return (
        (n_dep * norm + 0.5) * step,
        real,
        imag,
        (dr + 0.5 * real) * step,
        (di + 0.5 * imag) * step,
    )


def gauss_step(phase, atten, mom, wre, wim, weight, offset):
    mean_depth, real_part, imag_part, depth_cos, depth_sin = mom
    ra = depth_cos - mean_depth * real_part
    rt = -depth_sin
    ia = depth_sin - mean_depth * imag_part
    it = depth_cos
    er = wre - weight * real_part - offset
    ei = wim - weight * imag_part
    maa = weight * (ra * ra + ia * ia) + DAMPING
    map_ = weight * (ra * rt + ia * it)
    mpp = weight * (rt * rt + it * it) + DAMPING
    ga = ra * er + ia * ei
    gp = rt * er + it * ei
    inverse = 1.0 / (maa * mpp - map_ * map_)
    return (
        phase + (maa * gp - map_ * ga) * inverse,
        atten + (mpp * ga - map_ * gp) * inverse,
    )


def fit_tile(sums, weights, weight, offset, phase, atten, first):
    wre = wim = power = None
    for k in range(3):
        scale = lax.rsqrt(sums(k) * sums(3 + k) + EPSILON)
        cre = sums(6 + k) * scale
        cim = sums(9 + k) * scale
        square = cre * cre + cim * cim
        if k:
            wre = wre + cre * weights[k]
            wim = wim + cim * weights[k]
            power = power + square
        else:
            wre = cre * weights[k]
            wim = cim * weights[k]
            power = square
    for step in range(GAUSS_STEPS):
        now = moments(phase, atten) if step or first is None else first
        phase, atten = gauss_step(phase, atten, now, wre, wim, weight, offset)
    return phase, atten, power * (1.0 / 3.0)


def early_kernel(ground, ip, ie, mom, shares):
    ratios = [jnp.full((8, 128), ground[k], jnp.float32) for k in range(3)]
    weights = [1.0 / (1.0 + g) for g in ratios]
    weight = weights[0] * weights[0] + weights[1] * weights[1] + weights[2] * weights[2]
    offset = (
        ratios[0] * weights[0] * weights[0]
        + ratios[1] * weights[1] * weights[1]
        + ratios[2] * weights[2] * weights[2]
    )
    for n, value in enumerate((*weights, weight, offset)):
        shares[8 * n : 8 * n + 8] = value

    def tiles(i, carry):
        here = pl.ds(pl.multiple_of(8 * i, 8), 8)
        for b in range(4):
            cols = slice(128 * b, 128 * b + 128)
            for n, value in enumerate(moments(ip[here, cols], ie[here, cols])):
                mom[n, here, cols] = value
        return carry

    lax.fori_loop(0, H // 8, tiles, 0)


def split(value):
    first = value.astype(jnp.bfloat16)
    return first, (value - first.astype(jnp.float32)).astype(jnp.bfloat16)


def band(height, width, shift):
    up = lax.broadcasted_iota(jnp.int32, (height, width), 0) - shift
    across = lax.broadcasted_iota(jnp.int32, (height, width), 1)
    return (jnp.abs(up - across) <= RADIUS).astype(jnp.float32).astype(jnp.bfloat16)


def dot(a, b):
    return jnp.dot(a, b, preferred_element_type=jnp.float32)


def columns_kernel(rows, outer, far, near, ext, shares, held, win, mom, mid, hi, lo, sums, *scratch):
    if INTERPRET:
        mom[:, 0:H] = held[:, 0:H]

    def put(f, b, parts):
        for i, part in enumerate(parts):
            at = f * EH + 8 * i
            spot = slice(128 * b - 128, 128 * b)
            sums[at : at + 8, spot] = rows[at : at + 8, 128 * b : 128 * b + 128] + part

    halo_rows(far, near, (1, 2), scratch, put)
    for n in range(6):
        here = slice(80 * n, 80 * n + 80)
        hi[here, 0:128], lo[here, 0:128] = split(outer[here, 0:128])
        hi[here, 384:512], lo[here, 384:512] = split(outer[here, 128:256])
        for b in range(2):
            cols = slice(128 * b + 128, 128 * b + 256)
            hi[here, cols], lo[here, cols] = split(sums[here, 128 * b : 128 * b + 128])
    left = band(384, 256, 0)
    right = band(384, 256, 128)
    win[:, 0:256] = dot(hi[:, 0:384], left) + dot(lo[:, 0:384], left)
    win[:, 256:512] = dot(hi[:, 128:512], right) + dot(lo[:, 128:512], right)
    before = band(128, 128, 128)
    after = band(128, 128, -128)
    win[:, 512:640] = (dot(hi[:, 384:512], before) + dot(lo[:, 384:512], before)) + (
        dot(hi[:, 0:128], after) + dot(lo[:, 0:128], after)
    )
    for b in range(4):
        cols = slice(128 * b, 128 * b + 128)
        values = moments(ext[EH + H : EH + EH, cols], ext[2 * EH + H : 2 * EH + EH, cols])
        for n, value in enumerate(values):
            mom[n, H:EH, cols] = value
    weights = [shares[8 * n : 8 * n + 8] for n in range(3)]
    weight = shares[24:32]
    offset = shares[32:40]

    def fit(i, carry):
        here = pl.ds(pl.multiple_of(8 * i, 8), 8)
        for b in (1, 2):
            cols = slice(128 * b, 128 * b + 128)

            def sums(f):
                return win[pl.ds(pl.multiple_of(f * EH + 8 * i, 8), 8), cols]

            kz, phase, atten = (
                ext[pl.ds(pl.multiple_of(j * EH + 8 * i, 8), 8), cols] for j in range(3)
            )
            first = tuple(mom[n, here, cols] for n in range(5))
            phase, atten, power = fit_tile(sums, weights, weight, offset, phase, atten, first)
            spot = slice(128 * b - 128, 128 * b)
            mid[0, here, spot] = phase / kz
            mid[1, here, spot] = atten
            mid[2, here, spot] = power
        return carry

    lax.fori_loop(0, 5, fit, 0)


def around(field):
    return (
        pltpu.roll(field, 1, 0)
        + pltpu.roll(field, EH - 1, 0)
        + pltpu.roll(field, 1, 1)
        + pltpu.roll(field, EW - 1, 1)
    )


def make_fit_kernel(row_count, col_count, group):
    def kernel(
        win, ext, mom, shares, mid, far, near,
        depth, base, v0, v1, v2, sums,
        hi, lo, rim, wide,
    ):
        lane = lax.broadcasted_iota(jnp.int32, (8, 128), 1)
        row = lax.axis_index("row")
        col = lax.axis_index("col")
        odd_col = lax.rem(col, 2) == 1
        places = strips()
        packs = []
        for v in range(PACK // 8):
            one = far[8 * v : 8 * v + 8]
            two = near[8 * v : 8 * v + 8]
            packs.append((jnp.where(odd_col, one, two), jnp.where(odd_col, two, one)))

        def halo_tile(strip):
            v, at, width = places[strip]
            low, high = packs[v]
            if at:
                low = pltpu.roll(low, 128 - at, 1)
            high = pltpu.roll(high, 128 - at - width, 1)
            return jnp.where(lane < width, low, jnp.where(lane >= 128 - width, high, 0.0))

        for n in range(6):
            halo = jnp.concatenate([halo_tile(10 * n + i) for i in range(10)], axis=0)
            hi[80 * n : 80 * n + 80], lo[80 * n : 80 * n + 80] = split(halo)
        for n, shift in enumerate((128, 0, -128)):
            part = band(128, 128, shift)
            rim[:, 128 * n : 128 * n + 128] = dot(hi[...], part) + dot(lo[...], part)
        rim_of = {0: 0, 4: 1, 3: 2}
        weights = [shares[8 * n : 8 * n + 8] for n in range(3)]
        weight = shares[24:32]
        offset = shares[32:40]

        def tile(f, i, b):
            at = f * EH + 8 * i
            value = win[at : at + 8, 128 * b : 128 * b + 128]
            return value + rim[at : at + 8, 128 * rim_of[b] : 128 * rim_of[b] + 128]

        def gathered(parts):
            out = jnp.zeros((8, 128), jnp.float32)
            for i, part in enumerate(parts):
                here = (lane >= 8 * i) & (lane < 8 * i + 8)
                out = jnp.where(here, pltpu.roll(part, 8 * i + 4, 1), out)
            return out

        def rim_sums(f):
            return gathered([tile(f, i, 4) for i in range(5)])

        kz, phase, atten = (
            gathered([halo_tile((FIELDS + j) * 5 + i) for i in range(5)]) for j in range(3)
        )
        phase, _, power = fit_tile(rim_sums, weights, weight, offset, phase, atten, None)
        phase = phase / kz
        for i in range(5):
            here = slice(8 * i, 8 * i + 8)
            wide[0, here, W:EW] = pltpu.roll(phase, 124 - 8 * i, 1)
            wide[2, here, W:EW] = pltpu.roll(power, 124 - 8 * i, 1)
        for i in range(5):
            here = slice(8 * i, 8 * i + 8)
            for b in (0, 3):
                cols = slice(128 * b, 128 * b + 128)
                kz, phase, atten = (
                    ext[j * EH + 8 * i : j * EH + 8 * i + 8, cols] for j in range(3)
                )
                first = tuple(mom[n, here, cols] for n in range(5))
                phase, atten, power = fit_tile(
                    lambda f: tile(f, i, b), weights, weight, offset, phase, atten, first
                )
                wide[0, here, cols] = phase / kz
                wide[1, here, cols] = atten
                wide[2, here, cols] = power
        for n in range(3):
            wide[n, :, 128:384] = mid[n]
        depth[...] = wide[1, 0:H, 0:W]

        r = lax.broadcasted_iota(jnp.int32, (EH, EW), 0)
        c = lax.broadcasted_iota(jnp.int32, (EH, EW), 1)
        row_low = jnp.where(row == 0, EH - 4, EH)
        row_high = jnp.where(row == row_count - 1, H, EH - 4)
        col_low = jnp.where(col == 0, EW, EW - 4)
        col_high = jnp.where(col == col_count - 1, W, W + 4)
        row_bad = ((r >= row_high) & (r < EH - 4)) | (r >= row_low)
        col_bad = (c >= col_high) & (c < col_low)
        inside = jnp.logical_not(row_bad | col_bad)

        start = jnp.where(inside, wide[0], 0.0)
        confidence = wide[2] - 0.5
        base[...] = start[0:H, 0:W]
        first = jnp.where(inside, around(start) - 4.0 * start, 0.0)
        v0[...] = first[0:H, 0:W]

        def advance(field):
            return jnp.where(inside, (confidence * field - around(field)) * (1.0 / SCALE), 0.0)

        second = advance(first)
        v1[...] = second[0:H, 0:W]
        third = advance(second)
        v2[...] = third[0:H, 0:W]
        fourth = advance(third)
        a0, a1, a2, a3 = (x[0:H, 0:W] for x in (first, second, third, fourth))
        spots = lax.broadcasted_iota(jnp.int32, (1, 128), 1)
        line = jnp.zeros((1, 128), jnp.float32)
        for n, (p, q) in enumerate(((a0, a0), (a0, a1), (a1, a1), (a1, a2), (a2, a2), (a2, a3))):
            product = p * q
            total = jnp.sum(jnp.sum(product, axis=0, keepdims=True), axis=1, keepdims=True)
            line = jnp.where(spots == n, total, line)
        sums[...] = jnp.broadcast_to(line, (group, 128))

    return kernel


def make_relay_kernel(out_group):
    def kernel(parts, out):
        out[...] = jnp.broadcast_to(jnp.sum(parts[...], axis=0, keepdims=True), (out_group, 128))

    return kernel


def form(p, q, b):
    total = None
    for i, x in enumerate(p):
        for j, y in enumerate(q):
            term = x * y * b[i + j]
            total = term if total is None else total + term
    return total


def final_kernel(parts, base, v0, v1, v2, fitted, heights, depth, result, sems):
    first = pltpu.make_async_copy(fitted, depth, sems.at[0])
    first.start()
    line = jnp.sum(parts[...], axis=0, keepdims=True)
    spots = lax.broadcasted_iota(jnp.int32, (1, 128), 1)
    b = [
        jnp.sum(jnp.where(spots == n, line, 0.0), axis=1, keepdims=True) for n in range(6)
    ]

    def times_a(p):
        out = [SCALE * p[0]]
        for low, high in zip(p[:-1], p[1:]):
            out.append(SCALE * (low + high))
        return out + [SCALE * p[-1]]

    one = jnp.ones((1, 1), jnp.float32)
    zero = jnp.zeros((1, 1), jnp.float32)
    residual = [one]
    direction = [one]
    answer = [zero, zero, zero]
    now = b[0]
    for iteration in range(3):
        image = times_a(direction)
        alpha = now / form(direction, image, b)
        for n, x in enumerate(direction):
            answer[n] = answer[n] + alpha * x
        if iteration == 2:
            break
        residual = [
            (residual[n] if n < len(residual) else 0.0) - alpha * x for n, x in enumerate(image)
        ]
        after = form(residual, residual, b)
        beta = after / now
        direction = [
            x + (beta * direction[n] if n < len(direction) else 0.0)
            for n, x in enumerate(residual)
        ]
        now = after
    result[...] = base[...] + (answer[0] * v0[...] + (answer[1] * v1[...] + answer[2] * v2[...]))
    second = pltpu.make_async_copy(result, heights, sems.at[1])
    second.start()
    first.wait()
    second.wait()


def solution(mesh):
    row_count = mesh.shape["row"]
    col_count = mesh.shape["col"]

    def index(r, c):
        return r * col_count + c

    def outward(count):
        return sorted(range(count), key=lambda i: (abs(i - count // 2), i))

    ring = max(col_count // 8, 1)
    cores, ys = outward(2), outward(row_count // 2)
    xs, zs = outward(ring), outward(col_count // ring)
    near_groups = [
        [index(2 * y + core, x + ring * z) for core in cores for z in zs] for y in ys for x in xs
    ]
    far_groups = [
        [index(2 * y + core, x + ring * z) for y in ys for x in xs] for core in cores for z in zs
    ]
    near_count = len(near_groups[0])
    far_count = len(far_groups[0])
    both = ("row", "col")

    def swap(count, start):
        pairs = [(i, i + 1) for i in range(start, count - 1, 2)]
        return pairs + [(j, i) for i, j in pairs]

    def local(scatter_vectors, ground_ratio, wavenumber, phase, extinction):
        sv = scatter_vectors.reshape(FIELDS, H, W)
        inputs = (sv, wavenumber, phase, extinction)

        tile = pltpu.VMEM((FIELDS, 8, W), jnp.float32)
        edge = call(
            far_edges_kernel,
            f32(SEND_ROWS, W),
            [ANY] * 4,
            [tile, tile, pltpu.VMEM((3, 8, W), jnp.float32), pltpu.SemaphoreType.DMA((5,))],
            name="faredges",
            far=range(4),
        )(*inputs)
        busy = pl.CostEstimate(flops=6000000, transcendentals=0, bytes_accessed=0)
        far = lax.ppermute(edge, "row", swap(row_count, 1))
        edge = call(near_edges_kernel, f32(SEND_ROWS, W), [VM] * 4, name="nearedges", kept=range(4))(*inputs)
        near = lax.ppermute(edge, "row", swap(row_count, 0))
        mom, shares = call(
            early_kernel,
            (f32(5, EH, W), f32(40, 128)),
            [SM, VM, VM],
            name="early",
            kept=(1, 2),
            cost=busy,
        )(ground_ratio, phase, extinction)
        rows = call(
            own_rows_kernel,
            f32(FIELDS * EH, W),
            [VM],
            [pltpu.VMEM((4, 88, 128), jnp.float32), pltpu.VMEM((4, 64, 128), jnp.float32)],
            name="ownrows",
            kept=(0,),
            cost=busy,
        )(sv)
        far, near, mom, shares, rows = lax.optimization_barrier((far, near, mom, shares, rows))
        outer, ext, left, right = call(
            sides_kernel,
            (f32(FIELDS * EH, 256), f32(3 * EH, W), f32(PACK, 128), f32(PACK, 128)),
            [VM] * 6,
            HALO_SCRATCH,
            name="sides",
            kept=range(6),
        )(rows, wavenumber, phase, extinction, far, near)
        far_side = lax.ppermute(left, "col", swap(col_count, 1))
        near_side = lax.ppermute(right, "col", swap(col_count, 0))
        win, mom, mid = call(
            columns_kernel,
            (f32(FIELDS * EH, EW), f32(5, EH, W), f32(3, EH, 256)),
            [VM] * 7,
            [pltpu.VMEM((FIELDS * EH, W), jnp.bfloat16)] * 2
            + [pltpu.VMEM((FIELDS * EH, 256), jnp.float32)]
            + HALO_SCRATCH,
            name="colsums",
            kept=range(7),
            aliases={6: 1},
            cost=busy,
        )(rows, outer, far, near, ext, shares, mom)
        depth, base, v0, v1, v2, sums = call(
            make_fit_kernel(row_count, col_count, near_count),
            tuple(f32(H, W) for _ in range(5)) + (f32(near_count, 128),),
            [VM] * 7,
            [pltpu.VMEM((FIELDS * EH, 128), jnp.bfloat16)] * 2
            + [
                pltpu.VMEM((FIELDS * EH, 384), jnp.float32),
                pltpu.VMEM((3, EH, EW), jnp.float32),
            ],
            name="fit",
            kept=range(7),
        )(win, ext, mom, shares, mid, far_side, near_side)
        parts = lax.all_to_all(
            sums.reshape(near_count, 1, 128), both, 0, 0, axis_index_groups=near_groups
        ).reshape(near_count, 128)
        parts = call(make_relay_kernel(far_count), f32(far_count, 128), [VM], name="relay", kept=(0,))(parts)
        parts = lax.all_to_all(
            parts.reshape(far_count, 1, 128), both, 0, 0, axis_index_groups=far_groups
        ).reshape(far_count, 128)
        return call(
            final_kernel,
            (f32(H, W), f32(H, W)),
            [VM] * 6,
            [pltpu.VMEM((H, W), jnp.float32), pltpu.SemaphoreType.DMA((2,))],
            name="final",
            kept=range(6),
            leaves=(0, 1),
        )(parts, base, v0, v1, v2, depth)

    placed = (P(None, None, None, "row", "col"), P(), P("row", "col"), P("row", "col"), P("row", "col"))
    return jax.shard_map(
        local,
        mesh=mesh,
        in_specs=placed,
        out_specs=(P("row", "col"), P("row", "col")),
        check_vma=False,
    )
```
